128 devices in a mesh: row: 2 (over core), dep: 64 (over z, y, x).
Axes of the slice: x: 4, y: 4, z: 4, core: 2. Of those that a mesh axis runs over, the one named last changes fastest.
Arguments:
- x_vol: bfloat16 [2, 128, 8, 256, 128], P(None, 'dep', 'row')
- w_conv1: bfloat16 [3, 3, 3, 128, 128], replicated
- w_conv2: bfloat16 [3, 3, 3, 128, 128], replicated
- g_out: bfloat16 [2, 128, 8, 256, 128], P(None, 'dep', 'row')
Outputs:
- output 1: bfloat16 [2, 128, 8, 256, 128], P(None, 'dep', 'row')
- output 2: bfloat16 [2, 128, 8, 256, 128], P(None, 'dep', 'row')
- output 3: float32 [3, 3, 3, 128, 128], replicated
- output 4: float32 [3, 3, 3, 128, 128], replicated
All inputs are finite; a program needn't handle non-finite values.
Results may differ from the reference program's by a relative error of at most 0.00930195.
Values are sent between devices in bfloat16 or wider.
A program may use at most 1 GiB of HBM per device.

```python
import jax
import jax.numpy as jnp
from jax import lax

BATCH_SIZE = 2
VOL_DEPTH = 128
VOL_ROWS = 8
VOL_WIDTH = 256
CHANNELS = 128


def setup_inputs(seed: int = 0) -> dict:
    root_key = jax.random.key(seed)
    key_x, key_w1, key_w2, key_g = jax.random.split(root_key, 4)
    vol_shape = (BATCH_SIZE, VOL_DEPTH, VOL_ROWS, VOL_WIDTH, CHANNELS)
    kern_shape = (3, 3, 3, CHANNELS, CHANNELS)
    fan_scale = (27 * CHANNELS) ** -0.5
    x_vol = jax.random.normal(key_x, vol_shape, jnp.float32).astype(jnp.bfloat16)
    w_conv1 = (fan_scale * jax.random.normal(key_w1, kern_shape, jnp.float32)).astype(jnp.bfloat16)
    w_conv2 = (1.5 * fan_scale * jax.random.normal(key_w2, kern_shape, jnp.float32)).astype(jnp.bfloat16)
    g_out = jax.random.normal(key_g, vol_shape, jnp.float32).astype(jnp.bfloat16)
    return {'x_vol': x_vol, 'w_conv1': w_conv1, 'w_conv2': w_conv2, 'g_out': g_out}


def conv_same(volume, kernel):
    return lax.conv_general_dilated(volume, kernel, (1, 1, 1), 'SAME', dimension_numbers=('NDHWC', 'DHWIO', 'NDHWC'))


def gelu_tanh(values):
    return jax.nn.gelu(values, approximate=True)


def reference(x_vol, w_conv1, w_conv2, g_out):
    x_f32 = x_vol.astype(jnp.float32)
    g_f32 = g_out.astype(jnp.float32)
    pre_f32, conv1_back = jax.vjp(conv_same, x_f32, w_conv1.astype(jnp.float32))
    pre_act = pre_f32.astype(jnp.bfloat16)
    gelu_f32, gelu_back = jax.vjp(gelu_tanh, pre_act.astype(jnp.float32))
    gelu_bf = gelu_f32.astype(jnp.bfloat16)
    out_f32, conv2_back = jax.vjp(conv_same, gelu_bf.astype(jnp.float32), w_conv2.astype(jnp.float32))
    y_out = (out_f32 + x_f32).astype(jnp.bfloat16)
    dgelu_f32, dw_conv2 = conv2_back(g_f32)
    dpre_bf = gelu_back(dgelu_f32)[0].astype(jnp.bfloat16)
    dx_f32, dw_conv1 = conv1_back(dpre_bf.astype(jnp.float32))
    dx_vol = (dx_f32 + g_f32).astype(jnp.bfloat16)
    return (y_out, dx_vol, dw_conv1, dw_conv2)
```

```python
import functools
import math

import jax
import jax.numpy as jnp
from jax import lax
from jax.experimental import pallas as pl
from jax.experimental.pallas import tpu as pltpu
from jax.sharding import PartitionSpec as P

MESH = pl.DeviceIdType.MESH
F32 = jnp.float32
BF16 = jnp.bfloat16
S2PI = math.sqrt(2.0 / math.pi)
C3 = 0.044715

NB, ND, NH, NC = 2, 2, 4, 128
RING = 4
TAPS = 28
TQ = TAPS // RING


def kernel(width, depth_count,
           x_hbm, w1_hbm, w2_hbm, g_hbm,
           y_hbm, dx_hbm, dw1_hbm, dw2_hbm,
           xe, ge, ze, ae, w1, w2, acc1, acc2, dgel, zt, at, obuf,
           p2, p1, cr, r1, bz, r2, xb, ds, es,
           hs_send, hs_recv, rs_send, rs_recv, ar_send, ar_recv, lsem, osem):
    rows = NH * width
    row = lax.axis_index("row")
    dep = lax.axis_index("dep")
    x = lax.rem(dep, RING)
    y = lax.rem(dep // RING, RING)
    z = dep // (RING * RING)
    other = 1 - row
    exts = (xe, ge, ze, ae)
    edge = (NH - 1) - (NH - 1) * row
    my_pad = (NH + 1) * row

    def ring_dep(axis, off):
        if axis == "x":
            return dep - x + lax.rem(x + off, RING)
        if axis == "y":
            return dep - RING * y + RING * lax.rem(y + off, RING)
        return dep - RING * RING * z + RING * RING * lax.rem(z + off, RING)

    def rdma(src, dst, ssem, rsem, dev):
        return pltpu.make_async_remote_copy(src_ref=src, dst_ref=dst, send_sem=ssem, recv_sem=rsem, device_id=dev, device_id_type=MESH)

    has_below = dep > 0
    has_above = dep < depth_count - 1

    def face(k, src_of, up, part):
        h0, hn = (edge, 1) if part == 0 else (row, NH - 1)
        d_src, d_dst = (ND - 1, 0) if up else (0, ND + 1)
        dev = (row, dep + 1) if up else (row, dep - 1)
        n = 2 * part + (0 if up else 1)
        return rdma(src_of(d_src, h0, hn), exts[k].at[:, d_dst, pl.ds(1 + h0, hn)], hs_send.at[k, n], hs_recv.at[k, n], dev)

    def side(k, src_of):
        return rdma(src_of(None, edge, 1), exts[k].at[:, pl.ds(1, ND), pl.ds(my_pad, 1)], rs_send.at[k, 0], rs_recv.at[k, 0], (other, dep))

    def corner(k, up):
        d_dst = 0 if up else ND + 1
        n = 1 if up else 2
        return rdma(exts[k].at[:, d_dst, pl.ds(1 + edge, 1)], exts[k].at[:, d_dst, pl.ds(my_pad, 1)], rs_send.at[k, n], rs_recv.at[k, n], (other, dep))

    def from_hbm(ref):
        def src(d, h0, hn):
            return ref.at[:, pl.ds(0, ND) if d is None else d, pl.ds(h0, hn)]
        return src

    def from_ext(ref):
        def src(d, h0, hn):
            return ref.at[:, pl.ds(1, ND) if d is None else 1 + d, pl.ds(1 + h0, hn)]
        return src

    sources = (from_hbm(x_hbm), from_hbm(g_hbm), from_ext(ze), from_ext(ae))

    def send_faces(k):
        side(k, sources[k]).start()
        for part in range(2):
            @pl.when(has_above)
            def _():
                face(k, sources[k], True, part).start()

            @pl.when(has_below)
            def _():
                face(k, sources[k], False, part).start()

    def pass_corners(k):
        @pl.when(has_below)
        def _():
            face(k, sources[k], True, 0).wait_recv()
            corner(k, True).start()

        @pl.when(has_above)
        def _():
            face(k, sources[k], False, 0).wait_recv()
            corner(k, False).start()

    def take_faces(k):
        @pl.when(has_below)
        def _():
            face(k, sources[k], True, 1).wait_recv()
            corner(k, True).wait_recv()

        @pl.when(has_above)
        def _():
            face(k, sources[k], False, 1).wait_recv()
            corner(k, False).wait_recv()

    def finish_halo(k):
        side(k, sources[k]).wait_send()
        for part in range(2):
            @pl.when(has_above)
            def _():
                face(k, sources[k], True, part).wait_send()

            @pl.when(has_below)
            def _():
                face(k, sources[k], False, part).wait_send()

        @pl.when(has_below)
        def _():
            corner(k, True).wait_send()

        @pl.when(has_above)
        def _():
            corner(k, False).wait_send()

    barrier = pltpu.get_barrier_semaphore()
    pl.semaphore_signal(barrier, inc=1, device_id=(other, dep), device_id_type=MESH)
    for axis in ("x", "y", "z"):
        for off in range(1, RING):
            pl.semaphore_signal(barrier, inc=1, device_id=(row, ring_dep(axis, off)), device_id_type=MESH)

    for step in (1, depth_count - 1):
        pl.semaphore_signal(barrier, inc=1, device_id=(row, lax.rem(dep + step, depth_count)), device_id_type=MESH)

    loads = [
        pltpu.make_async_copy(x_hbm, xe.at[:, pl.ds(1, ND), pl.ds(1, NH)], lsem.at[0]),
        pltpu.make_async_copy(w1_hbm, w1, lsem.at[1]),
        pltpu.make_async_copy(g_hbm, ge.at[:, pl.ds(1, ND), pl.ds(1, NH)], lsem.at[2]),
        pltpu.make_async_copy(w2_hbm, w2, lsem.at[3]),
    ]
    for load in loads:
        load.start()

    pl.semaphore_wait(barrier, 12)

    send_faces(0)
    send_faces(1)

    zero_row = jnp.zeros((NB, 1, width, NC), BF16)
    for ext in exts:
        for dd in range(ND + 2):
            ext[:, dd, pl.ds(my_pad, 1)] = zero_row
    zero_face = jnp.zeros((NH + 2, width, NC), BF16)

    @pl.when(dep == 0)
    def _():
        for ext in exts:
            for b in range(NB):
                ext[b, 0] = zero_face

    @pl.when(dep == depth_count - 1)
    def _():
        for ext in exts:
            for b in range(NB):
                ext[b, ND + 1] = zero_face

    p2[TAPS - 1] = jnp.zeros((NC, NC), F32)
    p1[TAPS - 1] = jnp.zeros((NC, NC), F32)

    def lines(ext, b, dd, h0):
        return ext[b, dd, pl.ds(h0, NH)].reshape(rows, NC)

    def tap_block(w, td, th, tw, flip):
        return w[2 - td, 2 - th, 2 - tw] if flip else w[td, th, tw]

    def weights(w, cells, flip):
        zero = jnp.zeros((NC, NC), BF16)
        blocks = [[zero if t is None else tap_block(w, *t, flip) for t in line] for line in cells]
        if flip:
            return jnp.concatenate([jnp.concatenate([blocks[k][n] for k in range(len(blocks))], axis=1) for n in range(len(blocks[0]))], axis=0)
        return jnp.concatenate([jnp.concatenate(line, axis=1) for line in blocks], axis=0)

    def mul(lhs, rhs, flip):
        return lax.dot_general(lhs, rhs, (((1,), (1 if flip else 0,)), ((), ())), preferred_element_type=F32)

    def conv_inner(ext, w, acc, flip):
        cells = []
        for dd in (1, 2):
            for th in range(3):
                cells.append([(dd, th, 0), (dd, th, 1), (dd - 1, th, 0), (dd - 1, th, 1), (dd, th, 2), (dd - 1, th, 2)])
        order = ((0, 0), (0, 1), (1, 0), (1, 1), (0, 2), (1, 2))

        def one(b, carry):
            lhs = jnp.concatenate([lines(ext, b, dd, th) for dd in (1, 2) for th in range(3)], axis=1)
            for n in range(3):
                out = mul(lhs, weights(w, [line[2 * n:2 * n + 2] for line in cells], flip), flip)
                for j in range(2):
                    d, tw = order[2 * n + j]
                    acc[b, d * 3 + tw] = out[:, j * NC:(j + 1) * NC]
            return carry

        lax.fori_loop(0, NB, one, 0)

    def conv_outer(ext, w, acc, flip):
        def one(i, carry):
            b, d = i // ND, lax.rem(i, ND)
            td = 2 * d
            lhs = jnp.concatenate([lines(ext, b, 3 * d, th) for th in range(3)], axis=1)
            out = mul(lhs, weights(w, [[(td, th, tw) for tw in range(3)] for th in range(3)], flip), flip)
            for tw in range(3):
                acc[b, d * 3 + tw] += out[:, tw * NC:(tw + 1) * NC]
            return carry

        lax.fori_loop(0, NB * ND, one, 0)

    wpos = lax.broadcasted_iota(jnp.int32, (width, NC), 0)

    def from_left(v):
        return jnp.where(wpos > 0, pltpu.roll(v, 1, 0), 0.0)

    def from_right(v):
        return jnp.where(wpos < width - 1, pltpu.roll(v, width - 1, 0), 0.0)

    def each_row(acc, use):
        def one(i, carry):
            b, d, h = i // (ND * NH), lax.rem(i // NH, ND), lax.rem(i, NH)
            at_rows = pl.ds(pl.multiple_of(h * width, width), width)
            total = acc[b, d * 3 + 1, at_rows] + from_left(acc[b, d * 3, at_rows]) + from_right(acc[b, d * 3 + 2, at_rows])
            use(i, b, d, h, total)
            return carry

        lax.fori_loop(0, NB * ND * NH, one, 0)

    def after_conv1(i, b, d, h, total):
        a = total.astype(BF16).astype(F32)
        a2 = a * a
        t = jnp.tanh(S2PI * (a + C3 * (a2 * a)))
        cdf = 0.5 * (1.0 + t)
        gel = a * cdf
        dgel[i] = cdf + (0.5 * a * ((1.0 + t) * (1.0 - t))) * (S2PI * (1.0 + 3.0 * C3 * a2))
        ze[b, 1 + d, 1 + h] = gel.astype(BF16)
        for tw, v in enumerate((from_left(gel), gel, from_right(gel))):
            zt[i, pl.ds(tw * NC, NC)] = v.astype(BF16).T

    def after_conv_g(i, b, d, h, total):
        da = total * dgel[i]
        ae[b, 1 + d, 1 + h] = da.astype(BF16)
        for tw, v in enumerate((from_right(da), da, from_left(da))):
            at[i, pl.ds(tw * NC, NC)] = v.astype(BF16).T

    def after_add(ext):
        def use(i, b, d, h, total):
            obuf[b, d, h] = (total + ext[b, 1 + d, 1 + h].astype(F32)).astype(BF16)
        return use

    def weight_grad(own_t, ext, part, swap):
        def rhs(td, th):
            d0, h0 = (2 - td, 2 - th) if swap else (td, th)
            return jnp.concatenate([lines(ext, b, d + d0, h0) for b in range(NB) for d in range(ND)], axis=0)

        def product(right):
            lhs = jnp.concatenate([own_t[i] for i in range(NB * ND * NH)], axis=1)
            return jnp.dot(lhs, right, preferred_element_type=F32)

        def put(out, n, td, th):
            for tw in range(3):
                blk = out[tw * NC:(tw + 1) * NC, n * NC:(n + 1) * NC]
                part[td * 9 + th * 3 + tw] = blk if swap else blk.T

        def one(td, carry):
            out = product(jnp.concatenate([rhs(td, 0), rhs(td, 1)], axis=1))
            put(out, 0, td, 0)
            put(out, 1, td, 1)
            return carry

        lax.fori_loop(0, 3, one, 0)
        out = product(jnp.concatenate([rhs(0, 2), rhs(1, 2)], axis=1))
        put(out, 0, 0, 2)
        put(out, 1, 1, 2)
        put(product(rhs(2, 2)), 0, 2, 2)

    half, quarter = NC // 2, NC // 8
    axes = (("y", "z"), ("z", "y"))
    coord = {"x": x, "y": y, "z": z}
    parts = (p2, p1)
    outs = (dw2_hbm, dw1_hbm)

    def sems(s, n):
        return ar_send.at[s, n], ar_recv.at[s, n]

    def pair_copy(s):
        theirs = pl.ds(pl.multiple_of(other * half, half), half)
        return rdma(parts[s].at[:, theirs], cr.at[s], *sems(s, 0), (other, dep))

    def first_copy(s, off):
        axis = axes[s][0]
        j = lax.rem(coord[axis] + off, RING)
        src = parts[s].at[:, pl.ds(pl.multiple_of(row * half + j * quarter, quarter), quarter)]
        return rdma(src, r1.at[s, off - 1], *sems(s, off), (row, ring_dep(axis, off)))

    def second_copy(s, off):
        axis = axes[s][1]
        j = lax.rem(coord[axis] + off, RING)
        return rdma(bz.at[s, pl.ds(j * TQ, TQ)], r2.at[s, off - 1], *sems(s, 3 + off), (row, ring_dep(axis, off)))

    def third_copy(s, off, slot):
        return rdma(xb.at[s, slot], xb.at[s, slot], *sems(s, 6 + off), (row, ring_dep("x", off)))

    def fourth_copy(s, off, j):
        axis = axes[s][1]
        return rdma(ds.at[s, pl.ds(j * TQ, TQ)], ds.at[s, pl.ds(j * TQ, TQ)], *sems(s, 9 + off), (row, ring_dep(axis, off)))

    def fifth_copy(s, off, j):
        axis = axes[s][0]
        return rdma(ds.at[s], es.at[s, :, pl.ds(pl.multiple_of(j * quarter, quarter), quarter)], *sems(s, 12 + off), (row, ring_dep(axis, off)))

    my_half = pl.ds(pl.multiple_of(row * half, half), half)

    def last_copy(s):
        return rdma(es.at[s, pl.ds(0, 27)], outs[s].at[:, my_half], *sems(s, 16), (other, dep))

    def own_copy(s):
        return pltpu.make_async_copy(es.at[s, pl.ds(0, 27)], outs[s].at[:, my_half], osem.at[2 + s])

    def step_pair(s):
        pair_copy(s).wait_recv()

        def add(t, carry):
            parts[s][t, my_half] += cr[s, t]
            return carry

        lax.fori_loop(0, TAPS, add, 0)
        for off in (2, 1, 3):
            first_copy(s, off).start()

    def step_first(s):
        for off in (1, 2, 3):
            first_copy(s, off).wait_recv()
        mine = pl.ds(pl.multiple_of(row * half + coord[axes[s][0]] * quarter, quarter), quarter)

        def add(t, carry):
            bz[s, t] = (parts[s][t, mine] + r1[s, 0, t]) + (r1[s, 1, t] + r1[s, 2, t])
            return carry

        lax.fori_loop(0, TAPS, add, 0)
        for off in (2, 1, 3):
            second_copy(s, off).start()

    def step_second(s):
        for off in (1, 2, 3):
            second_copy(s, off).wait_recv()
        c = coord[axes[s][1]]

        def add(t, carry):
            xb[s, x, t] = (bz[s, c * TQ + t] + r2[s, 0, t]) + (r2[s, 1, t] + r2[s, 2, t])
            return carry

        lax.fori_loop(0, TQ, add, 0)
        for off in (2, 1, 3):
            third_copy(s, off, x).start()

    def step_third(s):
        for off in (1, 2, 3):
            third_copy(s, off, lax.rem(x + RING - off, RING)).wait_recv()
        c = coord[axes[s][1]]

        def add(t, carry):
            ds[s, c * TQ + t] = (xb[s, 0, t] + xb[s, 1, t]) + (xb[s, 2, t] + xb[s, 3, t])
            return carry

        lax.fori_loop(0, TQ, add, 0)
        for off in (2, 1, 3):
            fourth_copy(s, off, c).start()

    def step_fourth(s):
        c = coord[axes[s][1]]
        for off in (1, 2, 3):
            fourth_copy(s, off, lax.rem(c + RING - off, RING)).wait_recv()
        c0 = coord[axes[s][0]]
        for off in (2, 1, 3):
            fifth_copy(s, off, c0).start()

        def move(t, carry):
            es[s, t, pl.ds(pl.multiple_of(c0 * quarter, quarter), quarter)] = ds[s, t]
            return carry

        lax.fori_loop(0, TAPS, move, 0)

    def step_fifth(s):
        c0 = coord[axes[s][0]]
        for off in (1, 2, 3):
            fifth_copy(s, off, lax.rem(c0 + RING - off, RING)).wait_recv()
        last_copy(s).start()
        own_copy(s).start()

    def finish_sum(s):
        last_copy(s).wait()
        own_copy(s).wait()
        pair_copy(s).wait_send()
        for off in (1, 2, 3):
            first_copy(s, off).wait_send()
            second_copy(s, off).wait_send()
            third_copy(s, off, x).wait_send()
            fourth_copy(s, off, coord[axes[s][1]]).wait_send()
            fifth_copy(s, off, coord[axes[s][0]]).wait_send()

    loads[0].wait()
    loads[1].wait()
    side(0, sources[0]).wait_recv()
    conv_inner(xe, w1, acc1, False)
    loads[2].wait()
    loads[3].wait()
    side(1, sources[1]).wait_recv()
    conv_inner(ge, w2, acc2, True)
    pass_corners(0)
    take_faces(0)
    conv_outer(xe, w1, acc1, False)
    each_row(acc1, after_conv1)
    send_faces(2)
    pass_corners(1)
    take_faces(1)
    weight_grad(zt, ge, p2, True)
    pair_copy(0).start()
    conv_outer(ge, w2, acc2, True)
    each_row(acc2, after_conv_g)
    send_faces(3)
    step_pair(0)
    weight_grad(at, xe, p1, False)
    pair_copy(1).start()
    pass_corners(2)
    side(2, sources[2]).wait_recv()
    conv_inner(ze, w2, acc1, False)
    step_pair(1)
    step_first(0)
    side(3, sources[3]).wait_recv()
    conv_inner(ae, w1, acc2, True)
    step_second(0)
    take_faces(2)
    conv_outer(ze, w2, acc1, False)
    step_first(1)
    pass_corners(3)
    each_row(acc1, after_add(xe))
    y_out = pltpu.make_async_copy(obuf, y_hbm, osem.at[0])
    y_out.start()
    step_third(0)
    step_second(1)
    take_faces(3)
    conv_outer(ae, w1, acc2, True)
    step_fourth(0)
    step_third(1)
    y_out.wait()
    each_row(acc2, after_add(ge))
    dx_out = pltpu.make_async_copy(obuf, dx_hbm, osem.at[1])
    dx_out.start()
    step_fourth(1)
    step_fifth(0)
    step_fifth(1)
    dx_out.wait()
    for k in range(4):
        finish_halo(k)
    finish_sum(0)
    finish_sum(1)


def solution(mesh):
    depth_count = mesh.shape["dep"]
    vol_spec = P(None, "dep", "row", None, None)

    def local_step(x_tile, w_conv1, w_conv2, g_tile):
        width = x_tile.shape[3]
        ext = pltpu.VMEM((NB, ND + 2, NH + 2, width, NC), BF16)
        acc = pltpu.VMEM((NB, 6, NH * width, NC), F32)
        trans = pltpu.VMEM((NB * ND * NH, 3 * NC, width), BF16)
        wts = pltpu.VMEM((3, 3, 3, NC, NC), BF16)
        part = pltpu.VMEM((TAPS, NC, NC), F32)
        anywhere = pl.BlockSpec(memory_space=pl.ANY)
        outs = pl.pallas_call(
            functools.partial(kernel, width, depth_count),
            out_shape=(
                jax.ShapeDtypeStruct(x_tile.shape, BF16),
                jax.ShapeDtypeStruct(x_tile.shape, BF16),
                jax.ShapeDtypeStruct((27, NC, NC), F32),
                jax.ShapeDtypeStruct((27, NC, NC), F32),
            ),
            in_specs=[anywhere] * 4,
            out_specs=(anywhere,) * 4,
            scratch_shapes=[
                ext, ext, ext, ext, wts, wts, acc, acc,
                pltpu.VMEM((NB * ND * NH, width, NC), F32),
                trans, trans,
                pltpu.VMEM((NB, ND, NH, width, NC), BF16),
                part, part,
                pltpu.VMEM((2, TAPS, NC // 2, NC), F32),
                pltpu.VMEM((2, RING - 1, TAPS, NC // 8, NC), F32),
                pltpu.VMEM((2, TAPS, NC // 8, NC), F32),
                pltpu.VMEM((2, RING - 1, TQ, NC // 8, NC), F32),
                pltpu.VMEM((2, RING, TQ, NC // 8, NC), F32),
                pltpu.VMEM((2, TAPS, NC // 8, NC), F32),
                pltpu.VMEM((2, TAPS, NC // 2, NC), F32),
                pltpu.SemaphoreType.DMA((4, 4)),
                pltpu.SemaphoreType.DMA((4, 4)),
                pltpu.SemaphoreType.DMA((4, 3)),
                pltpu.SemaphoreType.DMA((4, 3)),
                pltpu.SemaphoreType.DMA((2, 17)),
                pltpu.SemaphoreType.DMA((2, 17)),
                pltpu.SemaphoreType.DMA((4,)),
                pltpu.SemaphoreType.DMA((4,)),
            ],
            compiler_params=pltpu.CompilerParams(collective_id=0, has_side_effects=True, vmem_limit_bytes=66 * 1000 * 1000),
        )(x_tile, w_conv1, w_conv2, g_tile)
        y_tile, dx_tile, dw1, dw2 = outs
        shape = w_conv1.shape
        return (y_tile, dx_tile, dw1.reshape(shape), dw2.reshape(shape))

    return jax.shard_map(local_step, mesh=mesh, in_specs=(vol_spec, P(), P(), vol_spec), out_specs=(vol_spec, vol_spec, P(), P()), check_vma=False)
```

```python
import functools
import math

import jax
import jax.numpy as jnp
from jax import lax
from jax.experimental import pallas as pl
from jax.experimental.pallas import tpu as pltpu
from jax.sharding import PartitionSpec as P

MESH = pl.DeviceIdType.MESH
F32 = jnp.float32
BF16 = jnp.bfloat16
S2PI = math.sqrt(2.0 / math.pi)
C3 = 0.044715

NB, ND, NH, NC = 2, 2, 4, 128
RING = 4
TAPS = 28
TQ = TAPS // RING


def kernel(width, depth_count,
           x_hbm, w1_hbm, w2_hbm, g_hbm,
           y_out, dx_out, dw1_out, dw2_out,
           xe, ge, ze, ae, w1, w2, acc1, acc2, dgel, zt, at,
           p2, p1, cr, ra, rb, rl, rr, bz, r2, xb, ds,
           hs_send, hs_recv, rs_send, rs_recv, ar_send, ar_recv, lsem):
    rows = NH * width
    row = lax.axis_index("row")
    dep = lax.axis_index("dep")
    x = lax.rem(dep, RING)
    y = lax.rem(dep // RING, RING)
    z = dep // (RING * RING)
    other = 1 - row
    exts = (xe, ge, ze, ae)
    edge = (NH - 1) - (NH - 1) * row
    my_pad = (NH + 1) * row

    def ring_dep(axis, off):
        if axis == "x":
            return dep - x + lax.rem(x + off, RING)
        if axis == "y":
            return dep - RING * y + RING * lax.rem(y + off, RING)
        return dep - RING * RING * z + RING * RING * lax.rem(z + off, RING)

    def rdma(src, dst, ssem, rsem, dev):
        return pltpu.make_async_remote_copy(src_ref=src, dst_ref=dst, send_sem=ssem, recv_sem=rsem, device_id=dev, device_id_type=MESH)

    has_below = dep > 0
    has_above = dep < depth_count - 1

    def face(k, src_of, up, part):
        h0, hn = (edge, 1) if part == 0 else (row, NH - 1)
        d_src, d_dst = (ND - 1, 0) if up else (0, ND + 1)
        dev = (row, dep + 1) if up else (row, dep - 1)
        n = 2 * part + (0 if up else 1)
        return rdma(src_of(d_src, h0, hn), exts[k].at[:, d_dst, pl.ds(1 + h0, hn)], hs_send.at[k, n], hs_recv.at[k, n], dev)

    def side(k, src_of):
        return rdma(src_of(None, edge, 1), exts[k].at[:, pl.ds(1, ND), pl.ds(my_pad, 1)], rs_send.at[k, 0], rs_recv.at[k, 0], (other, dep))

    def corner(k, up):
        d_dst = 0 if up else ND + 1
        n = 1 if up else 2
        return rdma(exts[k].at[:, d_dst, pl.ds(1 + edge, 1)], exts[k].at[:, d_dst, pl.ds(my_pad, 1)], rs_send.at[k, n], rs_recv.at[k, n], (other, dep))

    def from_hbm(ref):
        def src(d, h0, hn):
            return ref.at[:, pl.ds(0, ND) if d is None else d, pl.ds(h0, hn)]
        return src

    def from_ext(ref):
        def src(d, h0, hn):
            return ref.at[:, pl.ds(1, ND) if d is None else 1 + d, pl.ds(1 + h0, hn)]
        return src

    sources = (from_hbm(x_hbm), from_hbm(g_hbm), from_ext(ze), from_ext(ae))

    def send_faces(k):
        side(k, sources[k]).start()
        for part in range(2):
            @pl.when(has_above)
            def _():
                face(k, sources[k], True, part).start()

            @pl.when(has_below)
            def _():
                face(k, sources[k], False, part).start()

    def pass_corners(k):
        @pl.when(has_below)
        def _():
            face(k, sources[k], True, 0).wait_recv()
            corner(k, True).start()

        @pl.when(has_above)
        def _():
            face(k, sources[k], False, 0).wait_recv()
            corner(k, False).start()

    def take_faces(k):
        @pl.when(has_below)
        def _():
            face(k, sources[k], True, 1).wait_recv()
            corner(k, True).wait_recv()

        @pl.when(has_above)
        def _():
            face(k, sources[k], False, 1).wait_recv()
            corner(k, False).wait_recv()

    def finish_halo(k):
        side(k, sources[k]).wait_send()
        for part in range(2):
            @pl.when(has_above)
            def _():
                face(k, sources[k], True, part).wait_send()

            @pl.when(has_below)
            def _():
                face(k, sources[k], False, part).wait_send()

        @pl.when(has_below)
        def _():
            corner(k, True).wait_send()

        @pl.when(has_above)
        def _():
            corner(k, False).wait_send()

    barrier = pltpu.get_barrier_semaphore()
    pl.semaphore_signal(barrier, inc=1, device_id=(other, dep), device_id_type=MESH)
    for axis in ("x", "y", "z"):
        for off in range(1, RING):
            pl.semaphore_signal(barrier, inc=1, device_id=(row, ring_dep(axis, off)), device_id_type=MESH)

    for step in (1, depth_count - 1):
        pl.semaphore_signal(barrier, inc=1, device_id=(row, lax.rem(dep + step, depth_count)), device_id_type=MESH)

    loads = [
        pltpu.make_async_copy(x_hbm, xe.at[:, pl.ds(1, ND), pl.ds(1, NH)], lsem.at[0]),
        pltpu.make_async_copy(w1_hbm, w1, lsem.at[1]),
        pltpu.make_async_copy(g_hbm, ge.at[:, pl.ds(1, ND), pl.ds(1, NH)], lsem.at[2]),
        pltpu.make_async_copy(w2_hbm, w2, lsem.at[3]),
    ]
    for load in loads:
        load.start()

    pl.semaphore_wait(barrier, 12)

    send_faces(0)
    send_faces(1)

    zero_row = jnp.zeros((NB, 1, width, NC), BF16)
    for ext in exts:
        for dd in range(ND + 2):
            ext[:, dd, pl.ds(my_pad, 1)] = zero_row
    zero_face = jnp.zeros((NH + 2, width, NC), BF16)

    @pl.when(dep == 0)
    def _():
        for ext in exts:
            for b in range(NB):
                ext[b, 0] = zero_face

    @pl.when(dep == depth_count - 1)
    def _():
        for ext in exts:
            for b in range(NB):
                ext[b, ND + 1] = zero_face

    p2[TAPS - 1] = jnp.zeros((NC, NC), F32)
    p1[TAPS - 1] = jnp.zeros((NC, NC), F32)

    def lines(ext, b, dd, h0):
        return ext[b, dd, pl.ds(h0, NH)].reshape(rows, NC)

    def tap_block(w, td, th, tw, flip):
        return w[2 - td, 2 - th, 2 - tw] if flip else w[td, th, tw]

    def weights(w, cells, flip):
        zero = jnp.zeros((NC, NC), BF16)
        blocks = [[zero if t is None else tap_block(w, *t, flip) for t in line] for line in cells]
        if flip:
            return jnp.concatenate([jnp.concatenate([blocks[k][n] for k in range(len(blocks))], axis=1) for n in range(len(blocks[0]))], axis=0)
        return jnp.concatenate([jnp.concatenate(line, axis=1) for line in blocks], axis=0)

    def mul(lhs, rhs, flip):
        return lax.dot_general(lhs, rhs, (((1,), (1 if flip else 0,)), ((), ())), preferred_element_type=F32)

    def conv_inner(ext, w, acc, flip):
        cells = []
        for dd in (1, 2):
            for th in range(3):
                cells.append([(dd, th, 0), (dd, th, 1), (dd - 1, th, 0), (dd - 1, th, 1), (dd, th, 2), (dd - 1, th, 2)])
        order = ((0, 0), (0, 1), (1, 0), (1, 1), (0, 2), (1, 2))

        def one(b, carry):
            lhs = jnp.concatenate([lines(ext, b, dd, th) for dd in (1, 2) for th in range(3)], axis=1)
            for n in range(3):
                out = mul(lhs, weights(w, [line[2 * n:2 * n + 2] for line in cells], flip), flip)
                for j in range(2):
                    d, tw = order[2 * n + j]
                    acc[b, d * 3 + tw] = out[:, j * NC:(j + 1) * NC]
            return carry

        lax.fori_loop(0, NB, one, 0)

    def conv_outer(ext, w, acc, flip):
        def one(i, carry):
            b, d = i // ND, lax.rem(i, ND)
            td = 2 * d
            lhs = jnp.concatenate([lines(ext, b, 3 * d, th) for th in range(3)], axis=1)
            out = mul(lhs, weights(w, [[(td, th, tw) for tw in range(3)] for th in range(3)], flip), flip)
            for tw in range(3):
                acc[b, d * 3 + tw] += out[:, tw * NC:(tw + 1) * NC]
            return carry

        lax.fori_loop(0, NB * ND, one, 0)

    wpos = lax.broadcasted_iota(jnp.int32, (width, NC), 0)

    def from_left(v):
        return jnp.where(wpos > 0, pltpu.roll(v, 1, 0), 0.0)

    def from_right(v):
        return jnp.where(wpos < width - 1, pltpu.roll(v, width - 1, 0), 0.0)

    def each_row(acc, use):
        def one(i, carry):
            b, d, h = i // (ND * NH), lax.rem(i // NH, ND), lax.rem(i, NH)
            at_rows = pl.ds(pl.multiple_of(h * width, width), width)
            total = acc[b, d * 3 + 1, at_rows] + from_left(acc[b, d * 3, at_rows]) + from_right(acc[b, d * 3 + 2, at_rows])
            use(i, b, d, h, total)
            return carry

        lax.fori_loop(0, NB * ND * NH, one, 0)

    def after_conv1(i, b, d, h, total):
        a = total.astype(BF16).astype(F32)
        a2 = a * a
        t = jnp.tanh(S2PI * (a + C3 * (a2 * a)))
        cdf = 0.5 * (1.0 + t)
        gel = a * cdf
        dgel[i] = cdf + (0.5 * a * ((1.0 + t) * (1.0 - t))) * (S2PI * (1.0 + 3.0 * C3 * a2))
        ze[b, 1 + d, 1 + h] = gel.astype(BF16)
        for tw, v in enumerate((from_left(gel), gel, from_right(gel))):
            zt[i, pl.ds(tw * NC, NC)] = v.astype(BF16).T

    def after_conv_g(i, b, d, h, total):
        da = total * dgel[i]
        ae[b, 1 + d, 1 + h] = da.astype(BF16)
        for tw, v in enumerate((from_right(da), da, from_left(da))):
            at[i, pl.ds(tw * NC, NC)] = v.astype(BF16).T

    def after_add(ext, out):
        def use(i, b, d, h, total):
            out[b, d, h] = (total + ext[b, 1 + d, 1 + h].astype(F32)).astype(BF16)
        return use

    def tap_index(td, th):
        return td * 6 + th * 3 if th < 2 else 18 + td * 3

    def weight_grad(own_t, ext, part, swap, between):
        def rhs(td, th):
            d0, h0 = (2 - td, 2 - th) if swap else (td, th)
            return jnp.concatenate([lines(ext, b, d + d0, h0) for b in range(NB) for d in range(ND)], axis=0)

        def product(right):
            lhs = jnp.concatenate([own_t[i] for i in range(NB * ND * NH)], axis=1)
            return jnp.dot(lhs, right, preferred_element_type=F32)

        def put(out, n, td, th):
            for tw in range(3):
                blk = out[tw * NC:(tw + 1) * NC, n * NC:(n + 1) * NC]
                part[tap_index(td, th) + tw] = blk if swap else blk.T

        groups = [((td, 0), (td, 1)) for td in range(3)] + [((0, 2), (1, 2)), ((2, 2),)]
        for k, taps in enumerate(groups):
            out = product(jnp.concatenate([rhs(*t) for t in taps], axis=1))
            for n, t in enumerate(taps):
                put(out, n, *t)
            between(k)

    half, piece = NC // 2, NC // 16
    axes = (("y", "z"), ("z", "y"))
    coord = {"x": x, "y": y, "z": z}
    parts = (p2, p1)
    outs = (dw2_out, dw1_out)
    low, high = pl.ds(0, TAPS // 2), pl.ds(TAPS // 2, TAPS // 2)
    high27 = pl.ds(TAPS // 2, TAPS // 2 - 1)

    def sems(q, n):
        return ar_send.at[q, n], ar_recv.at[q, n]

    def turn(c, off):
        return lax.rem(c + off, RING)

    def chunk(q, off):
        c = turn(coord[axes[q % 2][0]], off)
        return pl.ds(pl.multiple_of(row * half + (q % 2) * (half // 2) + c * piece, piece), piece)

    def pair_copy(s, n):
        theirs = pl.ds(pl.multiple_of(other * half, half), half)
        taps = pl.ds(0, 18) if n == 0 else pl.ds(18, TAPS - 18)
        return rdma(parts[s].at[taps, theirs], cr.at[s, taps], *sems(2 * s + n, 22), (other, dep))

    def scatter_copy(q, n):
        part = parts[q // 2]
        nxt, prv = (row, ring_dep(axes[q % 2][0], 1)), (row, ring_dep(axes[q % 2][0], RING - 1))
        src, dst, dev = (
            (part.at[low, chunk(q, 2)], ra.at[q], nxt),
            (part.at[high, chunk(q, 2)], rb.at[q], prv),
            (part.at[high, chunk(q, 1)], rl.at[q, high], nxt),
            (part.at[low, chunk(q, 3)], rr.at[q, low], prv),
            (ra.at[q], rl.at[q, low], nxt),
            (rb.at[q], rr.at[q, high], prv),
        )[n]
        return rdma(src, dst, *sems(q, n), dev)

    def second_copy(q, off):
        axis = axes[q % 2][1]
        j = turn(coord[axis], off)
        return rdma(bz.at[q, pl.ds(j * TQ, TQ)], r2.at[q, off - 1], *sems(q, 5 + off), (row, ring_dep(axis, off)))

    def third_copy(q, off, slot):
        return rdma(xb.at[q, slot], xb.at[q, slot], *sems(q, 8 + off), (row, ring_dep("x", off)))

    def fourth_copy(q, off, j):
        return rdma(ds.at[q, pl.ds(j * TQ, TQ)], ds.at[q, pl.ds(j * TQ, TQ)], *sems(q, 11 + off), (row, ring_dep(axes[q % 2][1], off)))

    def gather_copy(q, n):
        out = outs[q // 2]
        nxt, prv = (row, ring_dep(axes[q % 2][0], 1)), (row, ring_dep(axes[q % 2][0], RING - 1))
        taps, off, dev = (
            (low, 0, nxt),
            (high27, 0, prv),
            (high27, 0, nxt),
            (low, 0, prv),
            (low, 3, nxt),
            (high27, 1, prv),
        )[n]
        src = ds.at[q, taps] if n < 4 else out.at[taps, chunk(q, off)]
        return rdma(src, out.at[taps, chunk(q, off)], *sems(q, 15 + n), dev)

    def last_copy(q):
        rows_q = pl.ds(pl.multiple_of(row * half + (q % 2) * (half // 2), half // 2), half // 2)
        return rdma(outs[q // 2].at[:, rows_q], outs[q // 2].at[:, rows_q], *sems(q, 21), (other, dep))

    my_half = pl.ds(pl.multiple_of(row * half, half), half)

    def step_pair(s):
        pair_copy(s, 0).wait_recv()
        pair_copy(s, 1).wait_recv()

        def add(t, carry):
            parts[s][t, my_half] += cr[s, t]
            return carry

        lax.fori_loop(0, TAPS, add, 0)
        for n in range(4):
            for u in range(2):
                scatter_copy(2 * s + u, n).start()

    def step_relay(q):
        part = parts[q // 2]
        to_next, to_prev = chunk(q, 1), chunk(q, 3)
        scatter_copy(q, 0).wait_recv()
        ra[q] += part[low, to_next]
        scatter_copy(q, 4).start()
        scatter_copy(q, 1).wait_recv()
        rb[q] += part[high, to_prev]
        scatter_copy(q, 5).start()

    def step_first(q):
        for n in range(2, 6):
            scatter_copy(q, n).wait_recv()
        bz[q] = parts[q // 2][:, chunk(q, 0)] + (rl[q] + rr[q])
        for off in (2, 1, 3):
            second_copy(q, off).start()

    def step_second(q):
        for off in (1, 2, 3):
            second_copy(q, off).wait_recv()
        c = coord[axes[q % 2][1]]
        xb[q, x] = (bz[q, pl.ds(c * TQ, TQ)] + r2[q, 0]) + (r2[q, 1] + r2[q, 2])
        for off in (2, 1, 3):
            third_copy(q, off, x).start()

    def step_third(q):
        for off in (1, 2, 3):
            third_copy(q, off, turn(x, RING - off)).wait_recv()
        c = coord[axes[q % 2][1]]
        ds[q, pl.ds(c * TQ, TQ)] = (xb[q, 0] + xb[q, 1]) + (xb[q, 2] + xb[q, 3])
        for off in (2, 1, 3):
            fourth_copy(q, off, c).start()

    def step_fourth(q):
        c = coord[axes[q % 2][1]]
        for off in (1, 2, 3):
            fourth_copy(q, off, turn(c, RING - off)).wait_recv()
        for n in range(4):
            gather_copy(q, n).start()
        outs[q // 2][:, chunk(q, 0)] = ds[q, pl.ds(0, 27)]

    def step_forward(q):
        gather_copy(q, 0).wait_recv()
        gather_copy(q, 4).start()
        gather_copy(q, 1).wait_recv()
        gather_copy(q, 5).start()

    def step_fifth(q):
        for n in range(2, 6):
            gather_copy(q, n).wait_recv()
        last_copy(q).start()

    def finish_sum(q):
        last_copy(q).wait()
        pair_copy(q // 2, q % 2).wait_send()
        for n in range(6):
            scatter_copy(q, n).wait_send()
            gather_copy(q, n).wait_send()
        for off in (1, 2, 3):
            second_copy(q, off).wait_send()
            third_copy(q, off, x).wait_send()
            fourth_copy(q, off, coord[axes[q % 2][1]]).wait_send()

    def after_dw2(k):
        if k == 2:
            pair_copy(0, 0).start()
        if k == 4:
            pair_copy(0, 1).start()

    def after_dw1(k):
        if k == 1:
            step_relay(0)
            step_relay(1)
        if k == 2:
            pair_copy(1, 0).start()
        if k == 4:
            pair_copy(1, 1).start()

    loads[0].wait()
    loads[1].wait()
    side(0, sources[0]).wait_recv()
    conv_inner(xe, w1, acc1, False)
    loads[2].wait()
    loads[3].wait()
    side(1, sources[1]).wait_recv()
    conv_inner(ge, w2, acc2, True)
    pass_corners(0)
    take_faces(0)
    conv_outer(xe, w1, acc1, False)
    each_row(acc1, after_conv1)
    send_faces(2)
    pass_corners(1)
    side(2, sources[2]).wait_recv()
    conv_inner(ze, w2, acc1, False)
    take_faces(1)
    weight_grad(zt, ge, p2, True, after_dw2)
    conv_outer(ge, w2, acc2, True)
    step_pair(0)
    each_row(acc2, after_conv_g)
    send_faces(3)
    weight_grad(at, xe, p1, False, after_dw1)
    pass_corners(2)
    step_first(0)
    step_first(1)
    step_pair(1)
    take_faces(2)
    conv_outer(ze, w2, acc1, False)
    step_second(0)
    step_second(1)
    each_row(acc1, after_add(xe, y_out))
    step_relay(2)
    step_relay(3)
    side(3, sources[3]).wait_recv()
    conv_inner(ae, w1, acc2, True)
    step_third(0)
    step_third(1)
    step_first(2)
    step_first(3)
    pass_corners(3)
    take_faces(3)
    conv_outer(ae, w1, acc2, True)
    each_row(acc2, after_add(ge, dx_out))
    step_fourth(0)
    step_fourth(1)
    step_second(2)
    step_second(3)
    step_forward(0)
    step_forward(1)
    step_third(2)
    step_third(3)
    step_fifth(0)
    step_fifth(1)
    step_fourth(2)
    step_fourth(3)
    step_forward(2)
    step_forward(3)
    step_fifth(2)
    step_fifth(3)
    for k in range(4):
        finish_halo(k)
    for q in range(4):
        finish_sum(q)


def to_hbm(y_vm, dx_vm, dw1_vm, dw2_vm, y_hbm, dx_hbm, dw1_hbm, dw2_hbm, sem):
    copies = [(y_vm, y_hbm), (dx_vm, dx_hbm)]
    for src, dst in ((dw1_vm, dw1_hbm), (dw2_vm, dw2_hbm)):
        for td in range(3):
            copies.append((src.at[pl.ds(td * 6, 6)], dst.at[pl.ds(td * 9, 6)]))
            copies.append((src.at[pl.ds(18 + td * 3, 3)], dst.at[pl.ds(td * 9 + 6, 3)]))
    started = [pltpu.make_async_copy(src, dst, sem.at[n]) for n, (src, dst) in enumerate(copies)]
    for copy in started:
        copy.start()
    for copy in started:
        copy.wait()


def solution(mesh):
    depth_count = mesh.shape["dep"]
    vol_spec = P(None, "dep", "row", None, None)

    def local_step(x_tile, w_conv1, w_conv2, g_tile):
        width = x_tile.shape[3]
        ext = pltpu.VMEM((NB, ND + 2, NH + 2, width, NC), BF16)
        acc = pltpu.VMEM((NB, 6, NH * width, NC), F32)
        trans = pltpu.VMEM((NB * ND * NH, 3 * NC, width), BF16)
        wts = pltpu.VMEM((3, 3, 3, NC, NC), BF16)
        part = pltpu.VMEM((TAPS, NC, NC), F32)
        anywhere = pl.BlockSpec(memory_space=pl.ANY)
        outs = pl.pallas_call(
            functools.partial(kernel, width, depth_count),
            out_shape=(
                pltpu.VMEM(x_tile.shape, BF16),
                pltpu.VMEM(x_tile.shape, BF16),
                pltpu.VMEM((27, NC, NC), F32),
                pltpu.VMEM((27, NC, NC), F32),
            ),
            in_specs=[anywhere] * 4,
            out_specs=(pl.BlockSpec(memory_space=pltpu.VMEM),) * 4,
            scratch_shapes=[
                ext, ext, ext, ext, wts, wts, acc, acc,
                pltpu.VMEM((NB * ND * NH, width, NC), F32),
                trans, trans,
                part, part,
                pltpu.VMEM((2, TAPS, NC // 2, NC), F32),
                pltpu.VMEM((4, TAPS // 2, NC // 16, NC), F32),
                pltpu.VMEM((4, TAPS // 2, NC // 16, NC), F32),
                pltpu.VMEM((4, TAPS, NC // 16, NC), F32),
                pltpu.VMEM((4, TAPS, NC // 16, NC), F32),
                pltpu.VMEM((4, TAPS, NC // 16, NC), F32),
                pltpu.VMEM((4, RING - 1, TQ, NC // 16, NC), F32),
                pltpu.VMEM((4, RING, TQ, NC // 16, NC), F32),
                pltpu.VMEM((4, TAPS, NC // 16, NC), F32),
                pltpu.SemaphoreType.DMA((4, 4)),
                pltpu.SemaphoreType.DMA((4, 4)),
                pltpu.SemaphoreType.DMA((4, 3)),
                pltpu.SemaphoreType.DMA((4, 3)),
                pltpu.SemaphoreType.DMA((4, 23)),
                pltpu.SemaphoreType.DMA((4, 23)),
                pltpu.SemaphoreType.DMA((4,)),
            ],
            compiler_params=pltpu.CompilerParams(collective_id=0, has_side_effects=True, vmem_limit_bytes=56 * 1000 * 1000),
        )(x_tile, w_conv1, w_conv2, g_tile)
        y_tile, dx_tile, dw1, dw2 = pl.pallas_call(
            to_hbm,
            out_shape=(
                jax.ShapeDtypeStruct(x_tile.shape, BF16),
                jax.ShapeDtypeStruct(x_tile.shape, BF16),
                jax.ShapeDtypeStruct((27, NC, NC), F32),
                jax.ShapeDtypeStruct((27, NC, NC), F32),
            ),
            in_specs=[pl.BlockSpec(memory_space=pltpu.VMEM)] * 4,
            out_specs=(anywhere,) * 4,
            scratch_shapes=[pltpu.SemaphoreType.DMA((14,))],
            compiler_params=pltpu.CompilerParams(vmem_limit_bytes=4 * 1000 * 1000),
        )(*outs)
        shape = w_conv1.shape
        return (y_tile, dx_tile, dw1.reshape(shape), dw2.reshape(shape))

    return jax.shard_map(local_step, mesh=mesh, in_specs=(vol_spec, P(), P(), vol_spec), out_specs=(vol_spec, vol_spec, P(), P()), check_vma=False)
```

```python
import functools
import math

import jax
import jax.numpy as jnp
from jax import lax
from jax.experimental import pallas as pl
from jax.experimental.pallas import tpu as pltpu
from jax.sharding import PartitionSpec as P

MESH = pl.DeviceIdType.MESH
F32 = jnp.float32
BF16 = jnp.bfloat16
S2PI = math.sqrt(2.0 / math.pi)
C3 = 0.044715

NB, ND, NH, NC = 2, 2, 4, 128
RING = 4
TAPS = 28
TQ = TAPS // RING


def kernel(width, depth_count,
           x_hbm, w1_hbm, w2_hbm, g_hbm,
           y_out, dx_out, dw1_out, dw2_out,
           xe, ge, ze, ae, w1, w2, acc1, acc2, dgel, zt, at,
           p2, p1, cr, ra, rb, rl, rr, bz, r2, xb, ds, hold,
           hs_send, hs_recv, rs_send, rs_recv, ar_send, ar_recv, hold_send, hold_recv, lsem):
    rows = NH * width
    row = lax.axis_index("row")
    dep = lax.axis_index("dep")
    x = lax.rem(dep, RING)
    y = lax.rem(dep // RING, RING)
    z = dep // (RING * RING)
    other = 1 - row
    exts = (xe, ge, ze, ae)
    edge = (NH - 1) - (NH - 1) * row
    my_pad = (NH + 1) * row

    def ring_dep(axis, off):
        if axis == "x":
            return dep - x + lax.rem(x + off, RING)
        if axis == "y":
            return dep - RING * y + RING * lax.rem(y + off, RING)
        return dep - RING * RING * z + RING * RING * lax.rem(z + off, RING)

    def rdma(src, dst, ssem, rsem, dev):
        return pltpu.make_async_remote_copy(src_ref=src, dst_ref=dst, send_sem=ssem, recv_sem=rsem, device_id=dev, device_id_type=MESH)

    has_below = dep > 0
    has_above = dep < depth_count - 1
    near_above, near_below = x < RING - 1, x > 0
    far_above, far_below = has_above & (x == RING - 1), has_below & (x == 0)

    def face(k, src_of, up, part):
        h0, hn = (edge, 1) if part == 0 else (row, NH - 1)
        d_src, d_dst = (ND - 1, 0) if up else (0, ND + 1)
        dev = (row, dep + 1) if up else (row, dep - 1)
        n = 2 * part + (0 if up else 1)
        return rdma(src_of(d_src, h0, hn), exts[k].at[:, d_dst, pl.ds(1 + h0, hn)], hs_send.at[k, n], hs_recv.at[k, n], dev)

    def side(k, src_of):
        return rdma(src_of(None, edge, 1), exts[k].at[:, pl.ds(1, ND), pl.ds(my_pad, 1)], rs_send.at[k, 0], rs_recv.at[k, 0], (other, dep))

    def corner(k, up):
        d_dst = 0 if up else ND + 1
        n = 1 if up else 2
        return rdma(exts[k].at[:, d_dst, pl.ds(1 + edge, 1)], exts[k].at[:, d_dst, pl.ds(my_pad, 1)], rs_send.at[k, n], rs_recv.at[k, n], (other, dep))

    def from_hbm(ref):
        def src(d, h0, hn):
            return ref.at[:, pl.ds(0, ND) if d is None else d, pl.ds(h0, hn)]
        return src

    def from_ext(ref):
        def src(d, h0, hn):
            return ref.at[:, pl.ds(1, ND) if d is None else 1 + d, pl.ds(1 + h0, hn)]
        return src

    sources = (from_hbm(x_hbm), from_hbm(g_hbm), from_ext(ze), from_ext(ae))

    def send_faces(k, above, below):
        for part in range(2):
            @pl.when(above)
            def _():
                face(k, sources[k], True, part).start()

            @pl.when(below)
            def _():
                face(k, sources[k], False, part).start()

    split = (2, 3)
    relays_up, relays_down = (x == RING - 1) & (dep >= RING), (x == 0) & (dep < depth_count - RING)

    def far_row(k, up):
        d_src, d_dst = (ND - 1, 0) if up else (0, ND + 1)
        dev = (row, dep + 1) if up else (row, dep - 1)
        n = 4 if up else 5
        return rdma(sources[k](d_src, row, 1), exts[k].at[:, d_dst, pl.ds(1 + row, 1)], hs_send.at[k, n], hs_recv.at[k, n], dev)

    def far_hop(k, up):
        dev = (row, dep + RING) if up else (row, dep - RING)
        return rdma(sources[k](ND - 1 if up else 0, row + 1, 2), hold.at[k - 2], hold_send.at[k - 2], hold_recv.at[k - 2], dev)

    def far_land(k, up):
        d_dst = 0 if up else ND + 1
        dev = (row, dep - (RING - 1)) if up else (row, dep + (RING - 1))
        n = 6 if up else 7
        return rdma(hold.at[k - 2], exts[k].at[:, d_dst, pl.ds(2 + row, 2)], hs_send.at[k, n], hs_recv.at[k, n], dev)

    def send_far_faces(k):
        for up, cond in ((True, far_above), (False, far_below)):
            @pl.when(cond)
            def _():
                face(k, sources[k], up, 0).start()
                far_row(k, up).start()

    def send_far_hops(k):
        for up, cond in ((True, far_above), (False, far_below)):
            @pl.when(cond)
            def _():
                far_hop(k, up).start()

    def relay_far(k):
        for up, cond in ((True, relays_up), (False, relays_down)):
            @pl.when(cond)
            def _():
                far_hop(k, up).wait_recv()
                far_land(k, up).start()

    def pass_corners(k):
        @pl.when(has_below)
        def _():
            face(k, sources[k], True, 0).wait_recv()
            corner(k, True).start()

        @pl.when(has_above)
        def _():
            face(k, sources[k], False, 0).wait_recv()
            corner(k, False).start()

    def take_faces(k):
        for up, has, whole in ((True, has_below, x > 0), (False, has_above, x < RING - 1)):
            @pl.when(has)
            def _():
                corner(k, up).wait_recv()

            @pl.when(has if k not in split else has & whole)
            def _():
                face(k, sources[k], up, 1).wait_recv()

            if k in split:
                @pl.when(has & jnp.logical_not(whole))
                def _():
                    far_row(k, up).wait_recv()
                    far_land(k, up).wait_recv()

    def finish_halo(k):
        side(k, sources[k]).wait_send()
        for up, has, far, whole in ((True, has_above, far_above, near_above), (False, has_below, far_below, near_below)):
            @pl.when(has)
            def _():
                face(k, sources[k], up, 0).wait_send()

            @pl.when(has if k not in split else whole)
            def _():
                face(k, sources[k], up, 1).wait_send()

            if k in split:
                @pl.when(far)
                def _():
                    far_row(k, up).wait_send()
                    far_hop(k, up).wait_send()

        if k in split:
            for up, cond in ((True, relays_up), (False, relays_down)):
                @pl.when(cond)
                def _():
                    far_land(k, up).wait_send()

        @pl.when(has_below)
        def _():
            corner(k, True).wait_send()

        @pl.when(has_above)
        def _():
            corner(k, False).wait_send()

    barrier = pltpu.get_barrier_semaphore()
    pl.semaphore_signal(barrier, inc=1, device_id=(other, dep), device_id_type=MESH)
    for axis in ("x", "y", "z"):
        for off in range(1, RING):
            pl.semaphore_signal(barrier, inc=1, device_id=(row, ring_dep(axis, off)), device_id_type=MESH)

    for step in (1, depth_count - 1, RING, depth_count - RING):
        pl.semaphore_signal(barrier, inc=1, device_id=(row, lax.rem(dep + step, depth_count)), device_id_type=MESH)

    loads = [
        pltpu.make_async_copy(x_hbm, xe.at[:, pl.ds(1, ND), pl.ds(1, NH)], lsem.at[0]),
        pltpu.make_async_copy(w1_hbm, w1, lsem.at[1]),
        pltpu.make_async_copy(g_hbm, ge.at[:, pl.ds(1, ND), pl.ds(1, NH)], lsem.at[2]),
        pltpu.make_async_copy(w2_hbm, w2, lsem.at[3]),
    ]
    for load in loads:
        load.start()

    pl.semaphore_wait(barrier, 14)

    for k in range(2):
        side(k, sources[k]).start()
        send_faces(k, has_above, has_below)

    zero_row = jnp.zeros((NB, 1, width, NC), BF16)
    for ext in exts:
        for dd in range(ND + 2):
            ext[:, dd, pl.ds(my_pad, 1)] = zero_row
    zero_face = jnp.zeros((NH + 2, width, NC), BF16)

    @pl.when(dep == 0)
    def _():
        for ext in exts:
            for b in range(NB):
                ext[b, 0] = zero_face

    @pl.when(dep == depth_count - 1)
    def _():
        for ext in exts:
            for b in range(NB):
                ext[b, ND + 1] = zero_face

    p2[TAPS - 1] = jnp.zeros((NC, NC), F32)
    p1[TAPS - 1] = jnp.zeros((NC, NC), F32)

    def lines(ext, b, dd, h0):
        return ext[b, dd, pl.ds(h0, NH)].reshape(rows, NC)

    def tap_block(w, td, th, tw, flip):
        return w[2 - td, 2 - th, 2 - tw] if flip else w[td, th, tw]

    def weights(w, cells, flip):
        zero = jnp.zeros((NC, NC), BF16)
        blocks = [[zero if t is None else tap_block(w, *t, flip) for t in line] for line in cells]
        if flip:
            return jnp.concatenate([jnp.concatenate([blocks[k][n] for k in range(len(blocks))], axis=1) for n in range(len(blocks[0]))], axis=0)
        return jnp.concatenate([jnp.concatenate(line, axis=1) for line in blocks], axis=0)

    def mul(lhs, rhs, flip):
        return lax.dot_general(lhs, rhs, (((1,), (1 if flip else 0,)), ((), ())), preferred_element_type=F32)

    def conv_inner(ext, w, acc, flip, b0=0, b1=NB):
        cells = []
        for dd in (1, 2):
            for th in range(3):
                cells.append([(dd, th, 0), (dd, th, 1), (dd - 1, th, 0), (dd - 1, th, 1), (dd, th, 2), (dd - 1, th, 2)])
        order = ((0, 0), (0, 1), (1, 0), (1, 1), (0, 2), (1, 2))

        def one(b, carry):
            lhs = jnp.concatenate([lines(ext, b, dd, th) for dd in (1, 2) for th in range(3)], axis=1)
            for n in range(3):
                out = mul(lhs, weights(w, [line[2 * n:2 * n + 2] for line in cells], flip), flip)
                for j in range(2):
                    d, tw = order[2 * n + j]
                    acc[b, d * 3 + tw] = out[:, j * NC:(j + 1) * NC]
            return carry

        lax.fori_loop(b0, b1, one, 0)

    def conv_outer(ext, w, acc, flip):
        def one(i, carry):
            b, d = i // ND, lax.rem(i, ND)
            td = 2 * d
            lhs = jnp.concatenate([lines(ext, b, 3 * d, th) for th in range(3)], axis=1)
            out = mul(lhs, weights(w, [[(td, th, tw) for tw in range(3)] for th in range(3)], flip), flip)
            for tw in range(3):
                acc[b, d * 3 + tw] += out[:, tw * NC:(tw + 1) * NC]
            return carry

        lax.fori_loop(0, NB * ND, one, 0)

    wpos = lax.broadcasted_iota(jnp.int32, (width, NC), 0)

    def from_left(v):
        return jnp.where(wpos > 0, pltpu.roll(v, 1, 0), 0.0)

    def from_right(v):
        return jnp.where(wpos < width - 1, pltpu.roll(v, width - 1, 0), 0.0)

    def each_row(acc, use):
        def one(i, carry):
            b, d, h = i // (ND * NH), lax.rem(i // NH, ND), lax.rem(i, NH)
            at_rows = pl.ds(pl.multiple_of(h * width, width), width)
            total = acc[b, d * 3 + 1, at_rows] + from_left(acc[b, d * 3, at_rows]) + from_right(acc[b, d * 3 + 2, at_rows])
            use(i, b, d, h, total)
            return carry

        lax.fori_loop(0, NB * ND * NH, one, 0)

    def after_conv1(i, b, d, h, total):
        a = total.astype(BF16).astype(F32)
        a2 = a * a
        t = jnp.tanh(S2PI * (a + C3 * (a2 * a)))
        cdf = 0.5 * (1.0 + t)
        gel = a * cdf
        dgel[i] = cdf + (0.5 * a * ((1.0 + t) * (1.0 - t))) * (S2PI * (1.0 + 3.0 * C3 * a2))
        ze[b, 1 + d, 1 + h] = gel.astype(BF16)
        for tw, v in enumerate((from_left(gel), gel, from_right(gel))):
            zt[i, pl.ds(tw * NC, NC)] = v.astype(BF16).T

    def after_conv_g(i, b, d, h, total):
        da = total * dgel[i]
        ae[b, 1 + d, 1 + h] = da.astype(BF16)
        for tw, v in enumerate((from_right(da), da, from_left(da))):
            at[i, pl.ds(tw * NC, NC)] = v.astype(BF16).T

    def after_add(ext, out):
        def use(i, b, d, h, total):
            out[b, d, h] = (total + ext[b, 1 + d, 1 + h].astype(F32)).astype(BF16)
        return use

    def tap_index(td, th):
        return td * 6 + th * 3 if th < 2 else 18 + td * 3

    def weight_grad(own_t, ext, part, swap, between):
        def rhs(td, th):
            d0, h0 = (2 - td, 2 - th) if swap else (td, th)
            return jnp.concatenate([lines(ext, b, d + d0, h0) for b in range(NB) for d in range(ND)], axis=0)

        def product(right):
            lhs = jnp.concatenate([own_t[i] for i in range(NB * ND * NH)], axis=1)
            return jnp.dot(lhs, right, preferred_element_type=F32)

        def put(out, n, td, th):
            for tw in range(3):
                blk = out[tw * NC:(tw + 1) * NC, n * NC:(n + 1) * NC]
                part[tap_index(td, th) + tw] = blk if swap else blk.T

        groups = [((td, 0), (td, 1)) for td in range(3)] + [((0, 2), (1, 2)), ((2, 2),)]
        for k, taps in enumerate(groups):
            out = product(jnp.concatenate([rhs(*t) for t in taps], axis=1))
            for n, t in enumerate(taps):
                put(out, n, *t)
            between(k)

    half, piece = NC // 2, NC // 16
    axes = (("y", "z"), ("z", "y"))
    coord = {"x": x, "y": y, "z": z}
    parts = (p2, p1)
    outs = (dw2_out, dw1_out)
    low, high = pl.ds(0, TAPS // 2), pl.ds(TAPS // 2, TAPS // 2)
    high27 = pl.ds(TAPS // 2, TAPS // 2 - 1)

    def sems(q, n):
        return ar_send.at[q, n], ar_recv.at[q, n]

    def turn(c, off):
        return lax.rem(c + off, RING)

    def chunk(q, off):
        c = turn(coord[axes[q % 2][0]], off)
        return pl.ds(pl.multiple_of(row * half + (q % 2) * (half // 2) + c * piece, piece), piece)

    def pair_copy(s, n):
        theirs = pl.ds(pl.multiple_of(other * half, half), half)
        taps = pl.ds(0, 18) if n == 0 else pl.ds(18, TAPS - 18)
        return rdma(parts[s].at[taps, theirs], cr.at[s, taps], *sems(2 * s + n, 26), (other, dep))

    def scatter_copy(q, n):
        part = parts[q // 2]
        nxt, prv = (row, ring_dep(axes[q % 2][0], 1)), (row, ring_dep(axes[q % 2][0], RING - 1))
        src, dst, dev = (
            (part.at[low, chunk(q, 2)], ra.at[q], nxt),
            (part.at[high, chunk(q, 2)], rb.at[q], prv),
            (part.at[high, chunk(q, 1)], rl.at[q, high], nxt),
            (part.at[low, chunk(q, 3)], rr.at[q, low], prv),
            (ra.at[q], rl.at[q, low], nxt),
            (rb.at[q], rr.at[q, high], prv),
        )[n]
        return rdma(src, dst, *sems(q, n), dev)

    def second_copy(q, off):
        axis = axes[q % 2][1]
        j = turn(coord[axis], off)
        return rdma(bz.at[q, pl.ds(j * TQ, TQ)], r2.at[q, off - 1], *sems(q, 5 + off), (row, ring_dep(axis, off)))

    def third_copy(q, off, slot):
        return rdma(xb.at[q, slot], xb.at[q, slot], *sems(q, 8 + off), (row, ring_dep("x", off)))

    def fourth_copy(q, off, j):
        return rdma(ds.at[q, pl.ds(j * TQ, TQ)], ds.at[q, pl.ds(j * TQ, TQ)], *sems(q, 11 + off), (row, ring_dep(axes[q % 2][1], off)))

    def gather_copy(q, n):
        out = outs[q // 2]
        nxt, prv = (row, ring_dep(axes[q % 2][0], 1)), (row, ring_dep(axes[q % 2][0], RING - 1))
        taps, off, dev = (
            (low, 0, nxt),
            (high27, 0, prv),
            (high27, 0, nxt),
            (low, 0, prv),
            (low, 3, nxt),
            (high27, 1, prv),
        )[n]
        src = ds.at[q, taps] if n < 4 else out.at[taps, chunk(q, off)]
        return rdma(src, out.at[taps, chunk(q, off)], *sems(q, 15 + n), dev)

    def out_copy(q, n):
        out = outs[q // 2]
        taps, off = ((pl.ds(0, 27), 0), (pl.ds(0, 27), 3), (pl.ds(0, 27), 1), (low, 2), (high27, 2))[n]
        src = ds.at[q, taps] if n == 0 else out.at[taps, chunk(q, off)]
        return rdma(src, out.at[taps, chunk(q, off)], *sems(q, 21 + n), (other, dep))

    my_half = pl.ds(pl.multiple_of(row * half, half), half)

    def step_pair(s):
        pair_copy(s, 0).wait_recv()
        pair_copy(s, 1).wait_recv()

        def add(t, carry):
            parts[s][t, my_half] += cr[s, t]
            return carry

        lax.fori_loop(0, TAPS, add, 0)
        for n in range(4):
            for u in range(2):
                scatter_copy(2 * s + u, n).start()

    def step_relay(q):
        part = parts[q // 2]
        to_next, to_prev = chunk(q, 1), chunk(q, 3)
        scatter_copy(q, 0).wait_recv()
        ra[q] += part[low, to_next]
        scatter_copy(q, 4).start()
        scatter_copy(q, 1).wait_recv()
        rb[q] += part[high, to_prev]
        scatter_copy(q, 5).start()

    def step_first(q):
        for n in range(2, 6):
            scatter_copy(q, n).wait_recv()
        bz[q] = parts[q // 2][:, chunk(q, 0)] + (rl[q] + rr[q])
        for off in (2, 1, 3):
            second_copy(q, off).start()

    def step_second(q):
        for off in (1, 2, 3):
            second_copy(q, off).wait_recv()
        c = coord[axes[q % 2][1]]
        xb[q, x] = (bz[q, pl.ds(c * TQ, TQ)] + r2[q, 0]) + (r2[q, 1] + r2[q, 2])
        for off in (2, 1, 3):
            third_copy(q, off, x).start()

    def step_third(q):
        for off in (1, 2, 3):
            third_copy(q, off, turn(x, RING - off)).wait_recv()
        c = coord[axes[q % 2][1]]
        ds[q, pl.ds(c * TQ, TQ)] = (xb[q, 0] + xb[q, 1]) + (xb[q, 2] + xb[q, 3])
        for off in (2, 1, 3):
            fourth_copy(q, off, c).start()

    def step_fourth(q):
        c = coord[axes[q % 2][1]]
        for off in (1, 2, 3):
            fourth_copy(q, off, turn(c, RING - off)).wait_recv()
        for n in range(4):
            gather_copy(q, n).start()
        out_copy(q, 0).start()
        outs[q // 2][:, chunk(q, 0)] = ds[q, pl.ds(0, 27)]

    def step_forward(q):
        gather_copy(q, 0).wait_recv()
        gather_copy(q, 4).start()
        gather_copy(q, 1).wait_recv()
        gather_copy(q, 5).start()

    def step_fifth(q):
        for n in range(2, 6):
            gather_copy(q, n).wait_recv()
            out_copy(q, n - 1).start()

    def finish_sum(q):
        for n in range(5):
            out_copy(q, n).wait()
        pair_copy(q // 2, q % 2).wait_send()
        for n in range(6):
            scatter_copy(q, n).wait_send()
            gather_copy(q, n).wait_send()
        for off in (1, 2, 3):
            second_copy(q, off).wait_send()
            third_copy(q, off, x).wait_send()
            fourth_copy(q, off, coord[axes[q % 2][1]]).wait_send()

    def after_dw2(k):
        if k == 2:
            pair_copy(0, 0).start()
        if k == 4:
            pair_copy(0, 1).start()

    def after_dw1(k):
        if k == 2:
            pair_copy(1, 0).start()
            step_relay(0)
            step_relay(1)
        if k == 4:
            pair_copy(1, 1).start()

    loads[0].wait()
    loads[1].wait()
    side(0, sources[0]).wait_recv()
    conv_inner(xe, w1, acc1, False)
    loads[2].wait()
    loads[3].wait()
    side(1, sources[1]).wait_recv()
    conv_inner(ge, w2, acc2, True)
    pass_corners(0)
    take_faces(0)
    conv_outer(xe, w1, acc1, False)
    each_row(acc1, after_conv1)
    side(2, sources[2]).start()
    send_faces(2, near_above, near_below)
    send_far_faces(2)
    send_far_hops(2)
    pass_corners(1)
    side(2, sources[2]).wait_recv()
    conv_inner(ze, w2, acc1, False)
    take_faces(1)
    weight_grad(zt, ge, p2, True, after_dw2)
    relay_far(2)
    conv_outer(ge, w2, acc2, True)
    step_pair(0)
    each_row(acc2, after_conv_g)
    side(3, sources[3]).start()
    send_faces(3, near_above, near_below)
    send_far_faces(3)
    send_far_hops(3)
    weight_grad(at, xe, p1, False, after_dw1)
    pass_corners(2)
    step_pair(1)
    step_first(0)
    step_first(1)
    take_faces(2)
    conv_outer(ze, w2, acc1, False)
    relay_far(3)
    step_relay(2)
    step_relay(3)
    step_second(0)
    step_second(1)
    each_row(acc1, after_add(xe, y_out))
    side(3, sources[3]).wait_recv()
    conv_inner(ae, w1, acc2, True, 0, 1)
    step_first(2)
    step_first(3)
    step_third(0)
    step_third(1)
    pass_corners(3)
    conv_inner(ae, w1, acc2, True, 1, 2)
    step_second(2)
    step_second(3)
    step_fourth(0)
    step_fourth(1)
    take_faces(3)
    conv_outer(ae, w1, acc2, True)
    step_third(2)
    step_third(3)
    step_forward(0)
    step_forward(1)
    each_row(acc2, after_add(ge, dx_out))
    step_fourth(2)
    step_fourth(3)
    step_fifth(0)
    step_fifth(1)
    step_forward(2)
    step_forward(3)
    step_fifth(2)
    step_fifth(3)
    for k in range(4):
        finish_halo(k)
    for q in range(4):
        finish_sum(q)


def to_hbm(y_vm, dx_vm, dw1_vm, dw2_vm, y_hbm, dx_hbm, dw1_hbm, dw2_hbm, sem):
    copies = [(y_vm, y_hbm), (dx_vm, dx_hbm)]
    for src, dst in ((dw1_vm, dw1_hbm), (dw2_vm, dw2_hbm)):
        for td in range(3):
            copies.append((src.at[pl.ds(td * 6, 6)], dst.at[pl.ds(td * 9, 6)]))
            copies.append((src.at[pl.ds(18 + td * 3, 3)], dst.at[pl.ds(td * 9 + 6, 3)]))
    started = [pltpu.make_async_copy(src, dst, sem.at[n]) for n, (src, dst) in enumerate(copies)]
    for copy in started:
        copy.start()
    for copy in started:
        copy.wait()


def solution(mesh):
    depth_count = mesh.shape["dep"]
    vol_spec = P(None, "dep", "row", None, None)

    def local_step(x_tile, w_conv1, w_conv2, g_tile):
        width = x_tile.shape[3]
        ext = pltpu.VMEM((NB, ND + 2, NH + 2, width, NC), BF16)
        acc = pltpu.VMEM((NB, 6, NH * width, NC), F32)
        trans = pltpu.VMEM((NB * ND * NH, 3 * NC, width), BF16)
        wts = pltpu.VMEM((3, 3, 3, NC, NC), BF16)
        part = pltpu.VMEM((TAPS, NC, NC), F32)
        anywhere = pl.BlockSpec(memory_space=pl.ANY)
        outs = pl.pallas_call(
            functools.partial(kernel, width, depth_count),
            out_shape=(
                pltpu.VMEM(x_tile.shape, BF16),
                pltpu.VMEM(x_tile.shape, BF16),
                pltpu.VMEM((27, NC, NC), F32),
                pltpu.VMEM((27, NC, NC), F32),
            ),
            in_specs=[anywhere] * 4,
            out_specs=(pl.BlockSpec(memory_space=pltpu.VMEM),) * 4,
            scratch_shapes=[
                ext, ext, ext, ext, wts, wts, acc, acc,
                pltpu.VMEM((NB * ND * NH, width, NC), F32),
                trans, trans,
                part, part,
                pltpu.VMEM((2, TAPS, NC // 2, NC), F32),
                pltpu.VMEM((4, TAPS // 2, NC // 16, NC), F32),
                pltpu.VMEM((4, TAPS // 2, NC // 16, NC), F32),
                pltpu.VMEM((4, TAPS, NC // 16, NC), F32),
                pltpu.VMEM((4, TAPS, NC // 16, NC), F32),
                pltpu.VMEM((4, TAPS, NC // 16, NC), F32),
                pltpu.VMEM((4, RING - 1, TQ, NC // 16, NC), F32),
                pltpu.VMEM((4, RING, TQ, NC // 16, NC), F32),
                pltpu.VMEM((4, TAPS, NC // 16, NC), F32),
                pltpu.VMEM((2, NB, 2, width, NC), BF16),
                pltpu.SemaphoreType.DMA((4, 8)),
                pltpu.SemaphoreType.DMA((4, 8)),
                pltpu.SemaphoreType.DMA((4, 3)),
                pltpu.SemaphoreType.DMA((4, 3)),
                pltpu.SemaphoreType.DMA((4, 27)),
                pltpu.SemaphoreType.DMA((4, 27)),
                pltpu.SemaphoreType.DMA((2,)),
                pltpu.SemaphoreType.DMA((2,)),
                pltpu.SemaphoreType.DMA((4,)),
            ],
            compiler_params=pltpu.CompilerParams(collective_id=0, has_side_effects=True, vmem_limit_bytes=56 * 1000 * 1000),
        )(x_tile, w_conv1, w_conv2, g_tile)
        y_tile, dx_tile, dw1, dw2 = pl.pallas_call(
            to_hbm,
            out_shape=(
                jax.ShapeDtypeStruct(x_tile.shape, BF16),
                jax.ShapeDtypeStruct(x_tile.shape, BF16),
                jax.ShapeDtypeStruct((27, NC, NC), F32),
                jax.ShapeDtypeStruct((27, NC, NC), F32),
            ),
            in_specs=[pl.BlockSpec(memory_space=pltpu.VMEM)] * 4,
            out_specs=(anywhere,) * 4,
            scratch_shapes=[pltpu.SemaphoreType.DMA((14,))],
            compiler_params=pltpu.CompilerParams(vmem_limit_bytes=4 * 1000 * 1000),
        )(*outs)
        shape = w_conv1.shape
        return (y_tile, dx_tile, dw1.reshape(shape), dw2.reshape(shape))

    return jax.shard_map(local_step, mesh=mesh, in_specs=(vol_spec, P(), P(), vol_spec), out_specs=(vol_spec, vol_spec, P(), P()), check_vma=False)
```

```python
import functools
import math

import jax
import jax.numpy as jnp
from jax import lax
from jax.experimental import pallas as pl
from jax.experimental.pallas import tpu as pltpu
from jax.sharding import PartitionSpec as P

MESH = pl.DeviceIdType.MESH
F32 = jnp.float32
BF16 = jnp.bfloat16
S2PI = math.sqrt(2.0 / math.pi)
C3 = 0.044715

NB, ND, NH, NC = 2, 2, 4, 128
RING = 4
TAPS = 28
TQ = TAPS // RING
OFFS = (1, 2, 3)
TAIL, TAIL_ORDER = 18, (0, 2, 1)
FAR_FIRST = (2, 1, 3)


def kernel(width, depth_count,
           x_hbm, w1_hbm, w2_hbm, g_hbm,
           y_out, dx_out, dw1_out, dw2_out,
           xe, ge, ze, ae, w1, w2, acc1, acc2, dgel, zt, at,
           p2, p1, cr, ra, rb, rl, rr, bz, r2, xb, ds, hold,
           hs_send, hs_recv, rs_send, rs_recv, ar_send, ar_recv, hold_send, hold_recv, lsem):
    rows = NH * width
    row = lax.axis_index("row")
    dep = lax.axis_index("dep")
    x = lax.rem(dep, RING)
    y = lax.rem(dep // RING, RING)
    z = dep // (RING * RING)
    other = 1 - row
    exts = (xe, ge, ze, ae)
    edge = (NH - 1) - (NH - 1) * row
    my_pad = (NH + 1) * row

    def ring_dep(axis, off):
        if axis == "x":
            return dep - x + lax.rem(x + off, RING)
        if axis == "y":
            return dep - RING * y + RING * lax.rem(y + off, RING)
        return dep - RING * RING * z + RING * RING * lax.rem(z + off, RING)

    def rdma(src, dst, ssem, rsem, dev):
        return pltpu.make_async_remote_copy(src_ref=src, dst_ref=dst, send_sem=ssem, recv_sem=rsem, device_id=dev, device_id_type=MESH)

    has_below = dep > 0
    has_above = dep < depth_count - 1
    near_above, near_below = x < RING - 1, x > 0

    lines_out = (edge, row, row + 1, row + 2)
    ways = ((True, has_above, has_below, near_above), (False, has_below, has_above, near_below))
    hops = {2: (2, 3), 3: (1, 3)}

    def source(k, up, n):
        d = ND - 1 if up else 0
        if k < 2:
            return (x_hbm, g_hbm)[k].at[:, d, pl.ds(lines_out[n], 1)]
        return exts[k].at[:, d + 1, pl.ds(1 + lines_out[n], 1)]

    def landing(k, up, n):
        return exts[k].at[:, 0 if up else ND + 1, pl.ds(1 + lines_out[n], 1)]

    def face(k, up, n):
        slot = 2 * n + up
        return rdma(source(k, up, n), landing(k, up, n), hs_send.at[k, slot], hs_recv.at[k, slot], (row, dep + (2 * up - 1)))

    def far_hop(k, up, n):
        i = hops[k].index(n)
        return rdma(source(k, up, n), hold.at[k - 2, i], hold_send.at[k - 2, i], hold_recv.at[k - 2, i], (row, dep + RING * (2 * up - 1)))

    def far_land(k, up, n):
        i = hops[k].index(n)
        return rdma(hold.at[k - 2, i], landing(k, up, n), hold_send.at[k - 2, 2 + i], hs_recv.at[k, 2 * n + up], (row, dep - (RING - 1) * (2 * up - 1)))

    def side(k):
        if k < 2:
            src = (x_hbm, g_hbm)[k].at[:, :, pl.ds(edge, 1)]
        else:
            src = exts[k].at[:, pl.ds(1, ND), pl.ds(1 + edge, 1)]
        return rdma(src, exts[k].at[:, pl.ds(1, ND), pl.ds(my_pad, 1)], rs_send.at[k, 0], rs_recv.at[k, 0], (other, dep))

    def corner(k, up):
        at_face = exts[k].at[:, 0 if up else ND + 1]
        return rdma(at_face.at[:, pl.ds(1 + edge, 1)], at_face.at[:, pl.ds(my_pad, 1)], rs_send.at[k, 1 + up], rs_recv.at[k, 1 + up], (other, dep))

    relays = ((x == RING - 1) & (dep >= RING), (x == 0) & (dep < depth_count - RING))

    def each_face(k, do, which):
        for n in which:
            far_way = n in hops.get(k, ())
            for up, has, _, near in ways:
                @pl.when(near if far_way else has)
                def _():
                    do(face(k, up, n))

                if far_way:
                    @pl.when(has & jnp.logical_not(near))
                    def _():
                        do(far_hop(k, up, n))

    def start(copy):
        copy.start()

    def sent(copy):
        copy.wait_send()

    def relay_far(k, which):
        for (up, *_), cond in zip(ways, relays):
            @pl.when(cond)
            def _():
                for n in which:
                    far_hop(k, up, n).wait_recv()
                    far_land(k, up, n).start()

    def pass_corners(k):
        for up, _, comes, *_ in ways:
            @pl.when(comes)
            def _():
                face(k, up, 0).wait_recv()
                corner(k, up).start()

    def take_faces(k):
        for up, _, comes, *_ in ways:
            @pl.when(comes)
            def _():
                corner(k, up).wait_recv()
                for n in OFFS:
                    face(k, up, n).wait_recv()

    def finish_halo(k):
        side(k).wait_send()
        each_face(k, sent, range(NH))
        for (up, *_), cond in zip(ways, relays):
            @pl.when(cond)
            def _():
                for n in hops.get(k, ()):
                    far_land(k, up, n).wait_send()

        for up, _, comes, *_ in ways:
            @pl.when(comes)
            def _():
                corner(k, up).wait_send()

    barrier = pltpu.get_barrier_semaphore()
    pl.semaphore_signal(barrier, inc=1, device_id=(other, dep), device_id_type=MESH)
    for axis in ("x", "y", "z"):
        for off in range(1, RING):
            pl.semaphore_signal(barrier, inc=1, device_id=(row, ring_dep(axis, off)), device_id_type=MESH)

    for step in (1, depth_count - 1, RING, depth_count - RING):
        pl.semaphore_signal(barrier, inc=1, device_id=(row, lax.rem(dep + step, depth_count)), device_id_type=MESH)

    loads = [
        pltpu.make_async_copy(x_hbm, xe.at[:, pl.ds(1, ND), pl.ds(1, NH)], lsem.at[0]),
        pltpu.make_async_copy(w1_hbm, w1, lsem.at[1]),
        pltpu.make_async_copy(g_hbm, ge.at[:, pl.ds(1, ND), pl.ds(1, NH)], lsem.at[2]),
        pltpu.make_async_copy(w2_hbm, w2, lsem.at[3]),
    ]
    for load in loads:
        load.start()

    pl.semaphore_wait(barrier, 14)

    for k in range(2):
        side(k).start()
        each_face(k, start, range(NH))

    zero_row = jnp.zeros((NB, 1, width, NC), BF16)
    for ext in exts:
        for dd in range(ND + 2):
            ext[:, dd, pl.ds(my_pad, 1)] = zero_row
    zero_face = jnp.zeros((NH + 2, width, NC), BF16)

    @pl.when(dep == 0)
    def _():
        for ext in exts:
            for b in range(NB):
                ext[b, 0] = zero_face

    @pl.when(dep == depth_count - 1)
    def _():
        for ext in exts:
            for b in range(NB):
                ext[b, ND + 1] = zero_face

    p2[TAPS - 1] = jnp.zeros((NC, NC), F32)
    p1[TAPS - 1] = jnp.zeros((NC, NC), F32)

    def lines(ext, b, dd, h0):
        return ext[b, dd, pl.ds(h0, NH)].reshape(rows, NC)

    def tap_block(w, td, th, tw, flip):
        return w[2 - td, 2 - th, 2 - tw] if flip else w[td, th, tw]

    def weights(w, cells, flip):
        zero = jnp.zeros((NC, NC), BF16)
        blocks = [[zero if t is None else tap_block(w, *t, flip) for t in line] for line in cells]
        if flip:
            return jnp.concatenate([jnp.concatenate([blocks[k][n] for k in range(len(blocks))], axis=1) for n in range(len(blocks[0]))], axis=0)
        return jnp.concatenate([jnp.concatenate(line, axis=1) for line in blocks], axis=0)

    def mul(lhs, rhs, flip):
        return lax.dot_general(lhs, rhs, (((1,), (1 if flip else 0,)), ((), ())), preferred_element_type=F32)

    def conv_inner(ext, w, acc, flip, b0=0, b1=NB):
        cells = []
        for dd in (1, 2):
            for th in range(3):
                cells.append([(dd, th, 0), (dd, th, 1), (dd - 1, th, 0), (dd - 1, th, 1), (dd, th, 2), (dd - 1, th, 2)])
        order = ((0, 0), (0, 1), (1, 0), (1, 1), (0, 2), (1, 2))

        def one(b, carry):
            lhs = jnp.concatenate([lines(ext, b, dd, th) for dd in (1, 2) for th in range(3)], axis=1)
            for n in range(3):
                out = mul(lhs, weights(w, [line[2 * n:2 * n + 2] for line in cells], flip), flip)
                for j in range(2):
                    d, tw = order[2 * n + j]
                    acc[b, d * 3 + tw] = out[:, j * NC:(j + 1) * NC]
            return carry

        lax.fori_loop(b0, b1, one, 0)

    def conv_outer(ext, w, acc, flip):
        def one(i, carry):
            b, d = i // ND, lax.rem(i, ND)
            td = 2 * d
            lhs = jnp.concatenate([lines(ext, b, 3 * d, th) for th in range(3)], axis=1)
            out = mul(lhs, weights(w, [[(td, th, tw) for tw in range(3)] for th in range(3)], flip), flip)
            for tw in range(3):
                acc[b, d * 3 + tw] += out[:, tw * NC:(tw + 1) * NC]
            return carry

        lax.fori_loop(0, NB * ND, one, 0)

    wpos = lax.broadcasted_iota(jnp.int32, (width, NC), 0)

    def from_left(v):
        return jnp.where(wpos > 0, pltpu.roll(v, 1, 0), 0.0)

    def from_right(v):
        return jnp.where(wpos < width - 1, pltpu.roll(v, width - 1, 0), 0.0)

    def each_row(acc, use):
        def one(j, carry):
            for i in (2 * j, 2 * j + 1):
                b, d, h = i // (ND * NH), lax.rem(i // NH, ND), lax.rem(i, NH)
                at_rows = pl.ds(pl.multiple_of(h * width, width), width)
                total = acc[b, d * 3 + 1, at_rows] + from_left(acc[b, d * 3, at_rows]) + from_right(acc[b, d * 3 + 2, at_rows])
                use(i, b, d, h, total)
            return carry

        lax.fori_loop(0, NB * ND * NH // 2, one, 0)

    def after_conv1(i, b, d, h, total):
        a = total.astype(BF16).astype(F32)
        a2 = a * a
        t = jnp.tanh(S2PI * (a + C3 * (a2 * a)))
        cdf = 0.5 * (1.0 + t)
        gel = a * cdf
        dgel[i] = cdf + (0.5 * a * ((1.0 + t) * (1.0 - t))) * (S2PI * (1.0 + 3.0 * C3 * a2))
        ze[b, 1 + d, 1 + h] = gel.astype(BF16)
        for tw, v in enumerate((from_left(gel), gel, from_right(gel))):
            zt[i, pl.ds(tw * NC, NC)] = v.astype(BF16).T

    def after_conv_g(i, b, d, h, total):
        da = total * dgel[i]
        ae[b, 1 + d, 1 + h] = da.astype(BF16)
        for tw, v in enumerate((from_right(da), da, from_left(da))):
            at[i, pl.ds(tw * NC, NC)] = v.astype(BF16).T

    def after_add(ext, out):
        def use(i, b, d, h, total):
            out[b, d, h] = (total + ext[b, 1 + d, 1 + h].astype(F32)).astype(BF16)
        return use

    def tap_index(td, th):
        return td * 6 + th * 3 if th < 2 else TAIL + 3 * TAIL_ORDER.index(td)

    def weight_grad(own_t, ext, part, swap, which, between):
        def rhs(td, th):
            d0, h0 = (2 - td, 2 - th) if swap else (td, th)
            return jnp.concatenate([lines(ext, b, d + d0, h0) for b in range(NB) for d in range(ND)], axis=0)

        def product(right):
            cut = 3 * NC // 2
            halves = []
            for top in (0, cut):
                lhs = jnp.concatenate([own_t[i, pl.ds(top, cut)] for i in range(NB * ND * NH)], axis=1)
                halves.append(jnp.dot(lhs, right, preferred_element_type=F32))
            return jnp.concatenate(halves, axis=0)

        def put(out, n, td, th):
            for tw in range(3):
                blk = out[tw * NC:(tw + 1) * NC, n * NC:(n + 1) * NC]
                part[tap_index(td, th) + tw] = blk if swap else blk.T

        groups = [((td, 0), (td, 1)) for td in range(3)] + [((0, 2), (2, 2)), ((1, 2),)]
        for k in which:
            taps = groups[k]
            out = product(jnp.concatenate([rhs(*t) for t in taps], axis=1))
            for n, t in enumerate(taps):
                put(out, n, *t)
            between(k)

    half, piece = NC // 2, NC // 16
    axes = (("y", "z"), ("z", "y"))
    coord = {"x": x, "y": y, "z": z}
    parts = (p2, p1)
    outs = (dw2_out, dw1_out)
    low, high = pl.ds(0, TAPS // 2), pl.ds(TAPS // 2, TAPS // 2)
    high27 = pl.ds(TAPS // 2, TAPS // 2 - 1)

    def sems(q, n):
        return ar_send.at[q, n], ar_recv.at[q, n]

    def turn(c, off):
        return lax.rem(c + off, RING)

    def chunk(q, off):
        c = turn(coord[axes[q % 2][0]], off)
        return pl.ds(pl.multiple_of(row * half + (q % 2) * (half // 2) + c * piece, piece), piece)

    def pair_copy(s, n):
        theirs = pl.ds(pl.multiple_of(other * half, half), half)
        taps = (pl.ds(0, TAIL), pl.ds(TAIL, 6), pl.ds(TAIL + 6, 4))[n]
        return rdma(parts[s].at[taps, theirs], cr.at[s, taps], *sems(s, 26 + n), (other, dep))

    def scatter_copy(q, n):
        part = parts[q // 2]
        nxt, prv = (row, ring_dep(axes[q % 2][0], 1)), (row, ring_dep(axes[q % 2][0], RING - 1))
        src, dst, dev = (
            (part.at[low, chunk(q, 2)], ra.at[q], nxt),
            (part.at[high, chunk(q, 2)], rb.at[q], prv),
            (part.at[high, chunk(q, 1)], rl.at[q, high], nxt),
            (part.at[low, chunk(q, 3)], rr.at[q, low], prv),
            (ra.at[q], rl.at[q, low], nxt),
            (rb.at[q], rr.at[q, high], prv),
        )[n]
        return rdma(src, dst, *sems(q, n), dev)

    def second_copy(q, off):
        axis = axes[q % 2][1]
        j = turn(coord[axis], off)
        return rdma(bz.at[q, pl.ds(j * TQ, TQ)], r2.at[q, off - 1], *sems(q, 5 + off), (row, ring_dep(axis, off)))

    def third_copy(q, off, slot):
        return rdma(xb.at[q, slot], xb.at[q, slot], *sems(q, 8 + off), (row, ring_dep("x", off)))

    def fourth_copy(q, off, j):
        return rdma(ds.at[q, pl.ds(j * TQ, TQ)], ds.at[q, pl.ds(j * TQ, TQ)], *sems(q, 11 + off), (row, ring_dep(axes[q % 2][1], off)))

    def gather_copy(q, n):
        out = outs[q // 2]
        nxt, prv = (row, ring_dep(axes[q % 2][0], 1)), (row, ring_dep(axes[q % 2][0], RING - 1))
        taps, off, dev = (
            (low, 0, nxt),
            (high27, 0, prv),
            (high27, 0, nxt),
            (low, 0, prv),
            (low, 3, nxt),
            (high27, 1, prv),
        )[n]
        src = ds.at[q, taps] if n < 4 else out.at[taps, chunk(q, off)]
        return rdma(src, out.at[taps, chunk(q, off)], *sems(q, 15 + n), dev)

    def out_copy(q, n):
        out = outs[q // 2]
        taps, off = ((pl.ds(0, 27), 0), (pl.ds(0, 27), 3), (pl.ds(0, 27), 1), (low, 2), (high27, 2))[n]
        src = ds.at[q, taps] if n == 0 else out.at[taps, chunk(q, off)]
        return rdma(src, out.at[taps, chunk(q, off)], *sems(q, 21 + n), (other, dep))

    my_half = pl.ds(pl.multiple_of(row * half, half), half)

    def both(step, q):
        step(q)
        step(q + 1)

    def step_pair(s):
        for n in range(3):
            pair_copy(s, n).wait_recv()

        def add(t, carry):
            parts[s][t, my_half] += cr[s, t]
            return carry

        lax.fori_loop(0, TAPS, add, 0)
        for n in range(4):
            for u in range(2):
                scatter_copy(2 * s + u, n).start()

    def step_relay(q):
        part = parts[q // 2]
        to_next, to_prev = chunk(q, 1), chunk(q, 3)
        scatter_copy(q, 0).wait_recv()
        ra[q] += part[low, to_next]
        scatter_copy(q, 4).start()
        scatter_copy(q, 1).wait_recv()
        rb[q] += part[high, to_prev]
        scatter_copy(q, 5).start()

    def step_first(q):
        for n in range(2, 6):
            scatter_copy(q, n).wait_recv()
        bz[q] = parts[q // 2][:, chunk(q, 0)] + (rl[q] + rr[q])
        for off in FAR_FIRST:
            second_copy(q, off).start()

    def step_second(q):
        for off in OFFS:
            second_copy(q, off).wait_recv()
        c = coord[axes[q % 2][1]]
        xb[q, x] = (bz[q, pl.ds(c * TQ, TQ)] + r2[q, 0]) + (r2[q, 1] + r2[q, 2])
        for off in FAR_FIRST:
            third_copy(q, off, x).start()

    def step_third(q):
        for off in OFFS:
            third_copy(q, off, turn(x, RING - off)).wait_recv()
        c = coord[axes[q % 2][1]]
        ds[q, pl.ds(c * TQ, TQ)] = (xb[q, 0] + xb[q, 1]) + (xb[q, 2] + xb[q, 3])
        for off in FAR_FIRST:
            fourth_copy(q, off, c).start()

    def step_fourth(q):
        c = coord[axes[q % 2][1]]
        for off in OFFS:
            fourth_copy(q, off, turn(c, RING - off)).wait_recv()
        for n in range(4):
            gather_copy(q, n).start()
        out_copy(q, 0).start()
        outs[q // 2][:, chunk(q, 0)] = ds[q, pl.ds(0, 27)]

    def step_forward(q):
        gather_copy(q, 0).wait_recv()
        gather_copy(q, 4).start()
        gather_copy(q, 1).wait_recv()
        gather_copy(q, 5).start()

    def step_fifth(q):
        for n in range(2, 6):
            gather_copy(q, n).wait_recv()
            out_copy(q, n - 1).start()

    def finish_sum(q):
        for n in range(5):
            out_copy(q, n).wait()
        for n in range(6):
            scatter_copy(q, n).wait_send()
            gather_copy(q, n).wait_send()
        for off in OFFS:
            second_copy(q, off).wait_send()
            third_copy(q, off, x).wait_send()
            fourth_copy(q, off, coord[axes[q % 2][1]]).wait_send()

    def after_dw2(k):
        if k == 2:
            pair_copy(0, 0).start()
        if k == 3:
            pair_copy(0, 1).start()
            pair_copy(0, 2).start()

    def after_dw1(k):
        if k >= 2:
            pair_copy(1, k - 2).start()
        if k == 2:
            both(step_relay, 0)

    loads[0].wait()
    loads[1].wait()
    side(0).wait_recv()
    conv_inner(xe, w1, acc1, False)
    loads[2].wait()
    loads[3].wait()
    side(1).wait_recv()
    conv_inner(ge, w2, acc2, True)
    pass_corners(0)
    take_faces(0)
    conv_outer(xe, w1, acc1, False)
    each_row(acc1, after_conv1)
    side(2).start()
    each_face(2, start, range(NH))
    pass_corners(1)
    side(2).wait_recv()
    conv_inner(ze, w2, acc1, False)
    weight_grad(zt, ge, p2, True, (1, 4), after_dw2)
    take_faces(1)
    weight_grad(zt, ge, p2, True, (0, 2, 3), after_dw2)
    relay_far(2, hops[2])
    conv_outer(ge, w2, acc2, True)
    step_pair(0)
    each_row(acc2, after_conv_g)
    side(3).start()
    each_face(3, start, range(2))
    weight_grad(at, xe, p1, False, range(5), after_dw1)
    pass_corners(2)
    step_pair(1)
    relay_far(3, (1,))
    both(step_first, 0)
    take_faces(2)
    conv_outer(ze, w2, acc1, False)
    both(step_relay, 2)
    side(3).wait_recv()
    conv_inner(ae, w1, acc2, True, 0, 1)
    both(step_second, 0)
    each_face(3, start, (2, 3))
    each_row(acc1, after_add(xe, y_out))
    both(step_first, 2)
    both(step_third, 0)
    pass_corners(3)
    conv_inner(ae, w1, acc2, True, 1, 2)
    both(step_second, 2)
    relay_far(3, (3,))
    both(step_fourth, 0)
    both(step_third, 2)
    both(step_forward, 0)
    both(step_fourth, 2)
    take_faces(3)
    conv_outer(ae, w1, acc2, True)
    each_row(acc2, after_add(ge, dx_out))
    both(step_forward, 2)
    both(step_fifth, 0)
    both(step_fifth, 2)
    for k in range(4):
        finish_halo(k)
    for q in range(4):
        finish_sum(q)
    for s in range(2):
        for n in range(3):
            pair_copy(s, n).wait_send()


def to_hbm(y_vm, dx_vm, dw1_vm, dw2_vm, y_hbm, dx_hbm, dw1_hbm, dw2_hbm, sem):
    copies = [(y_vm, y_hbm), (dx_vm, dx_hbm)]
    for src, dst in ((dw1_vm, dw1_hbm), (dw2_vm, dw2_hbm)):
        for td in range(3):
            copies.append((src.at[pl.ds(td * 6, 6)], dst.at[pl.ds(td * 9, 6)]))
            copies.append((src.at[pl.ds(TAIL + 3 * TAIL_ORDER.index(td), 3)], dst.at[pl.ds(td * 9 + 6, 3)]))
    started = [pltpu.make_async_copy(src, dst, sem.at[n]) for n, (src, dst) in enumerate(copies)]
    for copy in started:
        copy.start()
    for copy in started:
        copy.wait()


def solution(mesh):
    depth_count = mesh.shape["dep"]
    vol_spec = P(None, "dep", "row", None, None)

    def local_step(x_tile, w_conv1, w_conv2, g_tile):
        width = x_tile.shape[3]
        ext = pltpu.VMEM((NB, ND + 2, NH + 2, width, NC), BF16)
        acc = pltpu.VMEM((NB, 6, NH * width, NC), F32)
        trans = pltpu.VMEM((NB * ND * NH, 3 * NC, width), BF16)
        wts = pltpu.VMEM((3, 3, 3, NC, NC), BF16)
        part = pltpu.VMEM((TAPS, NC, NC), F32)
        anywhere = pl.BlockSpec(memory_space=pl.ANY)
        outs = pl.pallas_call(
            functools.partial(kernel, width, depth_count),
            out_shape=(
                pltpu.VMEM(x_tile.shape, BF16),
                pltpu.VMEM(x_tile.shape, BF16),
                pltpu.VMEM((27, NC, NC), F32),
                pltpu.VMEM((27, NC, NC), F32),
            ),
            in_specs=[anywhere] * 4,
            out_specs=(pl.BlockSpec(memory_space=pltpu.VMEM),) * 4,
            scratch_shapes=[
                ext, ext, ext, ext, wts, wts, acc, acc,
                pltpu.VMEM((NB * ND * NH, width, NC), F32),
                trans, trans,
                part, part,
                pltpu.VMEM((2, TAPS, NC // 2, NC), F32),
                pltpu.VMEM((4, TAPS // 2, NC // 16, NC), F32),
                pltpu.VMEM((4, TAPS // 2, NC // 16, NC), F32),
                pltpu.VMEM((4, TAPS, NC // 16, NC), F32),
                pltpu.VMEM((4, TAPS, NC // 16, NC), F32),
                pltpu.VMEM((4, TAPS, NC // 16, NC), F32),
                pltpu.VMEM((4, RING - 1, TQ, NC // 16, NC), F32),
                pltpu.VMEM((4, RING, TQ, NC // 16, NC), F32),
                pltpu.VMEM((4, TAPS, NC // 16, NC), F32),
                pltpu.VMEM((2, 2, NB, 1, width, NC), BF16),
                pltpu.SemaphoreType.DMA((4, 8)),
                pltpu.SemaphoreType.DMA((4, 8)),
                pltpu.SemaphoreType.DMA((4, 3)),
                pltpu.SemaphoreType.DMA((4, 3)),
                pltpu.SemaphoreType.DMA((4, 29)),
                pltpu.SemaphoreType.DMA((4, 29)),
                pltpu.SemaphoreType.DMA((2, 4)),
                pltpu.SemaphoreType.DMA((2, 2)),
                pltpu.SemaphoreType.DMA((4,)),
            ],
            compiler_params=pltpu.CompilerParams(collective_id=0, has_side_effects=True, vmem_limit_bytes=56 * 1000 * 1000),
        )(x_tile, w_conv1, w_conv2, g_tile)
        y_tile, dx_tile, dw1, dw2 = pl.pallas_call(
            to_hbm,
            out_shape=(
                jax.ShapeDtypeStruct(x_tile.shape, BF16),
                jax.ShapeDtypeStruct(x_tile.shape, BF16),
                jax.ShapeDtypeStruct((27, NC, NC), F32),
                jax.ShapeDtypeStruct((27, NC, NC), F32),
            ),
            in_specs=[pl.BlockSpec(memory_space=pltpu.VMEM)] * 4,
            out_specs=(anywhere,) * 4,
            scratch_shapes=[pltpu.SemaphoreType.DMA((14,))],
            compiler_params=pltpu.CompilerParams(vmem_limit_bytes=4 * 1000 * 1000),
        )(*outs)
        shape = w_conv1.shape
        return (y_tile, dx_tile, dw1.reshape(shape), dw2.reshape(shape))

    return jax.shard_map(local_step, mesh=mesh, in_specs=(vol_spec, P(), P(), vol_spec), out_specs=(vol_spec, vol_spec, P(), P()), check_vma=False)
```

```python
import functools
import math

import jax
import jax.numpy as jnp
from jax import lax
from jax.experimental import pallas as pl
from jax.experimental.pallas import tpu as pltpu
from jax.sharding import PartitionSpec as P

MESH = pl.DeviceIdType.MESH
F32 = jnp.float32
BF16 = jnp.bfloat16
S2PI = math.sqrt(2.0 / math.pi)
C3 = 0.044715

NB, ND, NH, NC = 2, 2, 4, 128
RING = 4
TAPS = 28
TQ = TAPS // RING
TAIL, TAIL_ORDER = 18, (0, 2, 1)
FAR_FIRST = (2, 1, 3)


def kernel(width, depth_count,
           x_hbm, w1_hbm, w2_hbm, g_hbm,
           y_out, dx_out, dw1_out, dw2_out,
           xe, ge, ze, ae, w1, w2, acc1, acc2, dgel, zt, at,
           p2, p1, cr, ra, rb, lr, bz, r2, xb, ds, hold,
           hs_send, hs_recv, rs_send, rs_recv, ar_send, ar_recv, hold_send, hold_recv, lsem):
    rows = NH * width
    row = lax.axis_index("row")
    dep = lax.axis_index("dep")
    x = lax.rem(dep, RING)
    y = lax.rem(dep // RING, RING)
    z = dep // (RING * RING)
    other = 1 - row
    exts = (xe, ge, ze, ae)
    edge = (NH - 1) - (NH - 1) * row
    my_pad = (NH + 1) * row

    def ring_dep(axis, off):
        if axis == "x":
            return dep - x + lax.rem(x + off, RING)
        if axis == "y":
            return dep - RING * y + RING * lax.rem(y + off, RING)
        return dep - RING * RING * z + RING * RING * lax.rem(z + off, RING)

    def rdma(src, dst, ssem, rsem, dev):
        return pltpu.make_async_remote_copy(src_ref=src, dst_ref=dst, send_sem=ssem, recv_sem=rsem, device_id=dev, device_id_type=MESH)

    has_below = dep > 0
    has_above = dep < depth_count - 1
    near_above, near_below = x < RING - 1, x > 0

    lines_out = (edge, row, row + 1, row + 2)
    ways = ((True, has_above, has_below, near_above), (False, has_below, has_above, near_below))
    hops = {2: (2, 3), 3: (1, 3)}
    every, early, late = range(NH), range(2), range(2, NH)

    def source(k, up, n):
        d = ND - 1 if up else 0
        if k < 2:
            return (x_hbm, g_hbm)[k].at[:, d, pl.ds(lines_out[n], 1)]
        return exts[k].at[:, d + 1, pl.ds(1 + lines_out[n], 1)]

    def landing(k, up, n):
        return exts[k].at[:, 0 if up else ND + 1, pl.ds(1 + lines_out[n], 1)]

    def face(k, up, n):
        return rdma(source(k, up, n), landing(k, up, n), hs_send.at[k, int(up)], hs_recv.at[k, int(up), min(n, 1)], (row, dep + (2 * up - 1)))

    def rows_of(k, up, count):
        ref = exts[k].at[:, 0, pl.ds(1, count)]
        return rdma(ref, ref, hs_send.at[k, int(up)], hs_recv.at[k, int(up), 1], (row, dep))

    def far_hop(k, up, n):
        i = hops[k].index(n)
        return rdma(source(k, up, n), hold.at[k - 2, i], hold_send.at[k - 2, i], hold_recv.at[k - 2, i], (row, dep + RING * (2 * up - 1)))

    def far_land(k, up, n):
        i = hops[k].index(n)
        return rdma(hold.at[k - 2, i], landing(k, up, n), hold_send.at[k - 2, 2 + i], hs_recv.at[k, int(up), 1], (row, dep - (RING - 1) * (2 * up - 1)))

    def side(k):
        if k < 2:
            src = (x_hbm, g_hbm)[k].at[:, :, pl.ds(edge, 1)]
        else:
            src = exts[k].at[:, pl.ds(1, ND), pl.ds(1 + edge, 1)]
        return rdma(src, exts[k].at[:, pl.ds(1, ND), pl.ds(my_pad, 1)], rs_send.at[k, 0], rs_recv.at[k, 0], (other, dep))

    def corner(k, up):
        at_face = exts[k].at[:, 0 if up else ND + 1]
        return rdma(at_face.at[:, pl.ds(1 + edge, 1)], at_face.at[:, pl.ds(my_pad, 1)], rs_send.at[k, 1 + up], rs_recv.at[k, 1 + up], (other, dep))

    relays = ((x == RING - 1) & (dep >= RING), (x == 0) & (dep < depth_count - RING))

    def each_face(k, do, which, far_which):
        for n in range(NH):
            for up, has, _, near in ways:
                if n in which:
                    @pl.when(near)
                    def _():
                        do(face(k, up, n))

                if n in far_which:
                    @pl.when(has & jnp.logical_not(near))
                    def _():
                        do((far_hop if n in hops.get(k, ()) else face)(k, up, n))

    def start(copy):
        copy.start()

    def relay_far(k, which):
        for (up, *_), cond in zip(ways, relays):
            @pl.when(cond)
            def _():
                for n in which:
                    far_hop(k, up, n).wait_recv()
                    far_land(k, up, n).start()

    def pass_corners(k):
        for up, _, comes, *_ in ways:
            @pl.when(comes)
            def _():
                face(k, up, 0).wait_recv()
                corner(k, up).start()

    def take_faces(k):
        for up, _, comes, *_ in ways:
            @pl.when(comes)
            def _():
                corner(k, up).wait_recv()
                rows_of(k, up, NH - 1).wait_recv()

    def finish_halo(k):
        side(k).wait_send()
        for up, has, _, near in ways:
            @pl.when(near)
            def _():
                rows_of(k, up, NH).wait_send()

            @pl.when(has & jnp.logical_not(near))
            def _():
                rows_of(k, up, NH - len(hops.get(k, ()))).wait_send()
                for n in hops.get(k, ()):
                    far_hop(k, up, n).wait_send()

        for (up, *_), cond in zip(ways, relays):
            @pl.when(cond)
            def _():
                for n in hops.get(k, ()):
                    far_land(k, up, n).wait_send()

        for up, _, comes, *_ in ways:
            @pl.when(comes)
            def _():
                corner(k, up).wait_send()

    barrier = pltpu.get_barrier_semaphore()
    pl.semaphore_signal(barrier, inc=1, device_id=(other, dep), device_id_type=MESH)
    for axis in ("x", "y", "z"):
        for off in range(1, RING):
            pl.semaphore_signal(barrier, inc=1, device_id=(row, ring_dep(axis, off)), device_id_type=MESH)

    for step in (1, depth_count - 1, RING, depth_count - RING):
        pl.semaphore_signal(barrier, inc=1, device_id=(row, lax.rem(dep + step, depth_count)), device_id_type=MESH)

    loads = [
        pltpu.make_async_copy(x_hbm, xe.at[:, pl.ds(1, ND), pl.ds(1, NH)], lsem.at[0]),
        pltpu.make_async_copy(w1_hbm, w1, lsem.at[1]),
        pltpu.make_async_copy(g_hbm, ge.at[:, pl.ds(1, ND), pl.ds(1, NH)], lsem.at[2]),
        pltpu.make_async_copy(w2_hbm, w2, lsem.at[3]),
    ]
    for load in loads:
        load.start()

    pl.semaphore_wait(barrier, 14)

    for k in range(2):
        side(k).start()
        each_face(k, start, every, every)

    zero_row = jnp.zeros((NB, 1, width, NC), BF16)
    for ext in exts:
        for dd in range(ND + 2):
            ext[:, dd, pl.ds(my_pad, 1)] = zero_row
    zero_face = jnp.zeros((NH + 2, width, NC), BF16)

    @pl.when(dep == 0)
    def _():
        for ext in exts:
            for b in range(NB):
                ext[b, 0] = zero_face

    @pl.when(dep == depth_count - 1)
    def _():
        for ext in exts:
            for b in range(NB):
                ext[b, ND + 1] = zero_face

    p2[TAPS - 1] = jnp.zeros((NC, NC), F32)
    p1[TAPS - 1] = jnp.zeros((NC, NC), F32)

    def lines(ext, b, dd, h0):
        return ext[b, dd, pl.ds(h0, NH)].reshape(rows, NC)

    def tap_block(w, td, th, tw, flip):
        return w[2 - td, 2 - th, 2 - tw] if flip else w[td, th, tw]

    def weights(w, cells, flip):
        zero = jnp.zeros((NC, NC), BF16)
        blocks = [[zero if t is None else tap_block(w, *t, flip) for t in line] for line in cells]
        if flip:
            return jnp.concatenate([jnp.concatenate([blocks[k][n] for k in range(len(blocks))], axis=1) for n in range(len(blocks[0]))], axis=0)
        return jnp.concatenate([jnp.concatenate(line, axis=1) for line in blocks], axis=0)

    def mul(lhs, rhs, flip):
        return lax.dot_general(lhs, rhs, (((1,), (1 if flip else 0,)), ((), ())), preferred_element_type=F32)

    def conv_inner(ext, w, acc, flip, b0=0, b1=NB):
        order = ((0, 0), (0, 1), (1, 0), (1, 1), (0, 2), (1, 2))
        cells = [[(dd - d, th, tw) for d, tw in order] for dd in (1, 2) for th in range(3)]

        def one(b, carry):
            lhs = jnp.concatenate([lines(ext, b, dd, th) for dd in (1, 2) for th in range(3)], axis=1)
            for n in range(3):
                out = mul(lhs, weights(w, [line[2 * n:2 * n + 2] for line in cells], flip), flip)
                for j in range(2):
                    d, tw = order[2 * n + j]
                    acc[b, d * 3 + tw] = out[:, j * NC:(j + 1) * NC]
            return carry

        lax.fori_loop(b0, b1, one, 0)

    def outer_block(ext, w, acc, flip, b, d):
        lhs = jnp.concatenate([lines(ext, b, 3 * d, th) for th in range(3)], axis=1)
        out = mul(lhs, weights(w, [[(2 * d, th, tw) for tw in range(3)] for th in range(3)], flip), flip)
        for tw in range(3):
            acc[b, d * 3 + tw] += out[:, tw * NC:(tw + 1) * NC]

    def conv_outer(ext, w, acc, flip):
        def one(i, carry):
            outer_block(ext, w, acc, flip, i // ND, lax.rem(i, ND))
            return carry

        lax.fori_loop(0, NB * ND, one, 0)

    wpos = lax.broadcasted_iota(jnp.int32, (width, NC), 0)

    def from_left(v):
        return jnp.where(wpos > 0, pltpu.roll(v, 1, 0), 0.0)

    def from_right(v):
        return jnp.where(wpos < width - 1, pltpu.roll(v, width - 1, 0), 0.0)

    def one_row(acc, use, b, d, h):
        at_rows = pl.ds(h * width, width)
        total = acc[b, d * 3 + 1, at_rows] + from_left(acc[b, d * 3, at_rows]) + from_right(acc[b, d * 3 + 2, at_rows])
        use((b * ND + d) * NH + h, b, d, h, total)

    def each_row(acc, use):
        def one(j, carry):
            for h in range(NH):
                one_row(acc, use, j // ND, lax.rem(j, ND), h)
            return carry

        lax.fori_loop(0, NB * ND, one, 0)

    def conv_outer_rows(ext, w, acc, flip, use):
        blocks = [(b, d) for b in range(NB) for d in range(ND)]
        for now, done in zip(blocks + [()], [()] + blocks):
            if now:
                outer_block(ext, w, acc, flip, *now)
            if done:
                for h in range(NH):
                    one_row(acc, use, *done, h)

    def after_conv1(i, b, d, h, total):
        a = total.astype(BF16).astype(F32)
        a2 = a * a
        t = jnp.tanh(S2PI * (a + C3 * (a2 * a)))
        cdf = 0.5 * (1.0 + t)
        gel = a * cdf
        dgel[i] = cdf + (0.5 * a * ((1.0 + t) * (1.0 - t))) * (S2PI * (1.0 + 3.0 * C3 * a2))
        ze[b, 1 + d, 1 + h] = gel.astype(BF16)
        for tw, v in enumerate((from_left(gel), gel, from_right(gel))):
            zt[i, pl.ds(tw * NC, NC)] = v.astype(BF16).T

    def after_conv_g(i, b, d, h, total):
        da = total * dgel[i]
        ae[b, 1 + d, 1 + h] = da.astype(BF16)
        for tw, v in enumerate((from_right(da), da, from_left(da))):
            at[i, pl.ds(tw * NC, NC)] = v.astype(BF16).T

    def after_add(ext, out):
        def use(i, b, d, h, total):
            out[b, d, h] = (total + ext[b, 1 + d, 1 + h].astype(F32)).astype(BF16)
        return use

    def tap_index(td, th):
        return td * 6 + th * 3 if th < 2 else TAIL + 3 * TAIL_ORDER.index(td)

    def weight_grad(own_t, ext, part, swap, which, between):
        def rhs(td, th):
            d0, h0 = (2 - td, 2 - th) if swap else (td, th)
            return jnp.concatenate([lines(ext, b, d + d0, h0) for b in range(NB) for d in range(ND)], axis=0)

        def product(right):
            cut = 3 * NC // 2
            halves = []
            for top in (0, cut):
                lhs = jnp.concatenate([own_t[i, pl.ds(top, cut)] for i in range(NB * ND * NH)], axis=1)
                halves.append(jnp.dot(lhs, right, preferred_element_type=F32))
            return jnp.concatenate(halves, axis=0)

        def put(out, n, td, th):
            for tw in range(3):
                blk = out[tw * NC:(tw + 1) * NC, n * NC:(n + 1) * NC]
                part[tap_index(td, th) + tw] = blk if swap else blk.T

        groups = [((td, 0), (td, 1)) for td in range(3)] + [((0, 2), (2, 2)), ((1, 2),)]
        for k in which:
            taps = groups[k]
            out = product(jnp.concatenate([rhs(*t) for t in taps], axis=1))
            for n, t in enumerate(taps):
                put(out, n, *t)
            between(k)

    half, piece = NC // 2, NC // 16
    axes = (("y", "z"), ("z", "y"))
    coord = {"x": x, "y": y, "z": z}
    parts = (p2, p1)
    outs = (dw2_out, dw1_out)
    low, high = pl.ds(0, TAPS // 2), pl.ds(TAPS // 2, TAPS // 2)
    high27 = pl.ds(TAPS // 2, TAPS // 2 - 1)

    def sems(q, n):
        return ar_send.at[q, n], ar_recv.at[q, n]

    def turn(c, off):
        return lax.rem(c + off, RING)

    def chunk(q, off):
        c = turn(coord[axes[q % 2][0]], off)
        return pl.ds(pl.multiple_of(row * half + (q % 2) * (half // 2) + c * piece, piece), piece)

    def pair_copy(s, n):
        theirs = pl.ds(pl.multiple_of(other * half, half), half)
        taps = (pl.ds(0, TAIL), pl.ds(TAIL, 6), pl.ds(TAIL + 6, 4))[n]
        return rdma(parts[s].at[taps, theirs], cr.at[s, taps], *sems(s, 10), (other, dep))

    def scatter_copy(q, n):
        part = parts[q // 2]
        nxt, prv = (row, ring_dep(axes[q % 2][0], 1)), (row, ring_dep(axes[q % 2][0], RING - 1))
        src, dst, dev = (
            (part.at[low, chunk(q, 2)], ra.at[q], nxt),
            (part.at[high, chunk(q, 2)], rb.at[q], prv),
            (part.at[high, chunk(q, 1)], lr.at[q, 0, high], nxt),
            (part.at[low, chunk(q, 3)], lr.at[q, 1, low], prv),
            (ra.at[q], lr.at[q, 0, low], nxt),
            (rb.at[q], lr.at[q, 1, high], prv),
        )[n]
        return rdma(src, dst, *sems(q, min(n, 2)), dev)

    def second_copy(q, off):
        axis = axes[q % 2][1]
        j = turn(coord[axis], off)
        return rdma(bz.at[q, pl.ds(j * TQ, TQ)], r2.at[q, off - 1], *sems(q, 3), (row, ring_dep(axis, off)))

    def third_copy(q, off, slot):
        return rdma(xb.at[q, slot], xb.at[q, slot], *sems(q, 4), (row, ring_dep("x", off)))

    def fourth_copy(q, off, j):
        return rdma(ds.at[q, pl.ds(j * TQ, TQ)], ds.at[q, pl.ds(j * TQ, TQ)], *sems(q, 5), (row, ring_dep(axes[q % 2][1], off)))

    def gather_copy(q, n):
        out = outs[q // 2]
        nxt, prv = (row, ring_dep(axes[q % 2][0], 1)), (row, ring_dep(axes[q % 2][0], RING - 1))
        taps, off, dev = (
            (low, 0, nxt),
            (high27, 0, prv),
            (high27, 0, nxt),
            (low, 0, prv),
            (low, 3, nxt),
            (high27, 1, prv),
        )[n]
        src = ds.at[q, taps] if n < 4 else out.at[taps, chunk(q, off)]
        return rdma(src, out.at[taps, chunk(q, off)], *sems(q, 6 + min(n, 2)), dev)

    def out_copy(q, n):
        out = outs[q // 2]
        taps, off = ((low, 3), (high27, 1), (high27, 3), (low, 1), (low, 2), (high27, 2), (pl.ds(0, 27), 0))[n]
        src = ds.at[q, taps] if off == 0 else out.at[taps, chunk(q, off)]
        return rdma(src, out.at[taps, chunk(q, off)], *sems(q, 9), (other, dep))

    def group(q, n):
        ref = {
            0: ra.at[q], 1: rb.at[q], 2: lr.at[q], 3: r2.at[q], 4: r2.at[q], 5: r2.at[q],
            6: ra.at[q], 7: ra.at[q, pl.ds(1, TAPS // 2 - 1)],
            8: outs[0].at[:, pl.ds(0, 2 * piece)], 9: outs[0].at[:, pl.ds(0, 4 * piece)], 10: cr.at[0],
        }[n]
        return rdma(ref, ref, *sems(q, n), (other, dep))

    my_half = pl.ds(pl.multiple_of(row * half, half), half)

    dw2_q, dw1_q = 0, 2

    def both(step, q):
        step(q)
        step(q + 1)

    def step_pair(s):
        group(s, 10).wait_recv()

        def add(t, carry):
            parts[s][t, my_half] += cr[s, t]
            return carry

        lax.fori_loop(0, TAPS, add, 0)
        for n in range(4):
            for u in range(2):
                scatter_copy(2 * s + u, n).start()

    def step_relay(q):
        part = parts[q // 2]
        to_next, to_prev = chunk(q, 1), chunk(q, 3)
        scatter_copy(q, 0).wait_recv()
        ra[q] += part[low, to_next]
        scatter_copy(q, 4).start()
        scatter_copy(q, 1).wait_recv()
        rb[q] += part[high, to_prev]
        scatter_copy(q, 5).start()

    def step_first(q):
        group(q, 2).wait_recv()
        bz[q] = parts[q // 2][:, chunk(q, 0)] + (lr[q, 0] + lr[q, 1])
        for off in FAR_FIRST:
            second_copy(q, off).start()

    def step_second(q):
        group(q, 3).wait_recv()
        c = coord[axes[q % 2][1]]
        xb[q, x] = (bz[q, pl.ds(c * TQ, TQ)] + r2[q, 0]) + (r2[q, 1] + r2[q, 2])
        for off in FAR_FIRST:
            third_copy(q, off, x).start()

    def step_third(q):
        group(q, 4).wait_recv()
        c = coord[axes[q % 2][1]]
        ds[q, pl.ds(c * TQ, TQ)] = (xb[q, 0] + xb[q, 1]) + (xb[q, 2] + xb[q, 3])
        for off in FAR_FIRST:
            fourth_copy(q, off, c).start()

    def step_fourth(q):
        group(q, 5).wait_recv()
        for n in range(4):
            gather_copy(q, n).start()
        out_copy(q, 6).start()
        outs[q // 2][:, chunk(q, 0)] = ds[q, pl.ds(0, 27)]

    def step_forward(q):
        for n in range(2):
            gather_copy(q, n).wait_recv()
            gather_copy(q, 4 + n).start()
            out_copy(q, n).start()

    def step_fifth(q):
        group(q, 8).wait_recv()
        for n in range(2, 6):
            out_copy(q, n).start()

    def finish_sum(q):
        group(q, 9).wait_recv()
        for n in range(10 if q > 1 else 11):
            group(q, n).wait_send()

    def after_dw2(k):
        if k == 2:
            pair_copy(0, 0).start()
        if k == 3:
            pair_copy(0, 1).start()
            pair_copy(0, 2).start()

    def after_dw1(k):
        if k >= 2:
            pair_copy(1, k - 2).start()

    def finish_halos():
        for k in range(4):
            finish_halo(k)

    def finish_sums():
        for q in range(4):
            finish_sum(q)

    loads[0].wait()
    loads[1].wait()
    side(0).wait_recv()
    conv_inner(xe, w1, acc1, False)
    loads[2].wait()
    loads[3].wait()
    side(1).wait_recv()
    conv_inner(ge, w2, acc2, True)
    pass_corners(0)
    take_faces(0)
    conv_outer_rows(xe, w1, acc1, False, after_conv1)
    side(2).start()
    each_face(2, start, every, every)
    pass_corners(1)
    side(2).wait_recv()
    conv_inner(ze, w2, acc1, False)
    weight_grad(zt, ge, p2, True, (1, 4), after_dw2)
    take_faces(1)
    weight_grad(zt, ge, p2, True, (0, 2, 3), after_dw2)
    relay_far(2, hops[2])
    conv_outer_rows(ge, w2, acc2, True, after_conv_g)
    step_pair(0)
    side(3).start()
    each_face(3, start, early, early)
    weight_grad(at, xe, p1, False, range(5), after_dw1)
    pass_corners(2)
    both(step_relay, dw2_q)
    step_pair(1)
    relay_far(3, (1,))
    side(3).wait_recv()
    conv_inner(ae, w1, acc2, True, 0, 1)
    both(step_first, dw2_q)
    both(step_relay, dw1_q)
    take_faces(2)
    conv_outer(ze, w2, acc1, False)
    both(step_second, dw2_q)
    each_face(3, start, late, late)
    both(step_first, dw1_q)
    each_row(acc1, after_add(xe, y_out))
    both(step_third, dw2_q)
    pass_corners(3)
    both(step_second, dw1_q)
    conv_inner(ae, w1, acc2, True, 1, 2)
    relay_far(3, (3,))
    both(step_fourth, dw2_q)
    both(step_third, dw1_q)
    both(step_forward, dw2_q)
    both(step_fourth, dw1_q)
    take_faces(3)
    conv_outer(ae, w1, acc2, True)
    each_row(acc2, after_add(ge, dx_out))
    both(step_forward, dw1_q)
    both(step_fifth, dw2_q)
    both(step_fifth, dw1_q)
    finish_halos()
    finish_sums()


def to_hbm(y_vm, dx_vm, dw1_vm, dw2_vm, y_hbm, dx_hbm, dw1_hbm, dw2_hbm, sem):
    pairs = ((y_vm, y_hbm), (dx_vm, dx_hbm), (dw1_vm, dw1_hbm), (dw2_vm, dw2_hbm))
    for n, (src, dst) in enumerate(pairs):
        if n < 2:
            pltpu.make_async_copy(src, dst, sem.at[n]).start()
        else:
            for td in range(3):
                pltpu.make_async_copy(src.at[pl.ds(td * 6, 6)], dst.at[pl.ds(td * 9, 6)], sem.at[n]).start()
                tail = TAIL + 3 * TAIL_ORDER.index(td)
                pltpu.make_async_copy(src.at[pl.ds(tail, 3)], dst.at[pl.ds(td * 9 + 6, 3)], sem.at[n]).start()
    for n, (src, dst) in enumerate(pairs):
        pltpu.make_async_copy(src, dst, sem.at[n]).wait()


def solution(mesh):
    depth_count = mesh.shape["dep"]
    vol_spec = P(None, "dep", "row", None, None)

    def local_step(x_tile, w_conv1, w_conv2, g_tile):
        width = x_tile.shape[3]
        ext = pltpu.VMEM((NB, ND + 2, NH + 2, width, NC), BF16)
        acc = pltpu.VMEM((NB, 6, NH * width, NC), F32)
        trans = pltpu.VMEM((NB * ND * NH, 3 * NC, width), BF16)
        wts = pltpu.VMEM((3, 3, 3, NC, NC), BF16)
        part = pltpu.VMEM((TAPS, NC, NC), F32)
        anywhere = pl.BlockSpec(memory_space=pl.ANY)
        outs = pl.pallas_call(
            functools.partial(kernel, width, depth_count),
            out_shape=(
                pltpu.VMEM(x_tile.shape, BF16),
                pltpu.VMEM(x_tile.shape, BF16),
                pltpu.VMEM((27, NC, NC), F32),
                pltpu.VMEM((27, NC, NC), F32),
            ),
            in_specs=[anywhere] * 4,
            out_specs=(pl.BlockSpec(memory_space=pltpu.VMEM),) * 4,
            scratch_shapes=[
                ext, ext, ext, ext, wts, wts, acc, acc,
                pltpu.VMEM((NB * ND * NH, width, NC), F32),
                trans, trans,
                part, part,
                pltpu.VMEM((2, TAPS, NC // 2, NC), F32),
                pltpu.VMEM((4, TAPS // 2, NC // 16, NC), F32),
                pltpu.VMEM((4, TAPS // 2, NC // 16, NC), F32),
                pltpu.VMEM((4, 2, TAPS, NC // 16, NC), F32),
                pltpu.VMEM((4, TAPS, NC // 16, NC), F32),
                pltpu.VMEM((4, RING - 1, TQ, NC // 16, NC), F32),
                pltpu.VMEM((4, RING, TQ, NC // 16, NC), F32),
                pltpu.VMEM((4, TAPS, NC // 16, NC), F32),
                pltpu.VMEM((2, 2, NB, 1, width, NC), BF16),
                pltpu.SemaphoreType.DMA((4, 2)),
                pltpu.SemaphoreType.DMA((4, 2, 2)),
                pltpu.SemaphoreType.DMA((4, 3)),
                pltpu.SemaphoreType.DMA((4, 3)),
                pltpu.SemaphoreType.DMA((4, 11)),
                pltpu.SemaphoreType.DMA((4, 11)),
                pltpu.SemaphoreType.DMA((2, 4)),
                pltpu.SemaphoreType.DMA((2, 2)),
                pltpu.SemaphoreType.DMA((4,)),
            ],
            compiler_params=pltpu.CompilerParams(collective_id=0, has_side_effects=True, vmem_limit_bytes=56 * 1000 * 1000),
        )(x_tile, w_conv1, w_conv2, g_tile)
        y_tile, dx_tile, dw1, dw2 = pl.pallas_call(
            to_hbm,
            out_shape=(
                jax.ShapeDtypeStruct(x_tile.shape, BF16),
                jax.ShapeDtypeStruct(x_tile.shape, BF16),
                jax.ShapeDtypeStruct((27, NC, NC), F32),
                jax.ShapeDtypeStruct((27, NC, NC), F32),
            ),
            in_specs=[pl.BlockSpec(memory_space=pltpu.VMEM)] * 4,
            out_specs=(anywhere,) * 4,
            scratch_shapes=[pltpu.SemaphoreType.DMA((4,))],
            compiler_params=pltpu.CompilerParams(vmem_limit_bytes=4 * 1000 * 1000),
        )(*outs)
        shape = w_conv1.shape
        return (y_tile, dx_tile, dw1.reshape(shape), dw2.reshape(shape))

    return jax.shard_map(local_step, mesh=mesh, in_specs=(vol_spec, P(), P(), vol_spec), out_specs=(vol_spec, vol_spec, P(), P()), check_vma=False)
```

```python
import functools
import math

import jax
import jax.numpy as jnp
from jax import lax
from jax.experimental import pallas as pl
from jax.experimental.pallas import tpu as pltpu
from jax.sharding import PartitionSpec as P

MESH = pl.DeviceIdType.MESH
F32 = jnp.float32
BF16 = jnp.bfloat16
S2PI = math.sqrt(2.0 / math.pi)
C3 = 0.044715

NB, ND, NH, NC = 2, 2, 4, 128
RING = 4
TAPS = 28
TQ = TAPS // RING
TAIL, TAIL_ORDER = 18, (0, 2, 1)
FAR_FIRST = (2, 1, 3)


def kernel(width, depth_count,
           x_hbm, w1_hbm, w2_hbm, g_hbm,
           y_out, dx_out, dw1_out, dw2_out,
           xe, ge, ze, ae, w1, w2, acc1, acc2, dgel, zt, at,
           p2, p1, cr, ra, rb, lr, bz, r2, xb, ds, hold,
           hs_send, hs_recv, rs_send, rs_recv, ar_send, ar_recv, hold_send, hold_recv, lsem):
    rows = NH * width
    row = lax.axis_index("row")
    dep = lax.axis_index("dep")
    x = lax.rem(dep, RING)
    y = lax.rem(dep // RING, RING)
    z = dep // (RING * RING)
    other = 1 - row
    exts = (xe, ge, ze, ae)
    edge = (NH - 1) - (NH - 1) * row
    my_pad = (NH + 1) * row

    def ring_dep(axis, off):
        if axis == "x":
            return dep - x + lax.rem(x + off, RING)
        if axis == "y":
            return dep - RING * y + RING * lax.rem(y + off, RING)
        return dep - RING * RING * z + RING * RING * lax.rem(z + off, RING)

    def rdma(src, dst, ssem, rsem, dev):
        return pltpu.make_async_remote_copy(src_ref=src, dst_ref=dst, send_sem=ssem, recv_sem=rsem, device_id=dev, device_id_type=MESH)

    has_below = dep > 0
    has_above = dep < depth_count - 1
    near_above, near_below = x < RING - 1, x > 0

    lines_out = (edge, row, row + 1, row + 2)
    ways = ((True, has_above, has_below, near_above), (False, has_below, has_above, near_below))
    hops = {2: (2, 3), 3: (1, 3)}
    every, early, late = range(NH), range(2), range(2, NH)

    def source(k, up, n):
        d = ND - 1 if up else 0
        if k < 2:
            return (x_hbm, g_hbm)[k].at[:, d, pl.ds(lines_out[n], 1)]
        return exts[k].at[:, d + 1, pl.ds(1 + lines_out[n], 1)]

    def landing(k, up, n):
        return exts[k].at[:, 0 if up else ND + 1, pl.ds(1 + lines_out[n], 1)]

    def face(k, up, n):
        return rdma(source(k, up, n), landing(k, up, n), hs_send.at[k, int(up)], hs_recv.at[k, int(up), min(n, 1)], (row, dep + (2 * up - 1)))

    def rows_of(k, up, count):
        ref = exts[k].at[:, 0, pl.ds(1, count)]
        return rdma(ref, ref, hs_send.at[k, int(up)], hs_recv.at[k, int(up), 1], (row, dep))

    def far_hop(k, up, n):
        i = hops[k].index(n)
        return rdma(source(k, up, n), hold.at[k - 2, i], hold_send.at[k - 2, i], hold_recv.at[k - 2, i], (row, dep + RING * (2 * up - 1)))

    def far_land(k, up, n):
        i = hops[k].index(n)
        return rdma(hold.at[k - 2, i], landing(k, up, n), hold_send.at[k - 2, 2 + i], hs_recv.at[k, int(up), 1], (row, dep - (RING - 1) * (2 * up - 1)))

    def side(k):
        if k < 2:
            src = (x_hbm, g_hbm)[k].at[:, :, pl.ds(edge, 1)]
        else:
            src = exts[k].at[:, pl.ds(1, ND), pl.ds(1 + edge, 1)]
        return rdma(src, exts[k].at[:, pl.ds(1, ND), pl.ds(my_pad, 1)], rs_send.at[k, 0], rs_recv.at[k, 0], (other, dep))

    def corner(k, up):
        at_face = exts[k].at[:, 0 if up else ND + 1]
        return rdma(at_face.at[:, pl.ds(1 + edge, 1)], at_face.at[:, pl.ds(my_pad, 1)], rs_send.at[k, 1 + up], rs_recv.at[k, 1 + up], (other, dep))

    relays = ((x == RING - 1) & (dep >= RING), (x == 0) & (dep < depth_count - RING))

    def each_face(k, do, which, far_which):
        for n in range(NH):
            for up, has, _, near in ways:
                if n in which:
                    @pl.when(near)
                    def _():
                        do(face(k, up, n))

                if n in far_which:
                    @pl.when(has & jnp.logical_not(near))
                    def _():
                        do((far_hop if n in hops.get(k, ()) else face)(k, up, n))

    def start(copy):
        copy.start()

    def relay_far(k, which):
        for (up, *_), cond in zip(ways, relays):
            @pl.when(cond)
            def _():
                for n in which:
                    far_hop(k, up, n).wait_recv()
                    far_land(k, up, n).start()

    def pass_corners(k):
        for up, _, comes, *_ in ways:
            @pl.when(comes)
            def _():
                face(k, up, 0).wait_recv()
                corner(k, up).start()

    def take_faces(k):
        for up, _, comes, *_ in ways:
            @pl.when(comes)
            def _():
                corner(k, up).wait_recv()
                rows_of(k, up, NH - 1).wait_recv()

    def finish_halo(k):
        side(k).wait_send()
        for up, has, _, near in ways:
            @pl.when(near)
            def _():
                rows_of(k, up, NH).wait_send()

            @pl.when(has & jnp.logical_not(near))
            def _():
                rows_of(k, up, NH - len(hops.get(k, ()))).wait_send()
                for n in hops.get(k, ()):
                    far_hop(k, up, n).wait_send()

        for (up, *_), cond in zip(ways, relays):
            @pl.when(cond)
            def _():
                for n in hops.get(k, ()):
                    far_land(k, up, n).wait_send()

        for up, _, comes, *_ in ways:
            @pl.when(comes)
            def _():
                corner(k, up).wait_send()

    barrier = pltpu.get_barrier_semaphore()
    pl.semaphore_signal(barrier, inc=1, device_id=(other, dep), device_id_type=MESH)
    for axis in ("x", "y", "z"):
        for off in range(1, RING):
            pl.semaphore_signal(barrier, inc=1, device_id=(row, ring_dep(axis, off)), device_id_type=MESH)

    for step in (1, depth_count - 1, RING, depth_count - RING):
        pl.semaphore_signal(barrier, inc=1, device_id=(row, lax.rem(dep + step, depth_count)), device_id_type=MESH)

    loads = [
        pltpu.make_async_copy(x_hbm, xe.at[:, pl.ds(1, ND), pl.ds(1, NH)], lsem.at[0]),
        pltpu.make_async_copy(w1_hbm, w1, lsem.at[1]),
        pltpu.make_async_copy(g_hbm, ge.at[:, pl.ds(1, ND), pl.ds(1, NH)], lsem.at[2]),
        pltpu.make_async_copy(w2_hbm, w2, lsem.at[3]),
    ]
    for load in loads:
        load.start()

    pl.semaphore_wait(barrier, 14)

    for k in range(2):
        side(k).start()
        each_face(k, start, every, every)

    zero_row = jnp.zeros((NB, 1, width, NC), BF16)
    for ext in exts:
        for dd in range(ND + 2):
            ext[:, dd, pl.ds(my_pad, 1)] = zero_row
    zero_face = jnp.zeros((NH + 2, width, NC), BF16)

    @pl.when(dep == 0)
    def _():
        for ext in exts:
            for b in range(NB):
                ext[b, 0] = zero_face

    @pl.when(dep == depth_count - 1)
    def _():
        for ext in exts:
            for b in range(NB):
                ext[b, ND + 1] = zero_face

    p2[TAPS - 1] = jnp.zeros((NC, NC), F32)
    p1[TAPS - 1] = jnp.zeros((NC, NC), F32)

    def lines(ext, b, dd, h0):
        return ext[b, dd, pl.ds(h0, NH)].reshape(rows, NC)

    def tap_block(w, td, th, tw, flip):
        return w[2 - td, 2 - th, 2 - tw] if flip else w[td, th, tw]

    def weights(w, cells, flip):
        zero = jnp.zeros((NC, NC), BF16)
        blocks = [[zero if t is None else tap_block(w, *t, flip) for t in line] for line in cells]
        if flip:
            return jnp.concatenate([jnp.concatenate([blocks[k][n] for k in range(len(blocks))], axis=1) for n in range(len(blocks[0]))], axis=0)
        return jnp.concatenate([jnp.concatenate(line, axis=1) for line in blocks], axis=0)

    def mul(lhs, rhs, flip):
        return lax.dot_general(lhs, rhs, (((1,), (1 if flip else 0,)), ((), ())), preferred_element_type=F32)

    def conv_inner(ext, w, acc, flip, b0=0, b1=NB):
        order = ((0, 0), (0, 1), (1, 0), (1, 1), (0, 2), (1, 2))
        cells = [[(dd - d, th, tw) for d, tw in order] for dd in (1, 2) for th in range(3)]

        def one(b, carry):
            lhs = jnp.concatenate([lines(ext, b, dd, th) for dd in (1, 2) for th in range(3)], axis=1)
            for n in range(3):
                out = mul(lhs, weights(w, [line[2 * n:2 * n + 2] for line in cells], flip), flip)
                for j in range(2):
                    d, tw = order[2 * n + j]
                    acc[b, d * 3 + tw] = out[:, j * NC:(j + 1) * NC]
            return carry

        lax.fori_loop(b0, b1, one, 0)

    def outer_block(ext, w, acc, flip, b, d):
        lhs = jnp.concatenate([lines(ext, b, 3 * d, th) for th in range(3)], axis=1)
        out = mul(lhs, weights(w, [[(2 * d, th, tw) for tw in range(3)] for th in range(3)], flip), flip)
        for tw in range(3):
            acc[b, d * 3 + tw] += out[:, tw * NC:(tw + 1) * NC]

    def conv_outer(ext, w, acc, flip):
        def one(i, carry):
            outer_block(ext, w, acc, flip, i // ND, lax.rem(i, ND))
            return carry

        lax.fori_loop(0, NB * ND, one, 0)

    wpos = lax.broadcasted_iota(jnp.int32, (width, NC), 0)

    def from_left(v):
        return jnp.where(wpos > 0, pltpu.roll(v, 1, 0), 0.0)

    def from_right(v):
        return jnp.where(wpos < width - 1, pltpu.roll(v, width - 1, 0), 0.0)

    def one_row(acc, use, b, d, h):
        at_rows = pl.ds(h * width, width)
        total = acc[b, d * 3 + 1, at_rows] + from_left(acc[b, d * 3, at_rows]) + from_right(acc[b, d * 3 + 2, at_rows])
        use((b * ND + d) * NH + h, b, d, h, total)

    def each_row(acc, use):
        def one(j, carry):
            for h in range(NH):
                one_row(acc, use, j // ND, lax.rem(j, ND), h)
            return carry

        lax.fori_loop(0, NB * ND, one, 0)

    def conv_outer_rows(ext, w, acc, flip, use):
        blocks = [(b, d) for b in range(NB) for d in range(ND)]
        for now, done in zip(blocks + [()], [()] + blocks):
            if now:
                outer_block(ext, w, acc, flip, *now)
            if done:
                for h in range(NH):
                    one_row(acc, use, *done, h)

    def after_conv1(i, b, d, h, total):
        a = total.astype(BF16).astype(F32)
        a2 = a * a
        t = jnp.tanh(S2PI * (a + C3 * (a2 * a)))
        cdf = 0.5 * (1.0 + t)
        gel = a * cdf
        dgel[i] = cdf + (0.5 * a * ((1.0 + t) * (1.0 - t))) * (S2PI * (1.0 + 3.0 * C3 * a2))
        ze[b, 1 + d, 1 + h] = gel.astype(BF16)
        for tw, v in enumerate((from_left(gel), gel, from_right(gel))):
            zt[i, pl.ds(tw * NC, NC)] = v.astype(BF16).T

    def after_conv_g(i, b, d, h, total):
        da = total * dgel[i]
        ae[b, 1 + d, 1 + h] = da.astype(BF16)
        for tw, v in enumerate((from_right(da), da, from_left(da))):
            at[i, pl.ds(tw * NC, NC)] = v.astype(BF16).T

    def after_add(ext, out):
        def use(i, b, d, h, total):
            out[b, d, h] = (total + ext[b, 1 + d, 1 + h].astype(F32)).astype(BF16)
        return use

    def tap_index(td, th):
        return td * 6 + th * 3 if th < 2 else TAIL + 3 * TAIL_ORDER.index(td)

    def weight_grad(own_t, ext, part, swap, groups, between):
        for k, (layers, taps, more) in enumerate(groups):
            blocks = [(b, d) for b in range(NB) for d in layers]

            def rhs(td, th):
                d0, h0 = (2 - td, 2 - th) if swap else (td, th)
                return jnp.concatenate([lines(ext, b, d + d0, h0) for b, d in blocks], axis=0)

            right = jnp.concatenate([rhs(*t) for t in taps], axis=1)
            cut = 3 * NC // 2
            halves = []
            for top in (0, cut):
                lhs = jnp.concatenate([own_t[(b * ND + d) * NH + h, pl.ds(top, cut)] for b, d in blocks for h in range(NH)], axis=1)
                halves.append(jnp.dot(lhs, right, preferred_element_type=F32))
            out = jnp.concatenate(halves, axis=0)
            for n, (td, th) in enumerate(taps):
                for tw in range(3):
                    blk = out[tw * NC:(tw + 1) * NC, n * NC:(n + 1) * NC]
                    to = tap_index(td, th) + tw
                    blk = blk if swap else blk.T
                    part[to] = part[to] + blk if more else blk
            between(k)

    both_layers = tuple(range(ND))
    dw1_groups = [(both_layers, ((td, 0), (td, 1)), False) for td in range(3)] + [(both_layers, ((0, 2), (2, 2)), False), (both_layers, ((1, 2),), False)]

    def plane(td):
        return tuple((td, th) for th in range(3))

    dw2_inner = [dw1_groups[1], dw1_groups[4], ((0,), plane(0), False), ((1,), plane(2), False)]
    dw2_outer = [((1,), plane(0), True), ((0,), plane(2), True)]

    half, piece = NC // 2, NC // 16
    axes = (("y", "z"), ("z", "y"))
    coord = {"x": x, "y": y, "z": z}
    parts = (p2, p1)
    outs = (dw2_out, dw1_out)
    low, high = pl.ds(0, TAPS // 2), pl.ds(TAPS // 2, TAPS // 2)
    high27 = pl.ds(TAPS // 2, TAPS // 2 - 1)

    def sems(q, n):
        return ar_send.at[q, n // 10], ar_recv.at[q, n]

    def turn(c, off):
        return lax.rem(c + off, RING)

    def chunk(q, off):
        c = turn(coord[axes[q % 2][0]], off)
        return pl.ds(pl.multiple_of(row * half + (q % 2) * (half // 2) + c * piece, piece), piece)

    def pair_copy(s, n):
        theirs = pl.ds(pl.multiple_of(other * half, half), half)
        taps = (pl.ds(0, TAIL), pl.ds(TAIL, 6), pl.ds(TAIL + 6, 4))[n]
        return rdma(parts[s].at[taps, theirs], cr.at[s, taps], *sems(s, 10), (other, dep))

    def scatter_copy(q, n):
        part = parts[q // 2]
        nxt, prv = (row, ring_dep(axes[q % 2][0], 1)), (row, ring_dep(axes[q % 2][0], RING - 1))
        src, dst, dev = (
            (part.at[low, chunk(q, 2)], ra.at[q], nxt),
            (part.at[high, chunk(q, 2)], rb.at[q], prv),
            (part.at[high, chunk(q, 1)], lr.at[q, 0, high], nxt),
            (part.at[low, chunk(q, 3)], lr.at[q, 1, low], prv),
            (ra.at[q], lr.at[q, 0, low], nxt),
            (rb.at[q], lr.at[q, 1, high], prv),
        )[n]
        return rdma(src, dst, *sems(q, min(n, 2)), dev)

    def second_copy(q, off):
        axis = axes[q % 2][1]
        j = turn(coord[axis], off)
        return rdma(bz.at[q, pl.ds(j * TQ, TQ)], r2.at[q, off - 1], *sems(q, 3), (row, ring_dep(axis, off)))

    def third_copy(q, off, slot):
        return rdma(xb.at[q, slot], xb.at[q, slot], *sems(q, 4), (row, ring_dep("x", off)))

    def fourth_copy(q, off, j):
        return rdma(ds.at[q, pl.ds(j * TQ, TQ)], ds.at[q, pl.ds(j * TQ, TQ)], *sems(q, 5), (row, ring_dep(axes[q % 2][1], off)))

    def gather_copy(q, n):
        out = outs[q // 2]
        nxt, prv = (row, ring_dep(axes[q % 2][0], 1)), (row, ring_dep(axes[q % 2][0], RING - 1))
        taps, off, dev = (
            (low, 0, nxt),
            (high27, 0, prv),
            (high27, 0, nxt),
            (low, 0, prv),
            (low, 3, nxt),
            (high27, 1, prv),
        )[n]
        src = ds.at[q, taps] if n < 4 else out.at[taps, chunk(q, off)]
        return rdma(src, out.at[taps, chunk(q, off)], *sems(q, 6 + min(n, 2)), dev)

    def out_copy(q, n):
        out = outs[q // 2]
        taps, off = ((low, 3), (high27, 1), (high27, 3), (low, 1), (low, 2), (high27, 2), (pl.ds(0, 27), 0))[n]
        src = ds.at[q, taps] if off == 0 else out.at[taps, chunk(q, off)]
        return rdma(src, out.at[taps, chunk(q, off)], *sems(q, 9), (other, dep))

    def group(q, n):
        bands = [outs[0].at[:, pl.ds(0, k * piece)] for k in (2, 4)]
        refs = [ra.at[q], rb.at[q], lr.at[q]] + [r2.at[q]] * 3 + [ra.at[q], ra.at[q, pl.ds(1, TAPS // 2 - 1)]] + bands + [cr.at[0]]
        ref = refs[n]
        return rdma(ref, ref, *sems(q, n), (other, dep))

    my_half = pl.ds(pl.multiple_of(row * half, half), half)

    dw2_q, dw1_q = 0, 2

    def both(step, q):
        step(q)
        step(q + 1)

    def step_pair(s):
        group(s, 10).wait_recv()

        def add(t, carry):
            parts[s][t, my_half] += cr[s, t]
            return carry

        lax.fori_loop(0, TAPS, add, 0)
        for n in range(4):
            for u in range(2):
                scatter_copy(2 * s + u, n).start()

    def step_relay(q):
        part = parts[q // 2]
        to_next, to_prev = chunk(q, 1), chunk(q, 3)
        scatter_copy(q, 0).wait_recv()
        ra[q] += part[low, to_next]
        scatter_copy(q, 4).start()
        scatter_copy(q, 1).wait_recv()
        rb[q] += part[high, to_prev]
        scatter_copy(q, 5).start()

    def step_first(q):
        group(q, 2).wait_recv()
        bz[q] = parts[q // 2][:, chunk(q, 0)] + (lr[q, 0] + lr[q, 1])
        for off in FAR_FIRST:
            second_copy(q, off).start()

    def step_second(q):
        group(q, 3).wait_recv()
        c = coord[axes[q % 2][1]]
        xb[q, x] = (bz[q, pl.ds(c * TQ, TQ)] + r2[q, 0]) + (r2[q, 1] + r2[q, 2])
        for off in FAR_FIRST:
            third_copy(q, off, x).start()

    def step_third(q):
        group(q, 4).wait_recv()
        c = coord[axes[q % 2][1]]
        ds[q, pl.ds(c * TQ, TQ)] = (xb[q, 0] + xb[q, 1]) + (xb[q, 2] + xb[q, 3])
        for off in FAR_FIRST:
            fourth_copy(q, off, c).start()

    def step_fourth(q):
        group(q, 5).wait_recv()
        for n in range(4):
            gather_copy(q, n).start()
        out_copy(q, 6).start()
        outs[q // 2][:, chunk(q, 0)] = ds[q, pl.ds(0, 27)]

    def step_forward(q):
        for n in range(2):
            gather_copy(q, n).wait_recv()
            gather_copy(q, 4 + n).start()
            out_copy(q, n).start()

    def step_fifth(q):
        group(q, 8).wait_recv()
        for n in range(2, 6):
            out_copy(q, n).start()

    def finish_sum(q):
        group(q, 9).wait_recv()
        all_sent = cr.at[:, :, pl.ds(0, 6 * piece)]
        rdma(all_sent, all_sent, *sems(q, 0), (other, dep)).wait_send()
        if q < 2:
            group(q, 10).wait_send()

    def after_dw2(k):
        if k == 1:
            for n in range(3):
                pair_copy(0, n).start()

    def after_dw1(k):
        if k >= 2:
            pair_copy(1, k - 2).start()

    def finish_halos():
        for k in range(4):
            finish_halo(k)

    def finish_sums():
        for q in range(4):
            finish_sum(q)

    loads[0].wait()
    loads[1].wait()
    side(0).wait_recv()
    conv_inner(xe, w1, acc1, False)
    loads[2].wait()
    loads[3].wait()
    side(1).wait_recv()
    conv_inner(ge, w2, acc2, True)
    pass_corners(0)
    take_faces(0)
    conv_outer_rows(xe, w1, acc1, False, after_conv1)
    side(2).start()
    each_face(2, start, every, every)
    pass_corners(1)
    side(2).wait_recv()
    conv_inner(ze, w2, acc1, False)
    weight_grad(zt, ge, p2, True, dw2_inner, lambda k: None)
    take_faces(1)
    weight_grad(zt, ge, p2, True, dw2_outer, after_dw2)
    relay_far(2, hops[2])
    conv_outer_rows(ge, w2, acc2, True, after_conv_g)
    step_pair(0)
    side(3).start()
    each_face(3, start, early, early)
    weight_grad(at, xe, p1, False, dw1_groups, after_dw1)
    pass_corners(2)
    both(step_relay, dw2_q)
    step_pair(1)
    side(3).wait_recv()
    conv_inner(ae, w1, acc2, True, 0, 1)
    relay_far(3, (1,))
    both(step_first, dw2_q)
    both(step_relay, dw1_q)
    take_faces(2)
    conv_outer(ze, w2, acc1, False)
    both(step_second, dw2_q)
    each_face(3, start, late, ())
    both(step_first, dw1_q)
    each_face(3, start, (), late)
    each_row(acc1, after_add(xe, y_out))
    both(step_third, dw2_q)
    pass_corners(3)
    both(step_second, dw1_q)
    conv_inner(ae, w1, acc2, True, 1, 2)
    relay_far(3, (3,))
    both(step_fourth, dw2_q)
    both(step_third, dw1_q)
    both(step_forward, dw2_q)
    both(step_fourth, dw1_q)
    take_faces(3)
    conv_outer(ae, w1, acc2, True)
    each_row(acc2, after_add(ge, dx_out))
    both(step_forward, dw1_q)
    both(step_fifth, dw2_q)
    both(step_fifth, dw1_q)
    finish_halos()
    finish_sums()


def to_hbm(y_vm, dx_vm, dw1_vm, dw2_vm, y_hbm, dx_hbm, dw1_hbm, dw2_hbm, sem):
    pairs = ((y_vm, y_hbm), (dx_vm, dx_hbm), (dw1_vm, dw1_hbm), (dw2_vm, dw2_hbm))
    for n, (src, dst) in enumerate(pairs):
        if n < 2:
            pltpu.make_async_copy(src, dst, sem.at[n]).start()
        else:
            for td in range(3):
                pltpu.make_async_copy(src.at[pl.ds(td * 6, 6)], dst.at[pl.ds(td * 9, 6)], sem.at[n]).start()
                tail = TAIL + 3 * TAIL_ORDER.index(td)
                pltpu.make_async_copy(src.at[pl.ds(tail, 3)], dst.at[pl.ds(td * 9 + 6, 3)], sem.at[n]).start()
    for n, (src, dst) in enumerate(pairs):
        pltpu.make_async_copy(src, dst, sem.at[n]).wait()


def solution(mesh):
    depth_count = mesh.shape["dep"]
    vol_spec = P(None, "dep", "row", None, None)

    def local_step(x_tile, w_conv1, w_conv2, g_tile):
        width = x_tile.shape[3]
        ext = pltpu.VMEM((NB, ND + 2, NH + 2, width, NC), BF16)
        acc = pltpu.VMEM((NB, 6, NH * width, NC), F32)
        trans = pltpu.VMEM((NB * ND * NH, 3 * NC, width), BF16)
        wts = pltpu.VMEM((3, 3, 3, NC, NC), BF16)
        part = pltpu.VMEM((TAPS, NC, NC), F32)
        anywhere = pl.BlockSpec(memory_space=pl.ANY)
        outs = pl.pallas_call(
            functools.partial(kernel, width, depth_count),
            out_shape=(
                pltpu.VMEM(x_tile.shape, BF16),
                pltpu.VMEM(x_tile.shape, BF16),
                pltpu.VMEM((27, NC, NC), F32),
                pltpu.VMEM((27, NC, NC), F32),
            ),
            in_specs=[anywhere] * 4,
            out_specs=(pl.BlockSpec(memory_space=pltpu.VMEM),) * 4,
            scratch_shapes=[
                ext, ext, ext, ext, wts, wts, acc, acc,
                pltpu.VMEM((NB * ND * NH, width, NC), F32),
                trans, trans,
                part, part,
                pltpu.VMEM((2, TAPS, NC // 2, NC), F32),
                pltpu.VMEM((4, TAPS // 2, NC // 16, NC), F32),
                pltpu.VMEM((4, TAPS // 2, NC // 16, NC), F32),
                pltpu.VMEM((4, 2, TAPS, NC // 16, NC), F32),
                pltpu.VMEM((4, TAPS, NC // 16, NC), F32),
                pltpu.VMEM((4, RING - 1, TQ, NC // 16, NC), F32),
                pltpu.VMEM((4, RING, TQ, NC // 16, NC), F32),
                pltpu.VMEM((4, TAPS, NC // 16, NC), F32),
                pltpu.VMEM((2, 2, NB, 1, width, NC), BF16),
                pltpu.SemaphoreType.DMA((4, 2)),
                pltpu.SemaphoreType.DMA((4, 2, 2)),
                pltpu.SemaphoreType.DMA((4, 3)),
                pltpu.SemaphoreType.DMA((4, 3)),
                pltpu.SemaphoreType.DMA((4, 2)),
                pltpu.SemaphoreType.DMA((4, 11)),
                pltpu.SemaphoreType.DMA((2, 4)),
                pltpu.SemaphoreType.DMA((2, 2)),
                pltpu.SemaphoreType.DMA((4,)),
            ],
            compiler_params=pltpu.CompilerParams(collective_id=0, has_side_effects=True, vmem_limit_bytes=56 * 1000 * 1000),
        )(x_tile, w_conv1, w_conv2, g_tile)
        y_tile, dx_tile, dw1, dw2 = pl.pallas_call(
            to_hbm,
            out_shape=(
                jax.ShapeDtypeStruct(x_tile.shape, BF16),
                jax.ShapeDtypeStruct(x_tile.shape, BF16),
                jax.ShapeDtypeStruct((27, NC, NC), F32),
                jax.ShapeDtypeStruct((27, NC, NC), F32),
            ),
            in_specs=[pl.BlockSpec(memory_space=pltpu.VMEM)] * 4,
            out_specs=(anywhere,) * 4,
            scratch_shapes=[pltpu.SemaphoreType.DMA((4,))],
            compiler_params=pltpu.CompilerParams(vmem_limit_bytes=4 * 1000 * 1000),
        )(*outs)
        shape = w_conv1.shape
        return (y_tile, dx_tile, dw1.reshape(shape), dw2.reshape(shape))

    return jax.shard_map(local_step, mesh=mesh, in_specs=(vol_spec, P(), P(), vol_spec), out_specs=(vol_spec, vol_spec, P(), P()), check_vma=False)
```

```python
import functools
import math

import jax
import jax.numpy as jnp
from jax import lax
from jax.experimental import pallas as pl
from jax.experimental.pallas import tpu as pltpu
from jax.sharding import PartitionSpec as P

MESH = pl.DeviceIdType.MESH
F32 = jnp.float32
BF16 = jnp.bfloat16
S2PI = math.sqrt(2.0 / math.pi)
C3 = 0.044715

NB, ND, NH, NC = 2, 2, 4, 128
RING = 4
TAPS = 28
TQ = TAPS // RING
TAIL, TAIL_ORDER = 18, (0, 2, 1)
FAR_FIRST = (2, 1, 3)


def kernel(width, depth_count,
           x_hbm, w1_hbm, w2_hbm, g_hbm,
           y_out, dx_out, dw1_out, dw2_out,
           xe, ge, ze, ae, w1, w2, acc1, acc2, dgel, zt, at,
           p2, p1, cr, ra, rb, lr, bz, r2, xb, ds, hold,
           hs_send, hs_recv, rs_send, rs_recv, ar_send, ar_recv, hold_send, hold_recv, lsem):
    rows = NH * width
    row = lax.axis_index("row")
    dep = lax.axis_index("dep")
    x = lax.rem(dep, RING)
    y = lax.rem(dep // RING, RING)
    z = dep // (RING * RING)
    other = 1 - row
    exts = (xe, ge, ze, ae)
    edge = (NH - 1) - (NH - 1) * row
    my_pad = (NH + 1) * row

    def ring_dep(axis, off):
        if axis == "x":
            return dep - x + lax.rem(x + off, RING)
        if axis == "y":
            return dep - RING * y + RING * lax.rem(y + off, RING)
        return dep - RING * RING * z + RING * RING * lax.rem(z + off, RING)

    def rdma(src, dst, ssem, rsem, dev):
        return pltpu.make_async_remote_copy(src_ref=src, dst_ref=dst, send_sem=ssem, recv_sem=rsem, device_id=dev, device_id_type=MESH)

    has_below = dep > 0
    has_above = dep < depth_count - 1
    near_above, near_below = x < RING - 1, x > 0

    lines_out = (edge, row, row + 1, row + 2)
    ways = ((True, has_above, has_below, near_above), (False, has_below, has_above, near_below))
    hops = {2: (2, 3), 3: (1, 3)}
    every, early, late = range(NH), range(2), range(2, NH)

    def source(k, up, n):
        d = ND - 1 if up else 0
        if k < 2:
            return (x_hbm, g_hbm)[k].at[:, d, pl.ds(lines_out[n], 1)]
        return exts[k].at[:, d + 1, pl.ds(1 + lines_out[n], 1)]

    def landing(k, up, n):
        return exts[k].at[:, 0 if up else ND + 1, pl.ds(1 + lines_out[n], 1)]

    def face(k, up, n):
        return rdma(source(k, up, n), landing(k, up, n), hs_send.at[k, int(up)], hs_recv.at[k, int(up), min(n, 1)], (row, dep + (2 * up - 1)))

    def rows_of(k, up, count):
        ref = exts[k].at[:, 0, pl.ds(1, count)]
        return rdma(ref, ref, hs_send.at[k, int(up)], hs_recv.at[k, int(up), 1], (row, dep))

    def far_hop(k, up, n):
        i = hops[k].index(n)
        return rdma(source(k, up, n), hold.at[k - 2, i], hold_send.at[k - 2, i], hold_recv.at[k - 2, i], (row, dep + RING * (2 * up - 1)))

    def far_land(k, up, n):
        i = hops[k].index(n)
        return rdma(hold.at[k - 2, i], landing(k, up, n), hold_send.at[k - 2, 2 + i], hs_recv.at[k, int(up), 1], (row, dep - (RING - 1) * (2 * up - 1)))

    def side(k):
        if k < 2:
            src = (x_hbm, g_hbm)[k].at[:, :, pl.ds(edge, 1)]
        else:
            src = exts[k].at[:, pl.ds(1, ND), pl.ds(1 + edge, 1)]
        return rdma(src, exts[k].at[:, pl.ds(1, ND), pl.ds(my_pad, 1)], rs_send.at[k, 0], rs_recv.at[k, 0], (other, dep))

    def corner(k, up):
        at_face = exts[k].at[:, 0 if up else ND + 1]
        return rdma(at_face.at[:, pl.ds(1 + edge, 1)], at_face.at[:, pl.ds(my_pad, 1)], rs_send.at[k, 1 + up], rs_recv.at[k, 1 + up], (other, dep))

    relays = ((x == RING - 1) & (dep >= RING), (x == 0) & (dep < depth_count - RING))

    def each_face(k, do, which, far_which):
        for n in range(NH):
            for up, has, _, near in ways:
                if n in which:
                    @pl.when(near)
                    def _():
                        do(face(k, up, n))

                if n in far_which:
                    @pl.when(has & jnp.logical_not(near))
                    def _():
                        do((far_hop if n in hops.get(k, ()) else face)(k, up, n))

    def start(copy):
        copy.start()

    def relay_far(k, which):
        for (up, *_), cond in zip(ways, relays):
            @pl.when(cond)
            def _():
                for n in which:
                    far_hop(k, up, n).wait_recv()
                    far_land(k, up, n).start()

    def pass_corners(k):
        for up, _, comes, *_ in ways:
            @pl.when(comes)
            def _():
                face(k, up, 0).wait_recv()
                corner(k, up).start()

    def take_faces(k):
        for up, _, comes, *_ in ways:
            @pl.when(comes)
            def _():
                corner(k, up).wait_recv()
                rows_of(k, up, NH - 1).wait_recv()

    def finish_halo(k):
        side(k).wait_send()
        for up, has, _, near in ways:
            @pl.when(near)
            def _():
                rows_of(k, up, NH).wait_send()

            @pl.when(has & jnp.logical_not(near))
            def _():
                rows_of(k, up, NH - len(hops.get(k, ()))).wait_send()
                for n in hops.get(k, ()):
                    far_hop(k, up, n).wait_send()

        for (up, *_), cond in zip(ways, relays):
            @pl.when(cond)
            def _():
                for n in hops.get(k, ()):
                    far_land(k, up, n).wait_send()

        for up, _, comes, *_ in ways:
            @pl.when(comes)
            def _():
                corner(k, up).wait_send()

    barrier = pltpu.get_barrier_semaphore()
    pl.semaphore_signal(barrier, inc=1, device_id=(other, dep), device_id_type=MESH)
    for axis in ("x", "y", "z"):
        for off in range(1, RING):
            pl.semaphore_signal(barrier, inc=1, device_id=(row, ring_dep(axis, off)), device_id_type=MESH)

    for step in (1, depth_count - 1, RING, depth_count - RING):
        pl.semaphore_signal(barrier, inc=1, device_id=(row, lax.rem(dep + step, depth_count)), device_id_type=MESH)

    loads = [
        pltpu.make_async_copy(x_hbm, xe.at[:, pl.ds(1, ND), pl.ds(1, NH)], lsem.at[0]),
        pltpu.make_async_copy(w1_hbm, w1, lsem.at[1]),
        pltpu.make_async_copy(g_hbm, ge.at[:, pl.ds(1, ND), pl.ds(1, NH)], lsem.at[2]),
        pltpu.make_async_copy(w2_hbm, w2, lsem.at[3]),
    ]
    for load in loads:
        load.start()

    pl.semaphore_wait(barrier, 14)

    for k in range(2):
        side(k).start()
        each_face(k, start, every, every)

    zero_row = jnp.zeros((NB, 1, width, NC), BF16)
    for ext in exts:
        for dd in range(ND + 2):
            ext[:, dd, pl.ds(my_pad, 1)] = zero_row
    zero_face = jnp.zeros((NH + 2, width, NC), BF16)

    @pl.when(dep == 0)
    def _():
        for ext in exts:
            for b in range(NB):
                ext[b, 0] = zero_face

    @pl.when(dep == depth_count - 1)
    def _():
        for ext in exts:
            for b in range(NB):
                ext[b, ND + 1] = zero_face

    p2[TAPS - 1] = jnp.zeros((NC, NC), F32)
    p1[TAPS - 1] = jnp.zeros((NC, NC), F32)

    def lines(ext, b, dd, h0):
        return ext[b, dd, pl.ds(h0, NH)].reshape(rows, NC)

    def tap_block(w, td, th, tw, flip):
        return w[2 - td, 2 - th, 2 - tw] if flip else w[td, th, tw]

    def weights(w, cells, flip):
        zero = jnp.zeros((NC, NC), BF16)
        blocks = [[zero if t is None else tap_block(w, *t, flip) for t in line] for line in cells]
        if flip:
            return jnp.concatenate([jnp.concatenate([blocks[k][n] for k in range(len(blocks))], axis=1) for n in range(len(blocks[0]))], axis=0)
        return jnp.concatenate([jnp.concatenate(line, axis=1) for line in blocks], axis=0)

    def mul(lhs, rhs, flip):
        return lax.dot_general(lhs, rhs, (((1,), (1 if flip else 0,)), ((), ())), preferred_element_type=F32)

    def conv_inner(ext, w, acc, flip, b0=0, b1=NB):
        order = ((0, 0), (0, 1), (1, 0), (1, 1), (0, 2), (1, 2))
        cells = [[(dd - d, th, tw) for d, tw in order] for dd in (1, 2) for th in range(3)]

        def one(b, carry):
            lhs = jnp.concatenate([lines(ext, b, dd, th) for dd in (1, 2) for th in range(3)], axis=1)
            for n in range(3):
                out = mul(lhs, weights(w, [line[2 * n:2 * n + 2] for line in cells], flip), flip)
                for j in range(2):
                    d, tw = order[2 * n + j]
                    acc[b, d * 3 + tw] = out[:, j * NC:(j + 1) * NC]
            return carry

        lax.fori_loop(b0, b1, one, 0)

    def outer_block(ext, w, acc, flip, b, d):
        lhs = jnp.concatenate([lines(ext, b, 3 * d, th) for th in range(3)], axis=1)
        out = mul(lhs, weights(w, [[(2 * d, th, tw) for tw in range(3)] for th in range(3)], flip), flip)
        for tw in range(3):
            acc[b, d * 3 + tw] += out[:, tw * NC:(tw + 1) * NC]

    def conv_outer(ext, w, acc, flip):
        def one(i, carry):
            outer_block(ext, w, acc, flip, i // ND, lax.rem(i, ND))
            return carry

        lax.fori_loop(0, NB * ND, one, 0)

    wpos = lax.broadcasted_iota(jnp.int32, (width, NC), 0)

    def from_left(v):
        return jnp.where(wpos > 0, pltpu.roll(v, 1, 0), 0.0)

    def from_right(v):
        return jnp.where(wpos < width - 1, pltpu.roll(v, width - 1, 0), 0.0)

    def one_row(acc, use, b, d, h):
        at_rows = pl.ds(h * width, width)
        total = acc[b, d * 3 + 1, at_rows] + from_left(acc[b, d * 3, at_rows]) + from_right(acc[b, d * 3 + 2, at_rows])
        use((b * ND + d) * NH + h, b, d, h, total)

    def each_row(acc, use):
        def one(j, carry):
            for h in range(NH):
                one_row(acc, use, j // ND, lax.rem(j, ND), h)
            return carry

        lax.fori_loop(0, NB * ND, one, 0)

    def conv_outer_rows(ext, w, acc, flip, use):
        blocks = [(b, d) for b in range(NB) for d in range(ND)]
        for now, done in zip(blocks + [()], [()] + blocks):
            if now:
                outer_block(ext, w, acc, flip, *now)
            if done:
                for h in range(NH):
                    one_row(acc, use, *done, h)

    def after_conv1(i, b, d, h, total):
        a = total.astype(BF16).astype(F32)
        a2 = a * a
        t = jnp.tanh(S2PI * (a + C3 * (a2 * a)))
        cdf = 0.5 * (1.0 + t)
        gel = a * cdf
        dgel[i] = cdf + (0.5 * a * ((1.0 + t) * (1.0 - t))) * (S2PI * (1.0 + 3.0 * C3 * a2))
        ze[b, 1 + d, 1 + h] = gel.astype(BF16)
        for tw, v in enumerate((from_left(gel), gel, from_right(gel))):
            zt[i, pl.ds(tw * NC, NC)] = v.astype(BF16).T

    def after_conv_g(i, b, d, h, total):
        da = total * dgel[i]
        ae[b, 1 + d, 1 + h] = da.astype(BF16)
        for tw, v in enumerate((from_right(da), da, from_left(da))):
            at[i, pl.ds(tw * NC, NC)] = v.astype(BF16).T

    def after_add(ext, out):
        def use(i, b, d, h, total):
            out[b, d, h] = (total + ext[b, 1 + d, 1 + h].astype(F32)).astype(BF16)
        return use

    def tap_index(td, th):
        return td * 6 + th * 3 if th < 2 else TAIL + 3 * TAIL_ORDER.index(td)

    def weight_grad(own_t, ext, part, swap, groups, between):
        for k, (layers, taps, more) in enumerate(groups):
            blocks = [(b, d) for b in range(NB) for d in layers]

            def rhs(td, th):
                d0, h0 = (2 - td, 2 - th) if swap else (td, th)
                return jnp.concatenate([lines(ext, b, d + d0, h0) for b, d in blocks], axis=0)

            right = jnp.concatenate([rhs(*t) for t in taps], axis=1)
            cut = 3 * NC // 2
            halves = []
            for top in (0, cut):
                lhs = jnp.concatenate([own_t[(b * ND + d) * NH + h, pl.ds(top, cut)] for b, d in blocks for h in range(NH)], axis=1)
                halves.append(jnp.dot(lhs, right, preferred_element_type=F32))
            out = jnp.concatenate(halves, axis=0)
            for n, (td, th) in enumerate(taps):
                for tw in range(3):
                    blk = out[tw * NC:(tw + 1) * NC, n * NC:(n + 1) * NC]
                    to = tap_index(td, th) + tw
                    blk = blk if swap else blk.T
                    part[to] = part[to] + blk if more else blk
            between(k)

    both_layers = tuple(range(ND))
    dw1_groups = [(both_layers, ((td, 0), (td, 1)), False) for td in range(3)] + [(both_layers, ((0, 2), (2, 2)), False), (both_layers, ((1, 2),), False)]

    def plane(td):
        return tuple((td, th) for th in range(3))

    dw2_inner = [dw1_groups[1], dw1_groups[4], ((0,), plane(0), False), ((1,), plane(2), False)]
    dw2_outer = [((1,), plane(0), True), ((0,), plane(2), True)]

    half, piece = NC // 2, NC // 16
    axes = (("y", "z"), ("z", "y"))
    coord = {"x": x, "y": y, "z": z}
    parts = (p2, p1)
    outs = (dw2_out, dw1_out)
    low, high = pl.ds(0, TAPS // 2), pl.ds(TAPS // 2, TAPS // 2)
    high27 = pl.ds(TAPS // 2, TAPS // 2 - 1)

    def sems(q, n):
        return ar_send.at[q, n // 11], ar_recv.at[q, n]

    def turn(c, off):
        return lax.rem(c + off, RING)

    def chunk(q, off):
        c = turn(coord[axes[q % 2][0]], off)
        return pl.ds(pl.multiple_of(row * half + (q % 2) * (half // 2) + c * piece, piece), piece)

    def pair_copy(s, n):
        theirs = pl.ds(pl.multiple_of(other * half, half), half)
        taps = (pl.ds(0, TAIL), pl.ds(TAIL, 6), pl.ds(TAIL + 6, 4))[n]
        return rdma(parts[s].at[taps, theirs], cr.at[s, taps], *sems(s, 11), (other, dep))

    def scatter_copy(q, n):
        part = parts[q // 2]
        nxt, prv = (row, ring_dep(axes[q % 2][0], 1)), (row, ring_dep(axes[q % 2][0], RING - 1))
        src, dst, dev = (
            (part.at[low, chunk(q, 2)], ra.at[q], nxt),
            (part.at[high, chunk(q, 2)], rb.at[q], prv),
            (part.at[high, chunk(q, 1)], lr.at[q, 0, high], nxt),
            (part.at[low, chunk(q, 3)], lr.at[q, 1, low], prv),
            (ra.at[q], lr.at[q, 0, low], nxt),
            (rb.at[q], lr.at[q, 1, high], prv),
        )[n]
        return rdma(src, dst, *sems(q, min(n, 2)), dev)

    def second_copy(q, off):
        axis = axes[q % 2][1]
        j = turn(coord[axis], off)
        return rdma(bz.at[q, pl.ds(j * TQ, TQ)], r2.at[q, off - 1], *sems(q, 3), (row, ring_dep(axis, off)))

    def third_copy(q, off, slot):
        return rdma(xb.at[q, slot], xb.at[q, slot], *sems(q, 4), (row, ring_dep("x", off)))

    def fourth_copy(q, off, j):
        return rdma(ds.at[q, pl.ds(j * TQ, TQ)], ds.at[q, pl.ds(j * TQ, TQ)], *sems(q, 5), (row, ring_dep(axes[q % 2][1], off)))

    def gather_copy(q, n):
        out = outs[q // 2]
        nxt, prv = (row, ring_dep(axes[q % 2][0], 1)), (row, ring_dep(axes[q % 2][0], RING - 1))
        taps, off, dev = (
            (low, 0, nxt),
            (high27, 0, prv),
            (high27, 0, nxt),
            (low, 0, prv),
            (low, 3, nxt),
            (high27, 1, prv),
        )[n]
        src = ds.at[q, taps] if n < 4 else out.at[taps, chunk(q, off)]
        return rdma(src, out.at[taps, chunk(q, off)], *sems(q, 6 + min(n, 2) + n // 4), dev)

    def out_copy(q, n):
        out = outs[q // 2]
        taps, off = ((low, 3), (high27, 1), (high27, 3), (low, 1), (low, 2), (high27, 2), (pl.ds(0, 27), 0))[n]
        src = ds.at[q, taps] if off == 0 else out.at[taps, chunk(q, off)]
        return rdma(src, out.at[taps, chunk(q, off)], *sems(q, 10), (other, dep))

    def group(q, n):
        bands = [outs[0].at[:, pl.ds(0, k * piece)] for k in (1, 1, 4)]
        refs = [ra.at[q], rb.at[q], lr.at[q]] + [r2.at[q]] * 3 + [ra.at[q], ra.at[q, pl.ds(1, TAPS // 2 - 1)]] + bands + [cr.at[0]]
        ref = refs[n]
        return rdma(ref, ref, *sems(q, n), (other, dep))

    my_half = pl.ds(pl.multiple_of(row * half, half), half)

    dw2_q, dw1_q = 0, 2

    def both(step, q):
        step(q)
        step(q + 1)

    def step_pair(s):
        group(s, 11).wait_recv()

        def add(t, carry):
            parts[s][t, my_half] += cr[s, t]
            return carry

        lax.fori_loop(0, TAPS, add, 0)
        for n in range(4):
            for u in range(2):
                scatter_copy(2 * s + u, n).start()

    def step_relay(q):
        part = parts[q // 2]
        to_next, to_prev = chunk(q, 1), chunk(q, 3)
        scatter_copy(q, 0).wait_recv()
        ra[q] += part[low, to_next]
        scatter_copy(q, 4).start()
        scatter_copy(q, 1).wait_recv()
        rb[q] += part[high, to_prev]
        scatter_copy(q, 5).start()

    def step_first(q):
        group(q, 2).wait_recv()
        bz[q] = parts[q // 2][:, chunk(q, 0)] + (lr[q, 0] + lr[q, 1])
        for off in FAR_FIRST:
            second_copy(q, off).start()

    def step_second(q):
        group(q, 3).wait_recv()
        c = coord[axes[q % 2][1]]
        xb[q, x] = (bz[q, pl.ds(c * TQ, TQ)] + r2[q, 0]) + (r2[q, 1] + r2[q, 2])
        for off in FAR_FIRST:
            third_copy(q, off, x).start()

    def step_third(q):
        group(q, 4).wait_recv()
        c = coord[axes[q % 2][1]]
        ds[q, pl.ds(c * TQ, TQ)] = (xb[q, 0] + xb[q, 1]) + (xb[q, 2] + xb[q, 3])
        for off in FAR_FIRST:
            fourth_copy(q, off, c).start()

    def step_fourth(q):
        group(q, 5).wait_recv()
        for n in range(4):
            gather_copy(q, n).start()
        out_copy(q, 6).start()
        outs[q // 2][:, chunk(q, 0)] = ds[q, pl.ds(0, 27)]

    def step_forward(q):
        for n in range(2):
            gather_copy(q, n).wait_recv()
            gather_copy(q, 4 + n).start()
            out_copy(q, n).start()

    def step_fifth(q):
        for n in (8, 9):
            group(q, n).wait_recv()
            for piece_n in (2 * n - 14, 2 * n - 13):
                out_copy(q, piece_n).start()

    def finish_sum(q):
        group(q, 10).wait_recv()
        all_sent = cr.at[:, :, pl.ds(0, 6 * piece)]
        rdma(all_sent, all_sent, *sems(q, 0), (other, dep)).wait_send()
        if q < 2:
            group(q, 11).wait_send()

    def after_dw2(k):
        if k == 1:
            for n in range(3):
                pair_copy(0, n).start()

    def after_dw1(k):
        if k >= 2:
            pair_copy(1, k - 2).start()

    def finish_halos():
        for k in range(4):
            finish_halo(k)

    def finish_sums():
        for q in range(4):
            finish_sum(q)

    loads[0].wait()
    loads[1].wait()
    side(0).wait_recv()
    conv_inner(xe, w1, acc1, False)
    loads[2].wait()
    loads[3].wait()
    side(1).wait_recv()
    conv_inner(ge, w2, acc2, True)
    pass_corners(0)
    take_faces(0)
    conv_outer_rows(xe, w1, acc1, False, after_conv1)
    side(2).start()
    each_face(2, start, every, every)
    pass_corners(1)
    side(2).wait_recv()
    conv_inner(ze, w2, acc1, False)
    weight_grad(zt, ge, p2, True, dw2_inner, lambda k: None)
    take_faces(1)
    weight_grad(zt, ge, p2, True, dw2_outer, after_dw2)
    relay_far(2, hops[2])
    conv_outer_rows(ge, w2, acc2, True, after_conv_g)
    step_pair(0)
    side(3).start()
    each_face(3, start, early, early)
    weight_grad(at, xe, p1, False, dw1_groups, after_dw1)
    pass_corners(2)
    both(step_relay, dw2_q)
    step_pair(1)
    side(3).wait_recv()
    conv_inner(ae, w1, acc2, True, 0, 1)
    relay_far(3, (1,))
    both(step_first, dw2_q)
    both(step_relay, dw1_q)
    take_faces(2)
    conv_outer(ze, w2, acc1, False)
    both(step_second, dw2_q)
    each_face(3, start, late, ())
    both(step_first, dw1_q)
    each_face(3, start, (), late)
    each_row(acc1, after_add(xe, y_out))
    both(step_third, dw2_q)
    pass_corners(3)
    both(step_second, dw1_q)
    conv_inner(ae, w1, acc2, True, 1, 2)
    relay_far(3, (3,))
    both(step_fourth, dw2_q)
    both(step_third, dw1_q)
    both(step_forward, dw2_q)
    both(step_fourth, dw1_q)
    take_faces(3)
    conv_outer(ae, w1, acc2, True)
    each_row(acc2, after_add(ge, dx_out))
    both(step_forward, dw1_q)
    both(step_fifth, dw2_q)
    both(step_fifth, dw1_q)
    finish_halos()
    finish_sums()


def to_hbm(y_vm, dx_vm, dw1_vm, dw2_vm, y_hbm, dx_hbm, dw1_hbm, dw2_hbm, sem):
    pairs = ((y_vm, y_hbm), (dx_vm, dx_hbm), (dw1_vm, dw1_hbm), (dw2_vm, dw2_hbm))
    for n, (src, dst) in enumerate(pairs):
        if n < 2:
            pltpu.make_async_copy(src, dst, sem.at[n]).start()
        else:
            for td in range(3):
                pltpu.make_async_copy(src.at[pl.ds(td * 6, 6)], dst.at[pl.ds(td * 9, 6)], sem.at[n]).start()
                tail = TAIL + 3 * TAIL_ORDER.index(td)
                pltpu.make_async_copy(src.at[pl.ds(tail, 3)], dst.at[pl.ds(td * 9 + 6, 3)], sem.at[n]).start()
    for n, (src, dst) in enumerate(pairs):
        pltpu.make_async_copy(src, dst, sem.at[n]).wait()


def solution(mesh):
    depth_count = mesh.shape["dep"]
    vol_spec = P(None, "dep", "row", None, None)

    def local_step(x_tile, w_conv1, w_conv2, g_tile):
        width = x_tile.shape[3]
        ext = pltpu.VMEM((NB, ND + 2, NH + 2, width, NC), BF16)
        acc = pltpu.VMEM((NB, 6, NH * width, NC), F32)
        trans = pltpu.VMEM((NB * ND * NH, 3 * NC, width), BF16)
        wts = pltpu.VMEM((3, 3, 3, NC, NC), BF16)
        part = pltpu.VMEM((TAPS, NC, NC), F32)
        anywhere = pl.BlockSpec(memory_space=pl.ANY)
        outs = pl.pallas_call(
            functools.partial(kernel, width, depth_count),
            out_shape=(
                pltpu.VMEM(x_tile.shape, BF16),
                pltpu.VMEM(x_tile.shape, BF16),
                pltpu.VMEM((27, NC, NC), F32),
                pltpu.VMEM((27, NC, NC), F32),
            ),
            in_specs=[anywhere] * 4,
            out_specs=(pl.BlockSpec(memory_space=pltpu.VMEM),) * 4,
            scratch_shapes=[
                ext, ext, ext, ext, wts, wts, acc, acc,
                pltpu.VMEM((NB * ND * NH, width, NC), F32),
                trans, trans,
                part, part,
                pltpu.VMEM((2, TAPS, NC // 2, NC), F32),
                pltpu.VMEM((4, TAPS // 2, NC // 16, NC), F32),
                pltpu.VMEM((4, TAPS // 2, NC // 16, NC), F32),
                pltpu.VMEM((4, 2, TAPS, NC // 16, NC), F32),
                pltpu.VMEM((4, TAPS, NC // 16, NC), F32),
                pltpu.VMEM((4, RING - 1, TQ, NC // 16, NC), F32),
                pltpu.VMEM((4, RING, TQ, NC // 16, NC), F32),
                pltpu.VMEM((4, TAPS, NC // 16, NC), F32),
                pltpu.VMEM((2, 2, NB, 1, width, NC), BF16),
                pltpu.SemaphoreType.DMA((4, 2)),
                pltpu.SemaphoreType.DMA((4, 2, 2)),
                pltpu.SemaphoreType.DMA((4, 3)),
                pltpu.SemaphoreType.DMA((4, 3)),
                pltpu.SemaphoreType.DMA((4, 2)),
                pltpu.SemaphoreType.DMA((4, 12)),
                pltpu.SemaphoreType.DMA((2, 4)),
                pltpu.SemaphoreType.DMA((2, 2)),
                pltpu.SemaphoreType.DMA((4,)),
            ],
            compiler_params=pltpu.CompilerParams(collective_id=0, has_side_effects=True, vmem_limit_bytes=56 * 1000 * 1000),
        )(x_tile, w_conv1, w_conv2, g_tile)
        y_tile, dx_tile, dw1, dw2 = pl.pallas_call(
            to_hbm,
            out_shape=(
                jax.ShapeDtypeStruct(x_tile.shape, BF16),
                jax.ShapeDtypeStruct(x_tile.shape, BF16),
                jax.ShapeDtypeStruct((27, NC, NC), F32),
                jax.ShapeDtypeStruct((27, NC, NC), F32),
            ),
            in_specs=[pl.BlockSpec(memory_space=pltpu.VMEM)] * 4,
            out_specs=(anywhere,) * 4,
            scratch_shapes=[pltpu.SemaphoreType.DMA((4,))],
            compiler_params=pltpu.CompilerParams(vmem_limit_bytes=4 * 1000 * 1000),
        )(*outs)
        shape = w_conv1.shape
        return (y_tile, dx_tile, dw1.reshape(shape), dw2.reshape(shape))

    return jax.shard_map(local_step, mesh=mesh, in_specs=(vol_spec, P(), P(), vol_spec), out_specs=(vol_spec, vol_spec, P(), P()), check_vma=False)
```

```python
import functools
import math

import jax
import jax.numpy as jnp
from jax import lax
from jax.experimental import pallas as pl
from jax.experimental.pallas import tpu as pltpu
from jax.sharding import PartitionSpec as P

MESH = pl.DeviceIdType.MESH
F32 = jnp.float32
BF16 = jnp.bfloat16
S2PI = math.sqrt(2.0 / math.pi)
C3 = 0.044715

NB, ND, NH, NC = 2, 2, 4, 128
RING = 4
TAPS = 28
TQ = TAPS // RING
TAIL, TAIL_ORDER = 18, (0, 2, 1)
FAR_FIRST = (2, 1, 3)


def kernel(width, depth_count,
           x_hbm, w1_hbm, w2_hbm, g_hbm,
           y_out, dx_out, dw1_out, dw2_out,
           xe, ge, ze, ae, w1, w2, acc1, acc2, dgel, zt, at,
           p2, p1, cr, ra, rb, lr, bz, r2, xb, ds, hold,
           hs_send, hs_recv, rs_send, rs_recv, ar_send, ar_recv, hold_send, hold_recv, lsem):
    rows = NH * width
    row = lax.axis_index("row")
    dep = lax.axis_index("dep")
    x = lax.rem(dep, RING)
    y = lax.rem(dep // RING, RING)
    z = dep // (RING * RING)
    other = 1 - row
    exts = (xe, ge, ze, ae)
    edge = (NH - 1) - (NH - 1) * row
    my_pad = (NH + 1) * row

    def ring_dep(axis, off):
        if axis == "x":
            return dep - x + lax.rem(x + off, RING)
        if axis == "y":
            return dep - RING * y + RING * lax.rem(y + off, RING)
        return dep - RING * RING * z + RING * RING * lax.rem(z + off, RING)

    def rdma(src, dst, ssem, rsem, dev):
        return pltpu.make_async_remote_copy(src_ref=src, dst_ref=dst, send_sem=ssem, recv_sem=rsem, device_id=dev, device_id_type=MESH)

    has_below = dep > 0
    has_above = dep < depth_count - 1
    near_above, near_below = x < RING - 1, x > 0

    lines_out = (edge, row, row + 1, row + 2)
    ways = ((True, has_above, has_below, near_above), (False, has_below, has_above, near_below))
    hops = {2: (2, 3), 3: (1, 3)}
    every, early, late = range(NH), range(2), range(2, NH)

    def source(k, up, n):
        d = ND - 1 if up else 0
        if k < 2:
            return (x_hbm, g_hbm)[k].at[:, d, pl.ds(lines_out[n], 1)]
        return exts[k].at[:, d + 1, pl.ds(1 + lines_out[n], 1)]

    def landing(k, up, n):
        return exts[k].at[:, 0 if up else ND + 1, pl.ds(1 + lines_out[n], 1)]

    def face(k, up, n):
        return rdma(source(k, up, n), landing(k, up, n), hs_send.at[k, int(up)], hs_recv.at[k, int(up), min(n, 1)], (row, dep + (2 * up - 1)))

    def rows_of(k, up, count):
        ref = exts[k].at[:, 0, pl.ds(1, count)]
        return rdma(ref, ref, hs_send.at[k, int(up)], hs_recv.at[k, int(up), 1], (row, dep))

    def far_hop(k, up, n):
        i = hops[k].index(n)
        return rdma(source(k, up, n), hold.at[k - 2, i], hold_send.at[k - 2, i], hold_recv.at[k - 2, i], (row, dep + RING * (2 * up - 1)))

    def far_land(k, up, n):
        i = hops[k].index(n)
        return rdma(hold.at[k - 2, i], landing(k, up, n), hold_send.at[k - 2, 2 + i], hs_recv.at[k, int(up), 1], (row, dep - (RING - 1) * (2 * up - 1)))

    def side(k):
        if k < 2:
            src = (x_hbm, g_hbm)[k].at[:, :, pl.ds(edge, 1)]
        else:
            src = exts[k].at[:, pl.ds(1, ND), pl.ds(1 + edge, 1)]
        return rdma(src, exts[k].at[:, pl.ds(1, ND), pl.ds(my_pad, 1)], rs_send.at[k, 0], rs_recv.at[k, 0], (other, dep))

    def corner(k, up):
        at_face = exts[k].at[:, 0 if up else ND + 1]
        return rdma(at_face.at[:, pl.ds(1 + edge, 1)], at_face.at[:, pl.ds(my_pad, 1)], rs_send.at[k, 1 + up], rs_recv.at[k, 1 + up], (other, dep))

    relays = ((x == RING - 1) & (dep >= RING), (x == 0) & (dep < depth_count - RING))

    def each_face(k, do, which, far_which):
        for n in range(NH):
            for up, has, _, near in ways:
                if n in which:
                    @pl.when(near)
                    def _():
                        do(face(k, up, n))

                if n in far_which:
                    @pl.when(has & jnp.logical_not(near))
                    def _():
                        do((far_hop if n in hops.get(k, ()) else face)(k, up, n))

    def start(copy):
        copy.start()

    def relay_far(k, which):
        for (up, *_), cond in zip(ways, relays):
            @pl.when(cond)
            def _():
                for n in which:
                    far_hop(k, up, n).wait_recv()
                    far_land(k, up, n).start()

    def pass_corners(k):
        for up, _, comes, *_ in ways:
            @pl.when(comes)
            def _():
                face(k, up, 0).wait_recv()
                corner(k, up).start()

    def take_faces(k):
        for up, _, comes, *_ in ways:
            @pl.when(comes)
            def _():
                corner(k, up).wait_recv()
                rows_of(k, up, NH - 1).wait_recv()

    def finish_halo(k):
        side(k).wait_send()
        for up, has, _, near in ways:
            @pl.when(near)
            def _():
                rows_of(k, up, NH).wait_send()

            @pl.when(has & jnp.logical_not(near))
            def _():
                rows_of(k, up, NH - len(hops.get(k, ()))).wait_send()
                for n in hops.get(k, ()):
                    far_hop(k, up, n).wait_send()

        for (up, *_), cond in zip(ways, relays):
            @pl.when(cond)
            def _():
                for n in hops.get(k, ()):
                    far_land(k, up, n).wait_send()

        for up, _, comes, *_ in ways:
            @pl.when(comes)
            def _():
                corner(k, up).wait_send()

    barrier = pltpu.get_barrier_semaphore()
    pl.semaphore_signal(barrier, inc=1, device_id=(other, dep), device_id_type=MESH)
    for axis in ("x", "y", "z"):
        for off in range(1, RING):
            pl.semaphore_signal(barrier, inc=1, device_id=(row, ring_dep(axis, off)), device_id_type=MESH)

    for step in (1, depth_count - 1, RING, depth_count - RING):
        pl.semaphore_signal(barrier, inc=1, device_id=(row, lax.rem(dep + step, depth_count)), device_id_type=MESH)

    loads = [
        pltpu.make_async_copy(x_hbm, xe.at[:, pl.ds(1, ND), pl.ds(1, NH)], lsem.at[0]),
        pltpu.make_async_copy(w1_hbm, w1, lsem.at[1]),
        pltpu.make_async_copy(g_hbm, ge.at[:, pl.ds(1, ND), pl.ds(1, NH)], lsem.at[2]),
        pltpu.make_async_copy(w2_hbm, w2, lsem.at[3]),
    ]
    for load in loads:
        load.start()

    pl.semaphore_wait(barrier, 14)

    for k in range(2):
        side(k).start()
        each_face(k, start, every, every)

    zero_row = jnp.zeros((NB, 1, width, NC), BF16)
    for ext in exts:
        for dd in range(ND + 2):
            ext[:, dd, pl.ds(my_pad, 1)] = zero_row
    zero_face = jnp.zeros((NH + 2, width, NC), BF16)

    @pl.when(dep == 0)
    def _():
        for ext in exts:
            for b in range(NB):
                ext[b, 0] = zero_face

    @pl.when(dep == depth_count - 1)
    def _():
        for ext in exts:
            for b in range(NB):
                ext[b, ND + 1] = zero_face

    p2[TAPS - 1] = jnp.zeros((NC, NC), F32)
    p1[TAPS - 1] = jnp.zeros((NC, NC), F32)

    def lines(ext, b, dd, h0):
        return ext[b, dd, pl.ds(h0, NH)].reshape(rows, NC)

    def tap_block(w, td, th, tw, flip):
        return w[2 - td, 2 - th, 2 - tw] if flip else w[td, th, tw]

    def weights(w, cells, flip):
        zero = jnp.zeros((NC, NC), BF16)
        blocks = [[zero if t is None else tap_block(w, *t, flip) for t in line] for line in cells]
        if flip:
            return jnp.concatenate([jnp.concatenate([blocks[k][n] for k in range(len(blocks))], axis=1) for n in range(len(blocks[0]))], axis=0)
        return jnp.concatenate([jnp.concatenate(line, axis=1) for line in blocks], axis=0)

    def mul(lhs, rhs, flip):
        return lax.dot_general(lhs, rhs, (((1,), (1 if flip else 0,)), ((), ())), preferred_element_type=F32)

    def conv_inner(ext, w, acc, flip, b0=0, b1=NB):
        order = ((0, 0), (0, 1), (1, 0), (1, 1), (0, 2), (1, 2))
        cells = [[(dd - d, th, tw) for d, tw in order] for dd in (1, 2) for th in range(3)]

        def one(b, carry):
            lhs = jnp.concatenate([lines(ext, b, dd, th) for dd in (1, 2) for th in range(3)], axis=1)
            for n in range(3):
                out = mul(lhs, weights(w, [line[2 * n:2 * n + 2] for line in cells], flip), flip)
                for j in range(2):
                    d, tw = order[2 * n + j]
                    acc[b, d * 3 + tw] = out[:, j * NC:(j + 1) * NC]
            return carry

        lax.fori_loop(b0, b1, one, 0)

    def outer_block(ext, w, acc, flip, b, d):
        lhs = jnp.concatenate([lines(ext, b, 3 * d, th) for th in range(3)], axis=1)
        out = mul(lhs, weights(w, [[(2 * d, th, tw) for tw in range(3)] for th in range(3)], flip), flip)
        for tw in range(3):
            acc[b, d * 3 + tw] += out[:, tw * NC:(tw + 1) * NC]

    def conv_outer(ext, w, acc, flip):
        def one(i, carry):
            outer_block(ext, w, acc, flip, i // ND, lax.rem(i, ND))
            return carry

        lax.fori_loop(0, NB * ND, one, 0)

    wpos = lax.broadcasted_iota(jnp.int32, (width, NC), 0)

    def from_left(v):
        return jnp.where(wpos > 0, pltpu.roll(v, 1, 0), 0.0)

    def from_right(v):
        return jnp.where(wpos < width - 1, pltpu.roll(v, width - 1, 0), 0.0)

    def one_row(acc, use, b, d, h):
        at_rows = pl.ds(h * width, width)
        total = acc[b, d * 3 + 1, at_rows] + from_left(acc[b, d * 3, at_rows]) + from_right(acc[b, d * 3 + 2, at_rows])
        use((b * ND + d) * NH + h, b, d, h, total)

    def each_row(acc, use):
        def one(j, carry):
            for h in range(NH):
                one_row(acc, use, j // ND, lax.rem(j, ND), h)
            return carry

        lax.fori_loop(0, NB * ND, one, 0)

    def conv_outer_rows(ext, w, acc, flip, use):
        blocks = [(b, d) for b in range(NB) for d in range(ND)]
        for now, done in zip(blocks + [()], [()] + blocks):
            if now:
                outer_block(ext, w, acc, flip, *now)
            if done:
                for h in range(NH):
                    one_row(acc, use, *done, h)

    def after_conv1(i, b, d, h, total):
        a = total.astype(BF16).astype(F32)
        a2 = a * a
        t = jnp.tanh(S2PI * (a + C3 * (a2 * a)))
        cdf = 0.5 * (1.0 + t)
        gel = a * cdf
        dgel[i] = cdf + (0.5 * a * ((1.0 + t) * (1.0 - t))) * (S2PI * (1.0 + 3.0 * C3 * a2))
        ze[b, 1 + d, 1 + h] = gel.astype(BF16)
        for tw, v in enumerate((from_left(gel), gel, from_right(gel))):
            zt[i, pl.ds(tw * NC, NC)] = v.astype(BF16).T

    def after_conv_g(i, b, d, h, total):
        da = total * dgel[i]
        ae[b, 1 + d, 1 + h] = da.astype(BF16)
        for tw, v in enumerate((from_right(da), da, from_left(da))):
            at[i, pl.ds(tw * NC, NC)] = v.astype(BF16).T

    def after_add(ext, out):
        def use(i, b, d, h, total):
            out[b, d, h] = (total + ext[b, 1 + d, 1 + h].astype(F32)).astype(BF16)
        return use

    def tap_index(td, th):
        return td * 6 + th * 3 if th < 2 else TAIL + 3 * TAIL_ORDER.index(td)

    def weight_grad(own_t, ext, part, swap, groups, between):
        for k, (layers, taps, more) in enumerate(groups):
            blocks = [(b, d) for b in range(NB) for d in layers]

            def rhs(td, th):
                d0, h0 = (2 - td, 2 - th) if swap else (td, th)
                return jnp.concatenate([lines(ext, b, d + d0, h0) for b, d in blocks], axis=0)

            right = jnp.concatenate([rhs(*t) for t in taps], axis=1)
            cut = 3 * NC // 2
            halves = []
            for top in (0, cut):
                lhs = jnp.concatenate([own_t[(b * ND + d) * NH + h, pl.ds(top, cut)] for b, d in blocks for h in range(NH)], axis=1)
                halves.append(jnp.dot(lhs, right, preferred_element_type=F32))
            out = jnp.concatenate(halves, axis=0)
            for n, (td, th) in enumerate(taps):
                for tw in range(3):
                    blk = out[tw * NC:(tw + 1) * NC, n * NC:(n + 1) * NC]
                    to = tap_index(td, th) + tw
                    blk = blk if swap else blk.T
                    part[to] = part[to] + blk if more else blk
            between(k)

    both_layers = tuple(range(ND))
    dw1_groups = [(both_layers, ((td, 0), (td, 1)), False) for td in range(3)] + [(both_layers, ((0, 2), (2, 2)), False), (both_layers, ((1, 2),), False)]

    def plane(td):
        return tuple((td, th) for th in range(3))

    dw2_inner = [dw1_groups[1], dw1_groups[4], ((0,), plane(0), False), ((1,), plane(2), False)]
    dw2_outer = [((1,), plane(0), True), ((0,), plane(2), True)]

    half, piece = NC // 2, NC // 16
    axes = (("y", "z"), ("z", "y"))
    coord = {"x": x, "y": y, "z": z}
    parts = (p2, p1)
    outs = (dw2_out, dw1_out)
    low, high = pl.ds(0, TAPS // 2), pl.ds(TAPS // 2, TAPS // 2)
    high27 = pl.ds(TAPS // 2, TAPS // 2 - 1)

    def sems(q, n):
        return ar_send.at[q, n // 11], ar_recv.at[q, n]

    def turn(c, off):
        return lax.rem(c + off, RING)

    def chunk(q, off):
        c = turn(coord[axes[q % 2][0]], off)
        return pl.ds(pl.multiple_of(row * half + (q % 2) * (half // 2) + c * piece, piece), piece)

    def pair_copy(s, n):
        theirs = pl.ds(pl.multiple_of(other * half, half), half)
        taps = (pl.ds(0, TAIL), pl.ds(TAIL, 6), pl.ds(TAIL + 6, 4))[n]
        return rdma(parts[s].at[taps, theirs], cr.at[s, taps], *sems(s, 11), (other, dep))

    def scatter_copy(q, n):
        part = parts[q // 2]
        nxt, prv = (row, ring_dep(axes[q % 2][0], 1)), (row, ring_dep(axes[q % 2][0], RING - 1))
        src, dst, dev = (
            (part.at[low, chunk(q, 2)], ra.at[q], nxt),
            (part.at[high, chunk(q, 2)], rb.at[q], prv),
            (part.at[high, chunk(q, 1)], lr.at[q, 0, high], nxt),
            (part.at[low, chunk(q, 3)], lr.at[q, 1, low], prv),
            (ra.at[q], lr.at[q, 0, low], nxt),
            (rb.at[q], lr.at[q, 1, high], prv),
        )[n]
        return rdma(src, dst, *sems(q, min(n, 2)), dev)

    def second_copy(q, off):
        axis = axes[q % 2][1]
        j = turn(coord[axis], off)
        return rdma(bz.at[q, pl.ds(j * TQ, TQ)], r2.at[q, off - 1], *sems(q, 3), (row, ring_dep(axis, off)))

    def third_copy(q, off, slot):
        return rdma(xb.at[q, slot], xb.at[q, slot], *sems(q, 4), (row, ring_dep("x", off)))

    def fourth_copy(q, off, j):
        return rdma(ds.at[q, pl.ds(j * TQ, TQ)], ds.at[q, pl.ds(j * TQ, TQ)], *sems(q, 5), (row, ring_dep(axes[q % 2][1], off)))

    def gather_copy(q, n):
        out = outs[q // 2]
        nxt, prv = (row, ring_dep(axes[q % 2][0], 1)), (row, ring_dep(axes[q % 2][0], RING - 1))
        taps, off, dev = (
            (low, 0, nxt),
            (high27, 0, prv),
            (high27, 0, nxt),
            (low, 0, prv),
            (low, 3, nxt),
            (high27, 1, prv),
        )[n]
        src = ds.at[q, taps] if n < 4 else out.at[taps, chunk(q, off)]
        return rdma(src, out.at[taps, chunk(q, off)], *sems(q, 6 + min(n, 2) + n // 4), dev)

    def out_copy(q, n):
        out = outs[q // 2]
        taps, off = ((low, 3), (high27, 1), (high27, 3), (low, 1), (low, 2), (high27, 2), (pl.ds(0, 27), 0))[n]
        src = ds.at[q, taps] if off == 0 else out.at[taps, chunk(q, off)]
        return rdma(src, out.at[taps, chunk(q, off)], *sems(q, 10), (other, dep))

    def group(q, n):
        bands = [outs[0].at[:, pl.ds(0, k * piece)] for k in (1, 1, 4)]
        refs = [ra.at[q], rb.at[q], lr.at[q]] + [r2.at[q]] * 3 + [ra.at[q], ra.at[q, pl.ds(1, TAPS // 2 - 1)]] + bands + [cr.at[0]]
        ref = refs[n]
        return rdma(ref, ref, *sems(q, n), (other, dep))

    my_half = pl.ds(pl.multiple_of(row * half, half), half)

    dw2_q, dw1_q = 0, 2

    def both(step, q):
        step(q)
        step(q + 1)

    def step_pair(s):
        group(s, 11).wait_recv()

        def add(t, carry):
            parts[s][t, my_half] += cr[s, t]
            return carry

        lax.fori_loop(0, TAPS, add, 0)
        for n in range(4):
            for u in range(2):
                scatter_copy(2 * s + u, n).start()

    def step_relay(q):
        part = parts[q // 2]
        to_next, to_prev = chunk(q, 1), chunk(q, 3)
        scatter_copy(q, 0).wait_recv()
        ra[q] += part[low, to_next]
        scatter_copy(q, 4).start()
        scatter_copy(q, 1).wait_recv()
        rb[q] += part[high, to_prev]
        scatter_copy(q, 5).start()

    def step_first(q):
        group(q, 2).wait_recv()
        bz[q] = parts[q // 2][:, chunk(q, 0)] + (lr[q, 0] + lr[q, 1])
        for off in FAR_FIRST:
            second_copy(q, off).start()

    def step_second(q):
        group(q, 3).wait_recv()
        c = coord[axes[q % 2][1]]
        xb[q, x] = (bz[q, pl.ds(c * TQ, TQ)] + r2[q, 0]) + (r2[q, 1] + r2[q, 2])
        for off in FAR_FIRST:
            third_copy(q, off, x).start()

    def step_third(q):
        group(q, 4).wait_recv()
        c = coord[axes[q % 2][1]]
        ds[q, pl.ds(c * TQ, TQ)] = (xb[q, 0] + xb[q, 1]) + (xb[q, 2] + xb[q, 3])
        for off in FAR_FIRST:
            fourth_copy(q, off, c).start()

    def step_fourth(q):
        group(q, 5).wait_recv()
        for n in range(4):
            gather_copy(q, n).start()
        out_copy(q, 6).start()
        outs[q // 2][:, chunk(q, 0)] = ds[q, pl.ds(0, 27)]

    def step_forward(q):
        for n in range(2):
            gather_copy(q, n).wait_recv()
            gather_copy(q, 4 + n).start()
            out_copy(q, n).start()

    def step_fifth(q):
        for n in (8, 9):
            group(q, n).wait_recv()
            for piece_n in (2 * n - 14, 2 * n - 13):
                out_copy(q, piece_n).start()

    def finish_sum(q):
        group(q, 10).wait_recv()
        all_sent = cr.at[:, :, pl.ds(0, 6 * piece)]
        rdma(all_sent, all_sent, *sems(q, 0), (other, dep)).wait_send()
        if q < 2:
            group(q, 11).wait_send()

    def after_dw2(k):
        if k == 1:
            for n in range(3):
                pair_copy(0, n).start()

    def after_dw1(k):
        if k >= 2:
            pair_copy(1, k - 2).start()

    def finish_halos():
        for k in range(4):
            finish_halo(k)

    def finish_sums():
        for q in range(4):
            finish_sum(q)

    loads[0].wait()
    loads[1].wait()
    side(0).wait_recv()
    conv_inner(xe, w1, acc1, False)
    loads[2].wait()
    loads[3].wait()
    side(1).wait_recv()
    conv_inner(ge, w2, acc2, True)
    pass_corners(0)
    take_faces(0)
    conv_outer_rows(xe, w1, acc1, False, after_conv1)
    side(2).start()
    each_face(2, start, every, every)
    pass_corners(1)
    side(2).wait_recv()
    conv_inner(ze, w2, acc1, False)
    weight_grad(zt, ge, p2, True, dw2_inner, lambda k: None)
    take_faces(1)
    weight_grad(zt, ge, p2, True, dw2_outer, after_dw2)
    relay_far(2, hops[2])
    conv_outer_rows(ge, w2, acc2, True, after_conv_g)
    step_pair(0)
    side(3).start()
    each_face(3, start, early, early)
    weight_grad(at, xe, p1, False, dw1_groups, after_dw1)
    pass_corners(2)
    both(step_relay, dw2_q)
    step_pair(1)
    side(3).wait_recv()
    conv_inner(ae, w1, acc2, True, 0, 1)
    relay_far(3, (1,))
    both(step_first, dw2_q)
    both(step_relay, dw1_q)
    take_faces(2)
    conv_outer(ze, w2, acc1, False)
    both(step_second, dw2_q)
    each_face(3, start, late, ())
    both(step_first, dw1_q)
    each_face(3, start, (), late)
    each_row(acc1, after_add(xe, y_out))
    both(step_third, dw2_q)
    pass_corners(3)
    both(step_second, dw1_q)
    conv_inner(ae, w1, acc2, True, 1, 2)
    relay_far(3, (3,))
    both(step_fourth, dw2_q)
    both(step_third, dw1_q)
    both(step_forward, dw2_q)
    both(step_fourth, dw1_q)
    take_faces(3)
    conv_outer_rows(ae, w1, acc2, True, after_add(ge, dx_out))
    both(step_forward, dw1_q)
    both(step_fifth, dw2_q)
    both(step_fifth, dw1_q)
    finish_halos()
    finish_sums()


def to_hbm(y_vm, dx_vm, dw1_vm, dw2_vm, y_hbm, dx_hbm, dw1_hbm, dw2_hbm, sem):
    pairs = ((y_vm, y_hbm), (dx_vm, dx_hbm), (dw1_vm, dw1_hbm), (dw2_vm, dw2_hbm))
    for n, (src, dst) in enumerate(pairs):
        if n < 2:
            pltpu.make_async_copy(src, dst, sem.at[n]).start()
        else:
            for td in range(3):
                pltpu.make_async_copy(src.at[pl.ds(td * 6, 6)], dst.at[pl.ds(td * 9, 6)], sem.at[n]).start()
                tail = TAIL + 3 * TAIL_ORDER.index(td)
                pltpu.make_async_copy(src.at[pl.ds(tail, 3)], dst.at[pl.ds(td * 9 + 6, 3)], sem.at[n]).start()
    for n, (src, dst) in enumerate(pairs):
        pltpu.make_async_copy(src, dst, sem.at[n]).wait()


def solution(mesh):
    depth_count = mesh.shape["dep"]
    vol_spec = P(None, "dep", "row", None, None)

    def local_step(x_tile, w_conv1, w_conv2, g_tile):
        width = x_tile.shape[3]
        ext = pltpu.VMEM((NB, ND + 2, NH + 2, width, NC), BF16)
        acc = pltpu.VMEM((NB, 6, NH * width, NC), F32)
        trans = pltpu.VMEM((NB * ND * NH, 3 * NC, width), BF16)
        wts = pltpu.VMEM((3, 3, 3, NC, NC), BF16)
        part = pltpu.VMEM((TAPS, NC, NC), F32)
        anywhere = pl.BlockSpec(memory_space=pl.ANY)
        outs = pl.pallas_call(
            functools.partial(kernel, width, depth_count),
            out_shape=(
                pltpu.VMEM(x_tile.shape, BF16),
                pltpu.VMEM(x_tile.shape, BF16),
                pltpu.VMEM((27, NC, NC), F32),
                pltpu.VMEM((27, NC, NC), F32),
            ),
            in_specs=[anywhere] * 4,
            out_specs=(pl.BlockSpec(memory_space=pltpu.VMEM),) * 4,
            scratch_shapes=[
                ext, ext, ext, ext, wts, wts, acc, acc,
                pltpu.VMEM((NB * ND * NH, width, NC), F32),
                trans, trans,
                part, part,
                pltpu.VMEM((2, TAPS, NC // 2, NC), F32),
                pltpu.VMEM((4, TAPS // 2, NC // 16, NC), F32),
                pltpu.VMEM((4, TAPS // 2, NC // 16, NC), F32),
                pltpu.VMEM((4, 2, TAPS, NC // 16, NC), F32),
                pltpu.VMEM((4, TAPS, NC // 16, NC), F32),
                pltpu.VMEM((4, RING - 1, TQ, NC // 16, NC), F32),
                pltpu.VMEM((4, RING, TQ, NC // 16, NC), F32),
                pltpu.VMEM((4, TAPS, NC // 16, NC), F32),
                pltpu.VMEM((2, 2, NB, 1, width, NC), BF16),
                pltpu.SemaphoreType.DMA((4, 2)),
                pltpu.SemaphoreType.DMA((4, 2, 2)),
                pltpu.SemaphoreType.DMA((4, 3)),
                pltpu.SemaphoreType.DMA((4, 3)),
                pltpu.SemaphoreType.DMA((4, 2)),
                pltpu.SemaphoreType.DMA((4, 12)),
                pltpu.SemaphoreType.DMA((2, 4)),
                pltpu.SemaphoreType.DMA((2, 2)),
                pltpu.SemaphoreType.DMA((4,)),
            ],
            compiler_params=pltpu.CompilerParams(collective_id=0, has_side_effects=True, vmem_limit_bytes=56 * 1000 * 1000),
        )(x_tile, w_conv1, w_conv2, g_tile)
        y_tile, dx_tile, dw1, dw2 = pl.pallas_call(
            to_hbm,
            out_shape=(
                jax.ShapeDtypeStruct(x_tile.shape, BF16),
                jax.ShapeDtypeStruct(x_tile.shape, BF16),
                jax.ShapeDtypeStruct((27, NC, NC), F32),
                jax.ShapeDtypeStruct((27, NC, NC), F32),
            ),
            in_specs=[pl.BlockSpec(memory_space=pltpu.VMEM)] * 4,
            out_specs=(anywhere,) * 4,
            scratch_shapes=[pltpu.SemaphoreType.DMA((4,))],
            compiler_params=pltpu.CompilerParams(vmem_limit_bytes=4 * 1000 * 1000),
        )(*outs)
        shape = w_conv1.shape
        return (y_tile, dx_tile, dw1.reshape(shape), dw2.reshape(shape))

    return jax.shard_map(local_step, mesh=mesh, in_specs=(vol_spec, P(), P(), vol_spec), out_specs=(vol_spec, vol_spec, P(), P()), check_vma=False)
```
